128 devices in a mesh: tok: 16 (over z, x), mp: 8 (over y, core).
Axes of the slice: x: 4, y: 4, z: 4, core: 2. Of those that a mesh axis runs over, the one named last changes fastest.
Arguments:
- tokens: bfloat16 [6144, 2048], P('tok', 'mp'), may hold values from -120 to 120
- norm_gain: float32 [2048], replicated, may hold values from 0.5 to 1.5
- running_sq: float32 [2048], P('mp'), may hold values from 0.5 to 4
- gate_weight: bfloat16 [2048, 8192], P(None, 'mp'), may hold values from -0.125 to 0.125
- up_weight: bfloat16 [2048, 8192], P(None, 'mp'), may hold values from -0.125 to 0.125
- down_weight_t: bfloat16 [2048, 8192], P(None, 'mp'), may hold values from -0.0625 to 0.0625
- groups: int32 [384], P('tok'), may hold values from 0 to 47, as said below
- cotangent: bfloat16 [6144, 2048], P('tok', 'mp'), may hold values from -6 to 6
Outputs:
- block_out: bfloat16 [6144, 2048], P('tok', 'mp')
- grad_tokens: bfloat16 [6144, 2048], P('tok', 'mp')
- running_new: float32 [2048], P('mp')
- grad_gain: float32 [2048], P('mp')
- grad_gate: float32 [2048, 8192], P('tok', 'mp')
- grad_up: float32 [2048, 8192], P('tok', 'mp')
- grad_down_t: float32 [2048, 8192], P('tok', 'mp')
The draws below stay inside these ranges and needn't reach their ends.
Inputs may be any that keep to these rules, and one draw needn't show every extreme that they name: Each of the 48 ghost groups holds exactly 8 blocks.
All inputs are finite; a program needn't handle non-finite values.
Results may differ from the reference program's by a relative error of at most 0.02.
Values may be sent and summed in bfloat16 or wider, within the bound.
A program may use at most 128 MiB of HBM per device.

```python
import math
import jax
import jax.numpy as jnp
from jax import lax

D = 2048
FF = 8192
GHOST = 128
BLK = 16
TOKENS = 6144
GROUPS = 48
NBLK = 384


def draw_groups(key, part):
    blocks_per_group = GHOST // BLK
    order = jax.random.permutation(jax.random.fold_in(key, 11), NBLK)
    return (order // blocks_per_group).astype(jnp.int32)


def draw_tokens(key, part):
    key_base, key_block, key_column = jax.random.split(jax.random.fold_in(key, 23), 3)
    position = jnp.arange(TOKENS, dtype=jnp.float32)
    rising = jnp.exp(jnp.log(3.0) * position / TOKENS)
    block_scale = jnp.exp(jax.random.uniform(key_block, (NBLK,), jnp.float32, jnp.log(0.5), jnp.log(2.0)))
    row_scale = jnp.broadcast_to(block_scale[:, None], (NBLK, BLK)).reshape(TOKENS) * rising
    column_scale = jnp.exp(jax.random.uniform(key_column, (D,), jnp.float32, jnp.log(0.3), jnp.log(3.0)))
    base = jnp.clip(jax.random.normal(key_base, (TOKENS, D), jnp.float32), -6.0, 6.0)
    return (base * row_scale[:, None] * column_scale[None, :]).astype(jnp.bfloat16)


def level_of(stream_key, dims, pieces, low, top_value):
    def one(dim, shards_of):
        draws = jax.random.uniform(jax.random.fold_in(jax.random.fold_in(stream_key, 6), dim), (shards_of,), jnp.float32, low / len(pieces), top_value / len(pieces))
        return jnp.repeat(jnp.exp(draws), dims[dim] // shards_of).reshape((-1,) + (1,) * (len(dims) - dim - 1))

    loudness = one(*pieces[0])
    for cut in pieces[1:]:
        loudness = loudness * one(*cut)
    return loudness


def noise(rng, extent, width, bound, shards=(), kind=jnp.bfloat16):
    array = jax.random.normal(rng, extent, jnp.float32) * width
    if len(shards) > 0:
        array = level_of(rng, extent, shards, -0.22, 0.18) * array
    return jnp.clip(array, min=-bound, max=bound).astype(kind)


def setup_inputs(seed: int = 0) -> dict:
    key_of = jax.random.split(jax.random.key(seed), 9)
    return {
        "tokens": draw_tokens(jax.random.fold_in(key_of[8], 71), 0),
        "norm_gain": jnp.clip(1.0 + 0.1 * jax.random.normal(key_of[1], (D,), jnp.float32), 0.5, 1.5),
        "running_sq": jnp.clip(jnp.exp(math.log(4.0) - 2.0794415 * jax.random.uniform(key_of[2], (D,), jnp.float32) ** level_of(key_of[2], (D,), ((0, 8),), -0.2, 0.2)), 0.5, 4.0),
        "gate_weight": noise(key_of[3], (D, FF), D ** -0.5, 0.125, ((1, 8),)),
        "up_weight": noise(key_of[4], (D, FF), D ** -0.5, 0.125, ((1, 8),)),
        "down_weight_t": noise(key_of[5], (D, FF), FF ** -0.5, 0.0625, ((1, 8),)),
        "groups": draw_groups(jax.random.fold_in(key_of[8], 71), 0),
        "cotangent": noise(key_of[7], (TOKENS, D), 1.0, 6.0, ((0, 16), (1, 8))),
    }


epsilon = 1e-05
momentum = 0.1
highest = lax.Precision.HIGHEST

def group_onehot(groups):
    return (groups[None, :] == jnp.arange(GROUPS, dtype=jnp.int32)[:, None]).astype(jnp.float32)

def group_sums(values, onehot):
    blocks = values.reshape(values.shape[0] // BLK, BLK, values.shape[1]).sum(axis=1)
    return jnp.dot(onehot, blocks, precision=highest, preferred_element_type=jnp.float32)

def per_token(table, onehot):
    per_block = jnp.dot(onehot.T, table, precision=highest, preferred_element_type=jnp.float32)
    wide = jnp.broadcast_to(per_block[:, None, :], (per_block.shape[0], BLK, per_block.shape[1]))
    return wide.reshape(per_block.shape[0] * BLK, per_block.shape[1])

def reference(tokens, norm_gain, running_sq, gate_weight, up_weight, down_weight_t, groups, cotangent):
    onehot = group_onehot(groups)
    x_float = tokens.astype(jnp.float32)
    quad_mean = group_sums(x_float * x_float, onehot) / GHOST
    scale = per_token(lax.rsqrt(quad_mean + epsilon), onehot)
    normed = x_float * scale
    hid_in = (norm_gain * normed).astype(jnp.bfloat16)
    gate = jnp.dot(hid_in, gate_weight, preferred_element_type=jnp.float32)
    lift = jnp.dot(hid_in, up_weight, preferred_element_type=jnp.float32)
    sigma = jax.nn.sigmoid(gate)
    hidden = (gate * sigma * lift).astype(jnp.bfloat16)
    branch = lax.dot_general(hidden, down_weight_t, (((1,), (1,)), ((), ())), preferred_element_type=jnp.float32)
    block_out = (x_float + branch).astype(jnp.bfloat16)
    running_new = (1.0 - momentum) * running_sq + momentum * lax.optimization_barrier(jnp.mean(quad_mean, axis=0))
    grad_down_t = lax.dot_general(cotangent, hidden, (((0,), (0,)), ((), ())), preferred_element_type=jnp.float32)
    grad_hidden = jnp.dot(cotangent, down_weight_t, preferred_element_type=jnp.float32)
    grad_gate_in = (grad_hidden * lift * sigma * (1.0 + gate * (1.0 - sigma))).astype(jnp.bfloat16)
    grad_lift = (grad_hidden * gate * sigma).astype(jnp.bfloat16)
    grad_gate = lax.dot_general(hid_in, grad_gate_in, (((0,), (0,)), ((), ())), preferred_element_type=jnp.float32)
    grad_up = lax.dot_general(hid_in, grad_lift, (((0,), (0,)), ((), ())), preferred_element_type=jnp.float32)
    grad_normed_in = lax.dot_general(grad_gate_in, gate_weight, (((1,), (1,)), ((), ())), preferred_element_type=jnp.float32)
    grad_normed_in = grad_normed_in + lax.dot_general(grad_lift, up_weight, (((1,), (1,)), ((), ())), preferred_element_type=jnp.float32)
    partial_value = group_sums(grad_normed_in * normed, onehot)
    grad_gain = lax.optimization_barrier(jnp.sum(partial_value, axis=0))
    mean_term = per_token(norm_gain * partial_value / GHOST, onehot)
    grad_tokens = (cotangent.astype(jnp.float32) + scale * (norm_gain * grad_normed_in - normed * mean_term)).astype(jnp.bfloat16)
    return (block_out, grad_tokens, running_new, grad_gain, grad_gate, grad_up, grad_down_t)
```

```python
import jax
import jax.numpy as jnp
from jax import lax
from jax.experimental import pallas as pl
from jax.experimental.pallas import tpu as pltpu
from jax.sharding import PartitionSpec as P

GHOST = 128
BLK = 16
ROWS = 384
FEAT = 256
WIDTH = 2048
HALF = 512
GROUPS = 48
NB = 24
TOK = 16
PIECES = 6

epsilon = 1e-05
momentum = 0.1
F32 = jnp.float32
BF16 = jnp.bfloat16
HIGHEST = lax.Precision.HIGHEST


def kernel(
    tok_hbm, gain_ref, run_ref, gw_hbm, uw_hbm, dw_hbm, grp_ref, cot_hbm,
    bo_ref, gt_ref, rn_ref, gg_ref, gr_ref,
    XT, NRM, BSUM, SCB, DYB, HB, LT, W, G, GT, LF, GH,
    SB, PS, PA, RSA, SPA, QA, R1, R2, PB, T1, T2, BK, BS, U1, BP, U2,
    EK, ES, ER, V1, V2, WS, W1, FS,
    lsem, gsend, grecv, ssend, srecv, wsend, wrecv, ysend, yrecv,
):
    t = lax.axis_index("tok")
    m = lax.axis_index("mp")
    z, x = t // 4, t % 4
    y, c = m // 2, m % 2
    zp = z + 1 - 2 * (z % 2)
    zs = 3 - z
    role = ((z + 1) // 2) % 2
    yp, ym, y2 = (y + 1) % 4, (y + 3) % 4, (y + 2) % 4
    xp, xm, x2 = (x + 1) % 4, (x + 3) % 4, (x + 2) % 4
    dC = (t, y * 2 + 1 - c)
    dP = (zp * 4 + x, m)
    dS = (zs * 4 + x, m)
    dYp, dYm = (t, yp * 2 + c), (t, ym * 2 + c)
    dXp, dXm = (z * 4 + xp, m), (z * 4 + xm, m)

    def rc(src, dst, ss, rs, dev):
        return pltpu.make_async_remote_copy(
            src_ref=src, dst_ref=dst, send_sem=ss, recv_sem=rs,
            device_id=dev, device_id_type=pl.DeviceIdType.MESH,
        )

    own_cols = pl.ds(pl.multiple_of(m * FEAT, FEAT), FEAT)

    cp_dy = pltpu.make_async_copy(cot_hbm, DYB.at[0, :, own_cols], lsem.at[0])
    cp_dy.start()
    cp_x = pltpu.make_async_copy(tok_hbm, XT, lsem.at[1])
    cp_x.start()
    wcols = pl.ds(pl.multiple_of(role * HALF, HALF), HALF)
    cp_w = [
        pltpu.make_async_copy(h.at[:, wcols], W.at[i], lsem.at[2 + i])
        for i, h in enumerate((gw_hbm, uw_hbm, dw_hbm))
    ]
    for k in (2, 0, 1):
        cp_w[k].start()

    bar = pltpu.get_barrier_semaphore()
    for k in range(1, TOK):
        pl.semaphore_signal(
            bar, inc=1, device_id=((t + k) % TOK, m), device_id_type=pl.DeviceIdType.MESH
        )
    for d in (dC, dYp, dYm):
        pl.semaphore_signal(bar, inc=1, device_id=d, device_id_type=pl.DeviceIdType.MESH)
    pl.semaphore_wait(bar, TOK - 1 + 3)

    def sl(B, slot, yy, cc, r0=0, n=ROWS):
        return B.at[slot, pl.ds(r0, n), pl.ds(pl.multiple_of((yy * 2 + cc) * FEAT, FEAT), FEAT)]

    def gcopy(B, g, k):
        h = ROWS // 2
        if k == 0:
            a, b, d = sl(B, 0, y, c), sl(B, 1, y, c), dP
        elif k == 1:
            a = b = sl(B, 0, y, c)
            d = dYp
        elif k == 2:
            a = b = sl(B, 0, y, c)
            d = dYm
        elif k == 3:
            a = b = sl(B, 0, ym, c, 0, h)
            d = dYp
        elif k == 4:
            a = b = sl(B, 0, yp, c, h, h)
            d = dYm
        elif k == 5:
            a = b = sl(B, 1, y, c)
            d = dYp
        elif k == 6:
            a = b = sl(B, 1, y, c)
            d = dYm
        elif k == 7:
            a, b, d = sl(B, 0, y2, c), sl(B, 1, y2, c), dP
        else:
            slot = (k - 8) // 4
            yy = (y, ym, yp, y2)[(k - 8) % 4]
            a = b = sl(B, slot, yy, c)
            d = dC
        return rc(a, b, gsend.at[g, k], grecv.at[g, k], d)

    def gland(B, g, k):
        h = ROWS // 2
        if k == 0:
            b = sl(B, 1, y, c)
        elif k == 1:
            b = sl(B, 0, ym, c)
        elif k == 2:
            b = sl(B, 0, yp, c)
        elif k == 3:
            b = sl(B, 0, y2, c, 0, h)
        elif k == 4:
            b = sl(B, 0, y2, c, h, h)
        elif k == 5:
            b = sl(B, 1, ym, c)
        elif k == 6:
            b = sl(B, 1, yp, c)
        elif k == 7:
            b = sl(B, 1, y2, c)
        else:
            b = sl(B, (k - 8) // 4, (y, ym, yp, y2)[(k - 8) % 4], 1 - c)
        rc(b, b, gsend.at[g, k], grecv.at[g, k], dC).wait_recv()

    def gstart(B, g, *ks):
        for k in ks:
            gcopy(B, g, k).start()

    def fwdA(B, g):
        gland(B, g, 1)
        gstart(B, g, 3, 9)
        gland(B, g, 2)
        gstart(B, g, 4, 10)

    def fwdP(B, g):
        gland(B, g, 0)
        gstart(B, g, 5, 6, 12)

    def fwdB(B, g):
        gland(B, g, 3)
        gland(B, g, 4)
        gstart(B, g, 7, 11)

    def fwdC(B, g):
        gland(B, g, 5)
        gstart(B, g, 13)
        gland(B, g, 6)
        gstart(B, g, 14)

    def fwdD(B, g):
        gland(B, g, 7)
        gstart(B, g, 15)

    def table_send(buf, e):
        for k in range(1, TOK):
            rc(buf.at[t], buf.at[t], ssend.at[e, k], srecv.at[e, k], ((t + k) % TOK, m)).start()

    def table_sum(buf, e):
        for k in range(1, TOK):
            s = (t + TOK - k) % TOK
            rc(buf.at[s], buf.at[s], ssend.at[e, k], srecv.at[e, k], dC).wait_recv()
        total = buf[0].astype(F32)
        for k in range(1, TOK):
            total = total + buf[k].astype(F32)
        return total

    grow = grp_ref[...]
    onehot = (
        lax.broadcasted_iota(jnp.int32, (GROUPS, NB), 0) == jnp.broadcast_to(grow, (GROUPS, NB))
    ).astype(F32)
    diag = lax.broadcasted_iota(jnp.int32, (NB, NB), 0) == lax.broadcasted_iota(
        jnp.int32, (NB, NB), 1
    )
    gcol = jnp.sum(
        jnp.where(diag, jnp.broadcast_to(grow, (NB, NB)), 0).astype(F32), axis=1, keepdims=True
    )
    onehot_t = (
        lax.broadcasted_iota(jnp.int32, (NB, GROUPS), 1).astype(F32)
        == jnp.broadcast_to(gcol, (NB, GROUPS))
    ).astype(F32)

    cp_dy.wait()
    gstart(DYB, 0, 1, 2, 8)
    cp_x.wait()
    for b in range(NB):
        xb = XT[b * BLK : (b + 1) * BLK, :].astype(F32)
        BSUM[b : b + 1, :] = jnp.sum(xb * xb, axis=0, keepdims=True)
    SB[t] = jnp.dot(onehot, BSUM[...], precision=HIGHEST, preferred_element_type=F32).astype(BF16)
    table_send(SB, 0)
    gstart(DYB, 0, 0)
    fwdA(DYB, 0)
    fwdP(DYB, 0)

    quad = table_sum(SB, 0) / GHOST
    rn_ref[...] = (1.0 - momentum) * run_ref[...] + momentum * (
        jnp.sum(quad, axis=0, keepdims=True) / GROUPS
    )
    SCB[...] = jnp.dot(
        onehot_t, lax.rsqrt(quad + epsilon), precision=HIGHEST, preferred_element_type=F32
    )
    gain = gain_ref[:, own_cols]
    for b in range(NB):
        rows = slice(b * BLK, (b + 1) * BLK)
        nb = XT[rows, :].astype(F32) * SCB[b : b + 1, :]
        NRM[rows, :] = nb
        HB[0, rows, own_cols] = (gain * nb).astype(BF16)
    gstart(HB, 1, 1, 2, 8, 0)

    fwdB(DYB, 0)
    fwdC(DYB, 0)
    fwdD(DYB, 0)
    for k in range(8, 16):
        gland(DYB, 0, k)

    def transposed(B, i, slot):
        @pl.loop(0, 8)
        def _(j):
            cols = pl.ds(pl.multiple_of(j * FEAT, FEAT), FEAT)
            LT[i, cols, pl.ds(slot * ROWS, ROWS)] = B[slot, :, cols].T

    def units(slot):
        GT[...] = jnp.dot(HB[slot], W[0], preferred_element_type=F32)
        LF[...] = jnp.dot(HB[slot], W[1], preferred_element_type=F32)

        @pl.loop(0, ROWS // 16)
        def _(i):
            r = pl.ds(pl.multiple_of(i * 16, 16), 16)
            ro = pl.ds(pl.multiple_of(slot * ROWS + i * 16, 16), 16)
            gate, lift, gh = GT[r, :], LF[r, :], GH[slot, r, :]
            sigma = jax.nn.sigmoid(gate)
            G[2, ro, :] = (gate * sigma * lift).astype(BF16)
            G[0, ro, :] = (gh * lift * sigma * (1.0 + gate * (1.0 - sigma))).astype(BF16)
            G[1, ro, :] = (gh * gate * sigma).astype(BF16)

    cp_w[2].wait()
    for s in range(2):
        GH[s] = jnp.dot(DYB[s], W[2], preferred_element_type=F32)
    fwdA(HB, 1)
    fwdP(HB, 1)
    transposed(DYB, 1, 0)
    transposed(DYB, 1, 1)
    fwdB(HB, 1)
    cp_w[0].wait()
    cp_w[1].wait()
    for k in range(8, 12):
        gland(HB, 1, k)
    transposed(HB, 0, 0)
    units(0)
    fwdC(HB, 1)
    fwdD(HB, 1)
    for k in range(12, 16):
        gland(HB, 1, k)
    transposed(HB, 0, 1)
    units(1)

    AS, AP, AX1P, AX1M, AX2P, AX2M, BX1P, BX1M, BX2P, BX2M, BSK, BPK = range(12)

    def wcopy(k, p, src, dst, dev):
        return rc(src, dst, wsend.at[k, p], wrecv.at[k, p], dev)

    def wland(k, p, dst):
        rc(dst, dst, wsend.at[k, p], wrecv.at[k, p], dC).wait_recv()

    pair = z // 2

    def c_as(p):
        rows = pl.ds(pl.multiple_of((1 - pair) * 1024, 1024), 1024)
        return wcopy(AS, p, PA.at[p, rows], RSA.at[p], dS)

    def c_ap(p):
        return wcopy(AP, p, SPA.at[p], QA.at[p, :, role], dP)

    def c_ax1(p):
        return (
            wcopy(AX1P, p, QA.at[p, x2, 0], R1.at[p, 0], dXp),
            wcopy(AX1M, p, QA.at[p, x2, 1], R1.at[p, 1], dXm),
        )

    def c_ax2(p):
        return (
            wcopy(AX2P, p, QA.at[p, xp], R2.at[p, 0], dXp),
            wcopy(AX2M, p, QA.at[p, xm], R2.at[p, 1], dXm),
        )

    def c_bx1(p):
        return (
            wcopy(BX1P, p, PB.at[p, x2, pl.ds(0, 2)], T1.at[p, 0], dXp),
            wcopy(BX1M, p, PB.at[p, x2, pl.ds(2, 2)], T1.at[p, 1], dXm),
        )

    def c_bx2(p):
        return (
            wcopy(BX2P, p, PB.at[p, xp], T2.at[p, 0], dXp),
            wcopy(BX2M, p, PB.at[p, xm], T2.at[p, 1], dXm),
        )

    def c_bs(p):
        return wcopy(BSK, p, BS.at[p], U1.at[p], dS)

    def c_bp(p):
        return wcopy(BPK, p, BP.at[p], U2.at[p], dP)

    def weights(lo, hi):
        @pl.loop(lo, hi)
        def _(p):
            mi, j = p // 2, p % 2

            @pl.loop(0, 4)
            def _(rb):
                rows = pl.ds(pl.multiple_of(rb * HALF, HALF), HALF)
                res = jnp.dot(
                    LT[mi // 2, rows, :],
                    G[mi, :, pl.ds(pl.multiple_of(j * 256, 256), 256)],
                    preferred_element_type=F32,
                ).astype(BF16)
                PA[p, rows, :] = res[:, :128]
                for xd in range(4):
                    PB[p, xd, rb] = res[xd * 128 : (xd + 1) * 128, 128:]

            c_as(p).start()
            for d in c_bx1(p):
                d.start()

    def plus(a, b):
        return a.astype(F32) + b.astype(F32)

    def step_bx2(lo, hi):
        @pl.loop(lo, hi)
        def _(p):
            up, down = c_bx2(p)
            wland(BX1P, p, T1.at[p, 0])
            for i in range(2):
                PB[p, xp, i] = plus(PB[p, xp, i], T1[p, 0, i]).astype(BF16)
            up.start()
            wland(BX1M, p, T1.at[p, 1])
            for i in range(2):
                PB[p, xm, 2 + i] = plus(PB[p, xm, 2 + i], T1[p, 1, i]).astype(BF16)
            down.start()

    def step_bs(lo, hi):
        @pl.loop(lo, hi)
        def _(p):
            wland(BX2P, p, T2.at[p, 0])
            wland(BX2M, p, T2.at[p, 1])
            for i in range(2):
                o = 2 * (1 - pair) + i
                BS[p, i] = (plus(PB[p, x, o], T2[p, 0, o]) + T2[p, 1, o].astype(F32)).astype(BF16)
            c_bs(p).start()
            for i in range(2):
                o = 2 * pair + i
                BK[p, i] = plus(PB[p, x, o], T2[p, 0, o]) + T2[p, 1, o].astype(F32)

    def out_cols(p, half, off):
        return pl.ds(pl.multiple_of(half * HALF + (p % 2) * 256 + off, 128), 128)

    def step_bp(lo, hi):
        @pl.loop(lo, hi)
        def _(p):
            wland(BSK, p, U1.at[p])
            BP[p] = plus(BK[p, zp % 2], U1[p, zp % 2]).astype(BF16)
            c_bp(p).start()
            gr_ref[p // 2, :, out_cols(p, role, 128)] = plus(BK[p, z % 2], U1[p, z % 2])

    def step_bf(lo, hi):
        @pl.loop(lo, hi)
        def _(p):
            wland(BPK, p, U2.at[p])
            gr_ref[p // 2, :, out_cols(p, 1 - role, 128)] = U2[p].astype(F32)

    def step_ap(lo, hi):
        @pl.loop(lo, hi)
        def _(p):
            wland(AS, p, RSA.at[p])
            for xd in range(4):
                ra = pl.ds(pl.multiple_of(zp * HALF + xd * 128, 128), 128)
                rr = pl.ds(pl.multiple_of((zp % 2) * HALF + xd * 128, 128), 128)
                SPA[p, xd] = plus(PA[p, ra, :], RSA[p, rr, :]).astype(BF16)
            c_ap(p).start()
            for xd in range(4):
                ra = pl.ds(pl.multiple_of(z * HALF + xd * 128, 128), 128)
                rr = pl.ds(pl.multiple_of((z % 2) * HALF + xd * 128, 128), 128)
                QA[p, xd, role] = plus(PA[p, ra, :], RSA[p, rr, :]).astype(BF16)

    def step_ax1(lo, hi):
        @pl.loop(lo, hi)
        def _(p):
            wland(AP, p, QA.at[p, :, 1 - role])
            for d in c_ax1(p):
                d.start()

    def step_ax2(lo, hi):
        @pl.loop(lo, hi)
        def _(p):
            up, down = c_ax2(p)
            wland(AX1P, p, R1.at[p, 0])
            QA[p, xp, 0] = plus(QA[p, xp, 0], R1[p, 0]).astype(BF16)
            up.start()
            wland(AX1M, p, R1.at[p, 1])
            QA[p, xm, 1] = plus(QA[p, xm, 1], R1[p, 1]).astype(BF16)
            down.start()

    def step_af(lo, hi):
        @pl.loop(lo, hi)
        def _(p):
            wland(AX2P, p, R2.at[p, 0])
            wland(AX2M, p, R2.at[p, 1])
            for h in range(2):
                gr_ref[p // 2, :, out_cols(p, h, 0)] = plus(QA[p, x, h], R2[p, 0, h]) + R2[
                    p, 1, h
                ].astype(F32)

    def ycopy(e, k):
        lo, hi = pl.ds(0, ROWS), pl.ds(ROWS, ROWS)
        a, b, d = (
            (ES.at[e], ER.at[e], dC),
            (EK.at[e, y2, lo], V1.at[e, 0], dYp),
            (EK.at[e, y2, hi], V1.at[e, 1], dYm),
            (EK.at[e, yp], V2.at[e, 0], dYp),
            (EK.at[e, ym], V2.at[e, 1], dYm),
            (WS.at[e], W1.at[e], dP),
        )[k]
        return rc(a, b, ysend.at[e, k], yrecv.at[e, k], d)

    def yland(e, k):
        b = (ER.at[e], V1.at[e, 0], V1.at[e, 1], V2.at[e, 0], V2.at[e, 1], W1.at[e])[k]
        rc(b, b, ysend.at[e, k], yrecv.at[e, k], dC).wait_recv()

    def nt(a, b):
        return lax.dot_general(a, b, (((1,), (1,)), ((), ())), preferred_element_type=F32)

    def y_compute(e):
        def block(dst, cc):
            @pl.loop(0, 4)
            def _(yy):
                rows = pl.ds(pl.multiple_of((yy * 2 + cc) * FEAT, FEAT), FEAT)
                if e == 0:
                    v = nt(G[0], W[0, rows, :]) + nt(G[1], W[1, rows, :])
                else:
                    v = nt(G[2], W[2, rows, :])
                dst[e, yy] = v.astype(BF16)

        block(ES, 1 - c)
        ycopy(e, 0).start()
        block(EK, c)

    def y_v1(e):
        yland(e, 0)
        for yy in (y2, yp, ym, y):
            @pl.loop(0, 6)
            def _(i):
                r = pl.ds(pl.multiple_of(i * 128, 128), 128)
                EK[e, yy, r, :] = plus(EK[e, yy, r, :], ER[e, yy, r, :]).astype(BF16)

            if yy is y2:
                ycopy(e, 1).start()
                ycopy(e, 2).start()

    def y_v2(e):
        for d, (k, yy) in enumerate(((1, yp), (2, ym))):
            yland(e, k)

            @pl.loop(0, 3)
            def _(i):
                r = pl.ds(pl.multiple_of(d * ROWS + i * 128, 128), 128)
                rv = pl.ds(pl.multiple_of(i * 128, 128), 128)
                EK[e, yy, r, :] = plus(EK[e, yy, r, :], V1[e, d, rv, :]).astype(BF16)

            ycopy(e, k + 2).start()

    def y_p(e):
        yland(e, 3)
        yland(e, 4)

        @pl.loop(0, 3)
        def _(i):
            r = pl.ds(pl.multiple_of(ROWS + i * 128, 128), 128)
            rv = pl.ds(pl.multiple_of(i * 128, 128), 128)
            WS[e, rv, :] = (
                plus(EK[e, y, r, :], V2[e, 0, r, :]) + V2[e, 1, r, :].astype(F32)
            ).astype(BF16)

        ycopy(e, 5).start()

        @pl.loop(0, 3)
        def _(i):
            r = pl.ds(pl.multiple_of(i * 128, 128), 128)
            FS[e, r, :] = plus(EK[e, y, r, :], V2[e, 0, r, :]) + V2[e, 1, r, :].astype(F32)

    def y_block_out():
        yland(1, 5)
        for b in range(NB):
            rows = slice(b * BLK, (b + 1) * BLK)
            branch = FS[1, rows, :] + W1[1, rows, :].astype(F32)
            bo_ref[rows, :] = (XT[rows, :].astype(F32) + branch).astype(BF16)

    def y_partial():
        yland(0, 5)
        for b in range(NB):
            rows = slice(b * BLK, (b + 1) * BLK)
            g = FS[0, rows, :] + W1[0, rows, :].astype(F32)
            FS[0, rows, :] = g
            BSUM[b : b + 1, :] = jnp.sum(g * NRM[rows, :], axis=0, keepdims=True)
        PS[t] = jnp.dot(
            onehot, BSUM[...], precision=HIGHEST, preferred_element_type=F32
        ).astype(BF16)
        table_send(PS, 1)

    def y_grad_tokens():
        total = table_sum(PS, 1)
        gg_ref[...] = jnp.sum(total, axis=0, keepdims=True)
        BSUM[...] = jnp.dot(
            onehot_t, gain * total / GHOST, precision=HIGHEST, preferred_element_type=F32
        )
        for b in range(NB):
            rows = slice(b * BLK, (b + 1) * BLK)
            g, nb = FS[0, rows, :], NRM[rows, :]
            dyb = DYB[0, rows, own_cols].astype(F32)
            gt_ref[rows, :] = (
                dyb + SCB[b : b + 1, :] * (gain * g - nb * BSUM[b : b + 1, :])
            ).astype(BF16)

    weights(0, 3)
    y_compute(0)
    weights(3, 6)
    y_v1(0)
    step_ap(0, 1)
    y_compute(1)
    step_bx2(0, 3)
    step_ax1(0, 1)
    step_ap(1, 2)
    y_v1(1)
    step_bx2(3, 6)
    y_v2(0)
    step_ax2(0, 1)
    step_ax1(1, 2)
    step_bs(0, 2)
    step_ap(2, 3)
    y_v2(1)
    step_ax2(1, 2)
    step_ax1(2, 3)
    step_bs(2, 4)
    step_ap(3, 4)
    y_p(0)
    step_ax2(2, 3)
    step_bs(4, 6)
    step_ax1(3, 4)
    y_partial()
    step_ap(4, 5)
    step_ax2(3, 4)
    y_p(1)
    step_ax1(4, 5)
    step_ap(5, 6)
    step_ax2(4, 5)
    step_ax1(5, 6)
    y_grad_tokens()
    y_block_out()
    step_af(0, 4)
    step_bp(0, 2)
    step_ax2(5, 6)
    step_bp(2, 6)
    step_af(4, 6)
    step_bf(0, 6)

    for g, B in ((0, DYB), (1, HB)):
        for k in range(16):
            gcopy(B, g, k).wait_send()
    for e, buf in ((0, SB), (1, PS)):
        for k in range(1, TOK):
            rc(buf.at[t], buf.at[t], ssend.at[e, k], srecv.at[e, k], dC).wait_send()
    for e in range(2):
        for k in range(6):
            ycopy(e, k).wait_send()

    @pl.loop(0, PIECES)
    def _(p):
        for d in (
            c_as(p), c_ap(p), *c_ax1(p), *c_ax2(p), *c_bx1(p), *c_bx2(p), c_bs(p), c_bp(p)
        ):
            d.wait_send()


def body(tokens, norm_gain, running_sq, gate_weight, up_weight, down_weight_t, groups, cotangent):
    V = pltpu.VMEM
    any_spec = pl.BlockSpec(memory_space=pl.ANY)
    vmem_spec = pl.BlockSpec(memory_space=pltpu.VMEM)
    n = PIECES
    sq = (128, 128)
    dma = pltpu.SemaphoreType.DMA
    scratch = [
        V((ROWS, FEAT), BF16), V((ROWS, FEAT), F32), V((NB, FEAT), F32), V((NB, FEAT), F32),
        V((2, ROWS, WIDTH), BF16), V((2, ROWS, WIDTH), BF16), V((2, WIDTH, 2 * ROWS), BF16),
        V((3, WIDTH, HALF), BF16), V((3, 2 * ROWS, HALF), BF16),
        V((ROWS, HALF), F32), V((ROWS, HALF), F32), V((2, ROWS, HALF), F32),
        V((TOK, GROUPS, FEAT), BF16), V((TOK, GROUPS, FEAT), BF16),
        V((n, WIDTH, 128), BF16), V((n, 1024, 128), BF16), V((n, 4, *sq), BF16),
        V((n, 4, 2, *sq), BF16), V((n, 2, *sq), BF16), V((n, 2, 2, *sq), BF16),
        V((n, 4, 4, *sq), BF16), V((n, 2, 2, *sq), BF16), V((n, 2, 4, *sq), BF16),
        V((n, 2, *sq), F32), V((n, 2, *sq), BF16), V((n, 2, *sq), BF16),
        V((n, *sq), BF16), V((n, *sq), BF16),
        V((2, 4, 2 * ROWS, FEAT), BF16), V((2, 4, 2 * ROWS, FEAT), BF16),
        V((2, 4, 2 * ROWS, FEAT), BF16), V((2, 2, ROWS, FEAT), BF16),
        V((2, 2, 2 * ROWS, FEAT), BF16), V((2, ROWS, FEAT), BF16), V((2, ROWS, FEAT), BF16),
        V((2, ROWS, FEAT), F32),
        dma((5,)), dma((2, 16)), dma((2, 16)), dma((2, TOK)), dma((2, TOK)),
        dma((12, n)), dma((12, n)), dma((2, 6)), dma((2, 6)),
    ]
    block_out, grad_tokens, run_new, gain_grad, grads = pl.pallas_call(
        kernel,
        out_shape=(
            jax.ShapeDtypeStruct((ROWS, FEAT), BF16),
            jax.ShapeDtypeStruct((ROWS, FEAT), BF16),
            jax.ShapeDtypeStruct((1, FEAT), F32),
            jax.ShapeDtypeStruct((1, FEAT), F32),
            jax.ShapeDtypeStruct((3, 128, 1024), F32),
        ),
        in_specs=[any_spec, vmem_spec, vmem_spec, any_spec, any_spec, any_spec, vmem_spec, any_spec],
        out_specs=(vmem_spec,) * 5,
        scratch_shapes=scratch,
        compiler_params=pltpu.CompilerParams(
            collective_id=0, has_side_effects=True, vmem_limit_bytes=67043328
        ),
    )(
        tokens, norm_gain.reshape(1, -1), running_sq.reshape(1, -1), gate_weight, up_weight,
        down_weight_t, groups.reshape(1, -1), cotangent,
    )
    return (
        block_out, grad_tokens, run_new.reshape(-1), gain_grad.reshape(-1),
        grads[0], grads[1], grads[2],
    )


def solution(mesh):
    placed = (
        P("tok", "mp"),
        P(),
        P("mp"),
        P(None, "mp"),
        P(None, "mp"),
        P(None, "mp"),
        P("tok"),
        P("tok", "mp"),
    )
    return jax.shard_map(
        body,
        mesh=mesh,
        in_specs=placed,
        out_specs=(
            P("tok", "mp"),
            P("tok", "mp"),
            P("mp"),
            P("mp"),
            P("tok", "mp"),
            P("tok", "mp"),
            P("tok", "mp"),
        ),
        check_vma=False,
    )
```

```python
import jax
import jax.numpy as jnp
from jax import lax
from jax.experimental import pallas as pl
from jax.experimental.pallas import tpu as pltpu
from jax.sharding import PartitionSpec as P

GHOST = 128
BLK = 16
ROWS = 384
FEAT = 256
WIDTH = 2048
HALF = 512
GROUPS = 48
NB = 24
A_PARTS = tuple((p, 0) for p in range(5))
B_PARTS = tuple((p, 1) for p in range(5)) + ((5, 0), (5, 1))

epsilon = 1e-05
momentum = 0.1
F32 = jnp.float32
BF16 = jnp.bfloat16
HIGHEST = lax.Precision.HIGHEST


def kernel(
    tok_hbm, gain_ref, run_ref, gw_hbm, uw_hbm, dw_hbm, grp_ref, cot_hbm,
    bo_ref, gt_ref, rn_ref, gg_ref, gr_ref,
    XT, NRM, BSUM, SCB, DYB, HB, LT, W, G, GT, LF, GH,
    TZ, TX, PA, RSA, SPA, QA, R1, R2, PB, T1, T2, BK, BS, U1, BP, U2,
    EK, ES, ER, V1, V2, WS, W1, FS,
    lsem, gsend, grecv, ssend, srecv, asend, arecv, bsend, brecv, ysend, yrecv, csend, crecv,
):
    t = lax.axis_index("tok")
    m = lax.axis_index("mp")
    z, x = t // 4, t % 4
    y, c = m // 2, m % 2
    zp = z + 1 - 2 * (z % 2)
    zs = 3 - z
    role = ((z + 1) // 2) % 2
    yp, ym, y2 = (y + 1) % 4, (y + 3) % 4, (y + 2) % 4
    xp, xm, x2 = (x + 1) % 4, (x + 3) % 4, (x + 2) % 4
    dC = (t, y * 2 + 1 - c)
    dP = (zp * 4 + x, m)
    dS = (zs * 4 + x, m)
    dYp, dYm = (t, yp * 2 + c), (t, ym * 2 + c)
    dXp, dXm = (z * 4 + xp, m), (z * 4 + xm, m)

    def rc(src, dst, ss, rs, dev):
        return pltpu.make_async_remote_copy(
            src_ref=src, dst_ref=dst, send_sem=ss, recv_sem=rs,
            device_id=dev, device_id_type=pl.DeviceIdType.MESH,
        )

    own_cols = pl.ds(pl.multiple_of(m * FEAT, FEAT), FEAT)

    cp_dy = pltpu.make_async_copy(cot_hbm, DYB.at[0, :, own_cols], lsem.at[0])
    cp_dy.start()
    cp_x = pltpu.make_async_copy(tok_hbm, XT, lsem.at[1])
    cp_x.start()
    wcols = pl.ds(pl.multiple_of(role * HALF, HALF), HALF)
    cp_w = [
        pltpu.make_async_copy(h.at[:, wcols], W.at[i], lsem.at[2 + i])
        for i, h in enumerate((gw_hbm, uw_hbm, dw_hbm))
    ]
    for k in (2, 0, 1):
        cp_w[k].start()

    bar = pltpu.get_barrier_semaphore()
    z_others = [(((z + k) % 4) * 4 + x, m) for k in range(1, 4)]
    x_others = [(z * 4 + (x + k) % 4, m) for k in range(1, 4)]
    for d in (*z_others, *x_others, dC, dYp, dYm):
        pl.semaphore_signal(bar, inc=1, device_id=d, device_id_type=pl.DeviceIdType.MESH)

    def sl(B, slot, yy, cc, r0=0, n=ROWS):
        return B.at[slot, pl.ds(r0, n), pl.ds(pl.multiple_of((yy * 2 + cc) * FEAT, FEAT), FEAT)]

    def gcopy(B, g, k):
        h = ROWS // 2
        if k == 0:
            a, b, d = sl(B, 0, y, c), sl(B, 1, y, c), dP
        elif k in (1, 16):
            a = b = sl(B, 0, y, c, 0 if k == 1 else h, h)
            d = dYp
        elif k in (2, 17):
            a = b = sl(B, 0, y, c, h if k == 2 else 0, h)
            d = dYm
        elif k == 3:
            a = b = sl(B, 0, ym, c, 0, h)
            d = dYp
        elif k == 4:
            a = b = sl(B, 0, yp, c, h, h)
            d = dYm
        elif k == 5:
            a = b = sl(B, 1, y, c)
            d = dYp
        elif k == 6:
            a = b = sl(B, 1, y, c)
            d = dYm
        elif k == 7:
            a, b, d = sl(B, 0, y2, c), sl(B, 1, y2, c), dP
        else:
            slot = (k - 8) // 4
            yy = (y, ym, yp, y2)[(k - 8) % 4]
            a = b = sl(B, slot, yy, c)
            d = dC
        return rc(a, b, gsend.at[g, k], grecv.at[g, k], d)

    def gland(B, g, k):
        h = ROWS // 2
        if k == 0:
            b = sl(B, 1, y, c)
        elif k in (1, 16):
            b = sl(B, 0, ym, c, 0 if k == 1 else h, h)
        elif k in (2, 17):
            b = sl(B, 0, yp, c, h if k == 2 else 0, h)
        elif k == 3:
            b = sl(B, 0, y2, c, 0, h)
        elif k == 4:
            b = sl(B, 0, y2, c, h, h)
        elif k == 5:
            b = sl(B, 1, ym, c)
        elif k == 6:
            b = sl(B, 1, yp, c)
        elif k == 7:
            b = sl(B, 1, y2, c)
        else:
            b = sl(B, (k - 8) // 4, (y, ym, yp, y2)[(k - 8) % 4], 1 - c)
        rc(b, b, gsend.at[g, k], grecv.at[g, k], dC).wait_recv()

    def gstart(B, g, *ks):
        for k in ks:
            gcopy(B, g, k).start()

    def send_own(B, g):
        gstart(B, g, 1, 2, 0, 16, 17, 8)

    def fwd(B, g, land, *sends):
        for k in land:
            gland(B, g, k)
        gstart(B, g, *sends)

    def tcopy(e, a, k):
        buf, me, d = ((TZ, z, z_others), (TX, x, x_others))[a]
        ref = buf.at[e, me]
        return rc(ref, ref, ssend.at[e, a, k], srecv.at[e, a, k], d[k - 1])

    def tsum(e, a):
        buf, me = ((TZ, z), (TX, x))[a]
        for k in range(1, 4):
            ref = buf.at[e, (me + 4 - k) % 4]
            rc(ref, ref, ssend.at[e, a, k], srecv.at[e, a, k], dC).wait_recv()
        return (buf[e, 0].astype(F32) + buf[e, 1].astype(F32)) + (
            buf[e, 2].astype(F32) + buf[e, 3].astype(F32)
        )

    def tsend(e, a):
        for k in range(1, 4):
            tcopy(e, a, k).start()

    def tmid(e):
        TX[e, x] = tsum(e, 0).astype(BF16)
        tsend(e, 1)

    grow = grp_ref[...]
    onehot = (
        lax.broadcasted_iota(jnp.int32, (GROUPS, NB), 0) == jnp.broadcast_to(grow, (GROUPS, NB))
    ).astype(F32)
    diag = lax.broadcasted_iota(jnp.int32, (NB, NB), 0) == lax.broadcasted_iota(
        jnp.int32, (NB, NB), 1
    )
    gcol = jnp.sum(
        jnp.where(diag, jnp.broadcast_to(grow, (NB, NB)), 0).astype(F32), axis=1, keepdims=True
    )
    onehot_t = (
        lax.broadcasted_iota(jnp.int32, (NB, GROUPS), 1).astype(F32)
        == jnp.broadcast_to(gcol, (NB, GROUPS))
    ).astype(F32)

    gain = gain_ref[:, own_cols]

    def start():
        cp_x.wait()
        for b in range(NB):
            xb = XT[b * BLK : (b + 1) * BLK, :].astype(F32)
            BSUM[b : b + 1, :] = jnp.sum(xb * xb, axis=0, keepdims=True)
        TZ[0, z] = jnp.dot(
            onehot, BSUM[...], precision=HIGHEST, preferred_element_type=F32
        ).astype(BF16)
        cp_dy.wait()
        pl.semaphore_wait(bar, 9)
        tsend(0, 0)
        send_own(DYB, 0)

    def stat2():
        quad = tsum(0, 1) / GHOST
        rn_ref[...] = (1.0 - momentum) * run_ref[...] + momentum * (
            jnp.sum(quad, axis=0, keepdims=True) / GROUPS
        )
        SCB[...] = jnp.dot(
            onehot_t, lax.rsqrt(quad + epsilon), precision=HIGHEST, preferred_element_type=F32
        )
        for b in range(NB):
            rows = slice(b * BLK, (b + 1) * BLK)
            nb = XT[rows, :].astype(F32) * SCB[b : b + 1, :]
            NRM[rows, :] = nb
            HB[0, rows, own_cols] = (gain * nb).astype(BF16)

    def transposed(B, i, slot):
        @pl.loop(0, 8)
        def _(j):
            cols = pl.ds(pl.multiple_of(j * FEAT, FEAT), FEAT)
            LT[i, cols, pl.ds(slot * ROWS, ROWS)] = B[slot, :, cols].T

    def units(slot):
        if slot == 0:
            cp_w[0].wait()
            cp_w[1].wait()
        GT[...] = jnp.dot(HB[slot], W[0], preferred_element_type=F32)
        LF[...] = jnp.dot(HB[slot], W[1], preferred_element_type=F32)

        @pl.loop(0, ROWS // 16)
        def _(i):
            r = pl.ds(pl.multiple_of(i * 16, 16), 16)
            ro = pl.ds(pl.multiple_of(slot * ROWS + i * 16, 16), 16)
            gate, lift, gh = GT[r, :], LF[r, :], GH[slot, r, :]
            sigma = jax.nn.sigmoid(gate)
            G[0, ro, :] = (gate * sigma * lift).astype(BF16)
            G[1, ro, :] = (gh * lift * sigma * (1.0 + gate * (1.0 - sigma))).astype(BF16)
            G[2, ro, :] = (gh * gate * sigma).astype(BF16)

    def gh(slot):
        if slot == 0:
            cp_w[2].wait()
        GH[slot] = jnp.dot(DYB[slot], W[2], preferred_element_type=F32)

    def slot_ready(B, g, slot):
        for k in range(8 + 4 * slot, 12 + 4 * slot):
            gland(B, g, k)

    AS, AP, AX1P, AX1M, AXIP, AXIM, AX2P, AX2M = range(8)
    BX1P, BX1M, BXIP, BXIM, BX2P, BX2M, BSK, BPK = range(8)
    pair = z // 2
    lo2, hi2 = pl.ds(0, 2), pl.ds(2, 2)

    def a_copy(k, a):
        far = pl.ds(pl.multiple_of((1 - pair) * 1024, 1024), 1024)
        src, dst, d = (
            (PA.at[a, far], RSA.at[a], dS),
            (SPA.at[a], QA.at[a, :, role], dP),
            (QA.at[a, x2, 0], R1.at[a, 0], dXp),
            (QA.at[a, x2, 1], R1.at[a, 1], dXm),
            (QA.at[a, xp, 1], R2.at[a, 0, 1], dXp),
            (QA.at[a, xm, 0], R2.at[a, 1, 0], dXm),
            (QA.at[a, xp, 0], R2.at[a, 0, 0], dXp),
            (QA.at[a, xm, 1], R2.at[a, 1, 1], dXm),
        )[k]
        return rc(src, dst, asend.at[k, a], arecv.at[k, a], d)

    def a_land(k, a):
        b = (
            RSA.at[a], QA.at[a, :, 1 - role], R1.at[a, 0], R1.at[a, 1],
            R2.at[a, 0, 1], R2.at[a, 1, 0], R2.at[a, 0, 0], R2.at[a, 1, 1],
        )[k]
        rc(b, b, asend.at[k, a], arecv.at[k, a], dC).wait_recv()

    def b_copy(k, b):
        src, dst, d = (
            (PB.at[b, x2, lo2], T1.at[b, 0], dXp),
            (PB.at[b, x2, hi2], T1.at[b, 1], dXm),
            (PB.at[b, xp, hi2], T2.at[b, 0, hi2], dXp),
            (PB.at[b, xm, lo2], T2.at[b, 1, lo2], dXm),
            (PB.at[b, xp, lo2], T2.at[b, 0, lo2], dXp),
            (PB.at[b, xm, hi2], T2.at[b, 1, hi2], dXm),
            (BS.at[b], U1.at[b], dS),
            (BP.at[b], U2.at[b], dP),
        )[k]
        return rc(src, dst, bsend.at[k, b], brecv.at[k, b], d)

    def b_land(k, b):
        r = (
            T1.at[b, 0], T1.at[b, 1], T2.at[b, 0, hi2], T2.at[b, 1, lo2],
            T2.at[b, 0, lo2], T2.at[b, 1, hi2], U1.at[b], U2.at[b],
        )[k]
        rc(r, r, bsend.at[k, b], brecv.at[k, b], dC).wait_recv()

    def weights(p):
        mi, j = p // 2, p % 2

        @pl.loop(0, 2)
        def _(rh):
            rows = pl.ds(pl.multiple_of(rh * 1024, 1024), 1024)
            res = jnp.dot(
                LT[(mi + 1) // 2, rows, :],
                G[mi, :, j * 256 : (j + 1) * 256],
                preferred_element_type=F32,
            ).astype(BF16)
            for off in range(2):
                part = res[:, off * 128 : (off + 1) * 128]
                if (p, off) in A_PARTS:
                    PA[A_PARTS.index((p, off)), rows, :] = part
                else:
                    b = B_PARTS.index((p, off))
                    for i in range(8):
                        PB[b, i % 4, rh * 2 + i // 4] = part[i * 128 : (i + 1) * 128]

        for off in range(2):
            if (p, off) in A_PARTS:
                a_copy(AS, A_PARTS.index((p, off))).start()
        for ks in ((BX1P, BX1M), (BXIP, BXIM)):
            for off in range(2):
                if (p, off) in B_PARTS:
                    for k in ks:
                        b_copy(k, B_PARTS.index((p, off))).start()

    def plus(a, b):
        return a.astype(F32) + b.astype(F32)

    def out_cols(part, half):
        p, off = part
        return pl.ds(pl.multiple_of(half * HALF + (p % 2) * 256 + off * 128, 128), 128)

    def step_ap(a):
        a_land(AS, a)
        for xd in range(4):
            ra = pl.ds(pl.multiple_of(zp * HALF + xd * 128, 128), 128)
            rr = pl.ds(pl.multiple_of((zp % 2) * HALF + xd * 128, 128), 128)
            SPA[a, xd] = plus(PA[a, ra, :], RSA[a, rr, :]).astype(BF16)
        a_copy(AP, a).start()
        for xd in range(4):
            ra = pl.ds(pl.multiple_of(z * HALF + xd * 128, 128), 128)
            rr = pl.ds(pl.multiple_of((z % 2) * HALF + xd * 128, 128), 128)
            QA[a, xd, role] = plus(PA[a, ra, :], RSA[a, rr, :]).astype(BF16)

    def step_ax1(a):
        a_land(AP, a)
        for k in (AX1P, AX1M, AXIP, AXIM):
            a_copy(k, a).start()

    def step_ax2(a):
        a_land(AX1P, a)
        QA[a, xp, 0] = plus(QA[a, xp, 0], R1[a, 0]).astype(BF16)
        a_copy(AX2P, a).start()
        a_land(AX1M, a)
        QA[a, xm, 1] = plus(QA[a, xm, 1], R1[a, 1]).astype(BF16)
        a_copy(AX2M, a).start()

    def step_af(a):
        for k in (AXIP, AXIM, AX2P, AX2M):
            a_land(k, a)
        for h in range(2):
            gr_ref[A_PARTS[a][0] // 2, :, out_cols(A_PARTS[a], h)] = plus(
                QA[a, x, h], R2[a, 0, h]
            ) + R2[a, 1, h].astype(F32)

    def step_bx2(b):
        b_land(BX1P, b)
        for i in range(2):
            PB[b, xp, i] = plus(PB[b, xp, i], T1[b, 0, i]).astype(BF16)
        b_copy(BX2P, b).start()
        b_land(BX1M, b)
        for i in range(2):
            PB[b, xm, 2 + i] = plus(PB[b, xm, 2 + i], T1[b, 1, i]).astype(BF16)
        b_copy(BX2M, b).start()

    def step_bs(b):
        for k in (BXIP, BXIM, BX2P, BX2M):
            b_land(k, b)
        for i in range(2):
            o = 2 * (1 - pair) + i
            BS[b, i] = (plus(PB[b, x, o], T2[b, 0, o]) + T2[b, 1, o].astype(F32)).astype(BF16)
        b_copy(BSK, b).start()
        for i in range(2):
            o = 2 * pair + i
            BK[b, i] = plus(PB[b, x, o], T2[b, 0, o]) + T2[b, 1, o].astype(F32)

    def step_bp(b):
        b_land(BSK, b)
        BP[b] = plus(BK[b, zp % 2], U1[b, zp % 2]).astype(BF16)
        b_copy(BPK, b).start()
        gr_ref[B_PARTS[b][0] // 2, :, out_cols(B_PARTS[b], role)] = plus(
            BK[b, z % 2], U1[b, z % 2]
        )

    def step_bf(b):
        b_land(BPK, b)
        gr_ref[B_PARTS[b][0] // 2, :, out_cols(B_PARTS[b], 1 - role)] = U2[b].astype(F32)

    V1P, V1M, VIP, VIM, V2P, V2M, WSK = range(7)
    lo, hi = pl.ds(0, ROWS), pl.ds(ROWS, ROWS)
    y_of = (y2, yp, ym, y)

    def y_copy(k, e):
        a, b, d = (
            (EK.at[e, y2, lo], V1.at[e, 0], dYp),
            (EK.at[e, y2, hi], V1.at[e, 1], dYm),
            (EK.at[e, yp, hi], V2.at[e, 0, hi], dYp),
            (EK.at[e, ym, lo], V2.at[e, 1, lo], dYm),
            (EK.at[e, yp, lo], V2.at[e, 0, lo], dYp),
            (EK.at[e, ym, hi], V2.at[e, 1, hi], dYm),
            (WS.at[e], W1.at[e], dP),
        )[k]
        return rc(a, b, ysend.at[e, k], yrecv.at[e, k], d)

    def y_land(k, e):
        b = (
            V1.at[e, 0], V1.at[e, 1], V2.at[e, 0, hi], V2.at[e, 1, lo],
            V2.at[e, 0, lo], V2.at[e, 1, hi], W1.at[e],
        )[k]
        rc(b, b, ysend.at[e, k], yrecv.at[e, k], dC).wait_recv()

    def sib_copy(e, i):
        return rc(
            ES.at[e, y_of[i]], ER.at[e, y_of[i]], csend.at[e, i], crecv.at[e, i], dC
        )

    def nt(a, b):
        return lax.dot_general(a, b, (((1,), (1,)), ((), ())), preferred_element_type=F32)

    def y_product(e, yy, cc):
        rows = pl.ds(pl.multiple_of((yy * 2 + cc) * FEAT, FEAT), FEAT)
        if e == 0:
            v = nt(G[1], W[0, rows, :]) + nt(G[2], W[1, rows, :])
        else:
            v = nt(G[0], W[2, rows, :])
        return v.astype(BF16)

    def y_sib(e, i):
        ES[e, y_of[i]] = y_product(e, y_of[i], 1 - c)
        sib_copy(e, i).start()

    def y_own(e, i):
        EK[e, y_of[i]] = y_product(e, y_of[i], c)

    def y_merge(e, i, *sends):
        sib_copy(e, i).wait_recv()
        yy = y_of[i]

        @pl.loop(0, 6)
        def _(n):
            r = pl.ds(pl.multiple_of(n * 128, 128), 128)
            EK[e, yy, r, :] = plus(EK[e, yy, r, :], ER[e, yy, r, :]).astype(BF16)

        for k in sends:
            y_copy(k, e).start()

    def y_relay(e, d):
        y_land((V1P, V1M)[d], e)
        yy = (yp, ym)[d]

        @pl.loop(0, 3)
        def _(n):
            r = pl.ds(pl.multiple_of(d * ROWS + n * 128, 128), 128)
            rv = pl.ds(pl.multiple_of(n * 128, 128), 128)
            EK[e, yy, r, :] = plus(EK[e, yy, r, :], V1[e, d, rv, :]).astype(BF16)

        y_copy((V2P, V2M)[d], e).start()

    def y_p(e):
        y_land(VIP, e)
        y_land(V2M, e)

        @pl.loop(0, 3)
        def _(n):
            r = pl.ds(pl.multiple_of(ROWS + n * 128, 128), 128)
            rv = pl.ds(pl.multiple_of(n * 128, 128), 128)
            WS[e, rv, :] = (
                plus(EK[e, y, r, :], V2[e, 0, r, :]) + V2[e, 1, r, :].astype(F32)
            ).astype(BF16)

        y_copy(WSK, e).start()

    def y_f(e):
        y_land(VIM, e)
        y_land(V2P, e)

        @pl.loop(0, 3)
        def _(n):
            r = pl.ds(pl.multiple_of(n * 128, 128), 128)
            FS[e, r, :] = plus(EK[e, y, r, :], V2[e, 0, r, :]) + V2[e, 1, r, :].astype(F32)

    def y_block_out():
        y_land(WSK, 1)
        for b in range(NB):
            rows = slice(b * BLK, (b + 1) * BLK)
            branch = FS[1, rows, :] + W1[1, rows, :].astype(F32)
            bo_ref[rows, :] = (XT[rows, :].astype(F32) + branch).astype(BF16)

    def y_partial():
        y_land(WSK, 0)
        for b in range(NB):
            rows = slice(b * BLK, (b + 1) * BLK)
            g = FS[0, rows, :] + W1[0, rows, :].astype(F32)
            FS[0, rows, :] = g
            BSUM[b : b + 1, :] = jnp.sum(g * NRM[rows, :], axis=0, keepdims=True)
        TZ[1, z] = jnp.dot(
            onehot, BSUM[...], precision=HIGHEST, preferred_element_type=F32
        ).astype(BF16)
        tsend(1, 0)

    def y_grad_tokens():
        total = tsum(1, 1)
        gg_ref[...] = jnp.sum(total, axis=0, keepdims=True)
        BSUM[...] = jnp.dot(
            onehot_t, gain * total / GHOST, precision=HIGHEST, preferred_element_type=F32
        )
        for b in range(NB):
            rows = slice(b * BLK, (b + 1) * BLK)
            g, nb = FS[0, rows, :], NRM[rows, :]
            dyb = DYB[0, rows, own_cols].astype(F32)
            gt_ref[rows, :] = (
                dyb + SCB[b : b + 1, :] * (gain * g - nb * BSUM[b : b + 1, :])
            ).astype(BF16)

    start()
    tmid(0)
    fwd(DYB, 0, (2,), 4)
    fwd(DYB, 0, (1,), 3)
    fwd(DYB, 0, (16,), 9)
    fwd(DYB, 0, (17,), 10)
    fwd(DYB, 0, (0,), 5, 6, 12)
    stat2()
    fwd(DYB, 0, (3, 4), 7, 11)
    send_own(HB, 1)
    slot_ready(DYB, 0, 0)
    gh(0)
    transposed(DYB, 0, 0)
    fwd(DYB, 0, (6,), 14)
    fwd(DYB, 0, (5,), 13)
    fwd(DYB, 0, (7,), 15)
    fwd(HB, 1, (1,), 3)
    fwd(HB, 1, (2,), 4)
    slot_ready(DYB, 0, 1)
    transposed(DYB, 0, 1)
    gh(1)
    fwd(HB, 1, (16,), 9)
    fwd(HB, 1, (17,), 10)
    fwd(HB, 1, (0,), 5, 6, 12)
    fwd(HB, 1, (3, 4), 7, 11)
    slot_ready(HB, 1, 0)
    units(0)
    transposed(HB, 1, 0)
    fwd(HB, 1, (6,), 14)
    fwd(HB, 1, (5,), 13)
    fwd(HB, 1, (7,), 15)
    slot_ready(HB, 1, 1)
    units(1)
    weights(0)
    y_sib(0, 0)
    y_sib(1, 3)
    y_sib(0, 2)
    y_sib(1, 1)
    weights(1)
    y_own(0, 0)
    y_merge(0, 0, V1P, V1M)
    y_sib(0, 1)
    y_own(0, 1)
    y_own(1, 3)
    transposed(HB, 1, 1)
    weights(5)
    y_merge(0, 1, VIP)
    weights(2)
    step_bx2(1)
    y_own(0, 3)
    y_sib(1, 0)
    y_own(1, 0)
    y_sib(1, 2)
    y_own(0, 2)
    y_merge(0, 2, VIM)
    y_relay(0, 1)
    step_bx2(5)
    y_relay(0, 0)
    step_ap(0)
    step_bx2(0)
    y_sib(0, 3)
    weights(4)
    y_merge(1, 0, V1P, V1M)
    step_bx2(6)
    y_own(1, 2)
    y_merge(1, 2, VIM)
    y_own(1, 1)
    y_merge(1, 1, VIP)
    y_merge(0, 3)
    y_merge(1, 3)
    step_ap(1)
    weights(3)
    step_ax1(0)
    step_bx2(2)
    step_ax1(1)
    step_bs(1)
    step_ap(2)
    step_bs(5)
    y_p(0)
    y_f(0)
    step_bs(0)
    y_relay(1, 0)
    step_bx2(4)
    step_ax1(2)
    step_ap(4)
    y_relay(1, 1)
    step_bs(6)
    step_bx2(3)
    y_partial()
    step_ax2(0)
    step_ap(3)
    step_ax1(4)
    step_bs(2)
    step_bp(1)
    step_ax2(1)
    step_bp(5)
    y_p(1)
    y_f(1)
    step_bs(4)
    step_bp(0)
    step_ax2(2)
    step_ax1(3)
    step_bf(1)
    step_bp(6)
    tmid(1)
    step_bf(5)
    step_bs(3)
    step_af(0)
    step_bp(2)
    step_ax2(4)
    step_bp(4)
    step_af(1)
    step_af(2)
    step_bp(3)
    y_block_out()
    step_ax2(3)
    step_bf(0)
    step_bf(6)
    step_bf(2)
    step_af(4)
    y_grad_tokens()
    step_bf(4)
    step_af(3)
    step_bf(3)
    for g, B in ((0, DYB), (1, HB)):
        for k in range(18):
            gcopy(B, g, k).wait_send()
    for e in range(2):
        for a in range(2):
            for k in range(1, 4):
                tcopy(e, a, k).wait_send()
        for i in range(4):
            sib_copy(e, i).wait_send()
        for k in range(7):
            y_copy(k, e).wait_send()
    for k in range(8):
        for a in range(len(A_PARTS)):
            a_copy(k, a).wait_send()
        for b in range(len(B_PARTS)):
            b_copy(k, b).wait_send()


def body(tokens, norm_gain, running_sq, gate_weight, up_weight, down_weight_t, groups, cotangent):
    V = pltpu.VMEM
    any_spec = pl.BlockSpec(memory_space=pl.ANY)
    vmem_spec = pl.BlockSpec(memory_space=pltpu.VMEM)
    na, nb = len(A_PARTS), len(B_PARTS)
    sq = (128, 128)
    dma = pltpu.SemaphoreType.DMA
    scratch = [
        V((ROWS, FEAT), BF16), V((ROWS, FEAT), F32), V((NB, FEAT), F32), V((NB, FEAT), F32),
        V((2, ROWS, WIDTH), BF16), V((2, ROWS, WIDTH), BF16), V((2, WIDTH, 2 * ROWS), BF16),
        V((3, WIDTH, HALF), BF16), V((3, 2 * ROWS, HALF), BF16),
        V((ROWS, HALF), F32), V((ROWS, HALF), F32), V((2, ROWS, HALF), F32),
        V((2, 4, GROUPS, FEAT), BF16), V((2, 4, GROUPS, FEAT), BF16),
        V((na, WIDTH, 128), BF16), V((na, 1024, 128), BF16), V((na, 4, *sq), BF16),
        V((na, 4, 2, *sq), BF16), V((na, 2, *sq), BF16), V((na, 2, 2, *sq), BF16),
        V((nb, 4, 4, *sq), BF16), V((nb, 2, 2, *sq), BF16), V((nb, 2, 4, *sq), BF16),
        V((nb, 2, *sq), F32), V((nb, 2, *sq), BF16), V((nb, 2, *sq), BF16),
        V((nb, *sq), BF16), V((nb, *sq), BF16),
        V((2, 4, 2 * ROWS, FEAT), BF16), V((2, 4, 2 * ROWS, FEAT), BF16),
        V((2, 4, 2 * ROWS, FEAT), BF16), V((2, 2, ROWS, FEAT), BF16),
        V((2, 2, 2 * ROWS, FEAT), BF16), V((2, ROWS, FEAT), BF16), V((2, ROWS, FEAT), BF16),
        V((2, ROWS, FEAT), F32),
        dma((5,)), dma((2, 18)), dma((2, 18)), dma((2, 2, 4)), dma((2, 2, 4)),
        dma((8, na)), dma((8, na)), dma((8, nb)), dma((8, nb)), dma((2, 7)), dma((2, 7)),
        dma((2, 4)), dma((2, 4)),
    ]
    block_out, grad_tokens, run_new, gain_grad, grads = pl.pallas_call(
        kernel,
        out_shape=(
            jax.ShapeDtypeStruct((ROWS, FEAT), BF16),
            jax.ShapeDtypeStruct((ROWS, FEAT), BF16),
            jax.ShapeDtypeStruct((1, FEAT), F32),
            jax.ShapeDtypeStruct((1, FEAT), F32),
            jax.ShapeDtypeStruct((3, 128, 1024), F32),
        ),
        in_specs=[any_spec, vmem_spec, vmem_spec, any_spec, any_spec, any_spec, vmem_spec, any_spec],
        out_specs=(vmem_spec,) * 5,
        scratch_shapes=scratch,
        compiler_params=pltpu.CompilerParams(
            collective_id=0, has_side_effects=True, vmem_limit_bytes=67043328
        ),
    )(
        tokens, norm_gain.reshape(1, -1), running_sq.reshape(1, -1), gate_weight, up_weight,
        down_weight_t, groups.reshape(1, -1), cotangent,
    )
    return (
        block_out, grad_tokens, run_new.reshape(-1), gain_grad.reshape(-1),
        grads[1], grads[2], grads[0],
    )


def solution(mesh):
    placed = (
        P("tok", "mp"),
        P(),
        P("mp"),
        P(None, "mp"),
        P(None, "mp"),
        P(None, "mp"),
        P("tok"),
        P("tok", "mp"),
    )
    return jax.shard_map(
        body,
        mesh=mesh,
        in_specs=placed,
        out_specs=(
            P("tok", "mp"),
            P("tok", "mp"),
            P("mp"),
            P("mp"),
            P("tok", "mp"),
            P("tok", "mp"),
            P("tok", "mp"),
        ),
        check_vma=False,
    )
```

```python
import jax
import jax.numpy as jnp
from jax import lax
from jax.experimental import pallas as pl
from jax.experimental.pallas import tpu as pltpu
from jax.sharding import PartitionSpec as P

GHOST = 128
BLK = 16
ROWS = 384
FEAT = 256
WIDTH = 2048
HALF = 512
GROUPS = 48
VMEM_LIMIT = 62 << 20
NB = 24
A_PARTS = tuple((p, 0) for p in range(5))
B_PARTS = tuple((p, 1) for p in range(5)) + ((5, 0), (5, 1))

epsilon = 1e-05
momentum = 0.1
F32 = jnp.float32
BF16 = jnp.bfloat16
HIGHEST = lax.Precision.HIGHEST


def kernel(
    tok_hbm, gain_hbm, run_hbm, gw_hbm, uw_hbm, dw_hbm, grp_hbm, cot_hbm,
    bo_ref, gt_ref, rn_ref, gg_ref, gr_ref,
    GR, GN, RN, XT, NRM, BSUM, SCB, DYB, HB, LT, W, G, GT, LF, GH,
    TZ, TX, PA, RSA, SPA, QA, R1, R2, PB, T1, T2, BK, BS, U1, BP, U2,
    EK, ES, ER, V1, V2, WS, W1, FS,
    lsem, gsend, grecv, ssend, srecv, asend, arecv, bsend, brecv, ysend, yrecv, csend, crecv,
):
    t = lax.axis_index("tok")
    m = lax.axis_index("mp")
    z, x = t // 4, t % 4
    y, c = m // 2, m % 2
    zp = z + 1 - 2 * (z % 2)
    zs = 3 - z
    role = ((z + 1) // 2) % 2
    yp, ym, y2 = (y + 1) % 4, (y + 3) % 4, (y + 2) % 4
    xp, xm, x2 = (x + 1) % 4, (x + 3) % 4, (x + 2) % 4
    dC = (t, y * 2 + 1 - c)
    dP = (zp * 4 + x, m)
    dS = (zs * 4 + x, m)
    dYp, dYm = (t, yp * 2 + c), (t, ym * 2 + c)
    dXp, dXm = (z * 4 + xp, m), (z * 4 + xm, m)

    def rc(src, dst, ss, rs, dev):
        return pltpu.make_async_remote_copy(
            src_ref=src, dst_ref=dst, send_sem=ss, recv_sem=rs,
            device_id=dev, device_id_type=pl.DeviceIdType.MESH,
        )

    own_cols = pl.ds(pl.multiple_of(m * FEAT, FEAT), FEAT)

    bar = pltpu.get_barrier_semaphore()
    z_others = [(((z + k) % 4) * 4 + x, m) for k in range(1, 4)]
    x_others = [(z * 4 + (x + k) % 4, m) for k in range(1, 4)]
    for d in (*z_others, *x_others, dC, dYp, dYm):
        pl.semaphore_signal(bar, inc=1, device_id=d, device_id_type=pl.DeviceIdType.MESH)

    cp_dy = pltpu.make_async_copy(cot_hbm, DYB.at[0, :, own_cols], lsem.at[0])
    cp_dy.start()
    cp_x = pltpu.make_async_copy(tok_hbm, XT, lsem.at[1])
    cp_x.start()
    small = [
        pltpu.make_async_copy(a, b, lsem.at[5 + i])
        for i, (a, b) in enumerate(
            ((grp_hbm, GR), (gain_hbm.at[:, own_cols], GN), (run_hbm, RN))
        )
    ]
    for d in small:
        d.start()
    wcols = pl.ds(pl.multiple_of(role * HALF, HALF), HALF)
    cp_w = [
        pltpu.make_async_copy(h.at[:, wcols], W.at[i], lsem.at[2 + i])
        for i, h in enumerate((gw_hbm, uw_hbm, dw_hbm))
    ]
    for k in (2, 0, 1):
        cp_w[k].start()

    def sl(B, slot, yy, cc, r0=0, n=ROWS):
        return B.at[slot, pl.ds(r0, n), pl.ds(pl.multiple_of((yy * 2 + cc) * FEAT, FEAT), FEAT)]

    def gcopy(B, g, k):
        h = ROWS // 2
        if k in (0, 18):
            r = 0 if k == 0 else h
            a, b, d = sl(B, 0, y, c, r, h), sl(B, 1, y, c, r, h), dP
        elif k in (1, 16):
            a = b = sl(B, 0, y, c, 0 if k == 1 else h, h)
            d = dYp
        elif k in (2, 17):
            a = b = sl(B, 0, y, c, h if k == 2 else 0, h)
            d = dYm
        elif k == 3:
            a = b = sl(B, 0, ym, c, 0, h)
            d = dYp
        elif k == 4:
            a = b = sl(B, 0, yp, c, h, h)
            d = dYm
        elif k in (5, 6, 19, 20):
            a = b = sl(B, 1, y, c, 0 if k < 7 else h, h)
            d = dYp if k in (5, 19) else dYm
        elif k == 7:
            a, b, d = sl(B, 0, y2, c), sl(B, 1, y2, c), dP
        else:
            slot = (k - 8) // 4
            yy = (y, ym, yp, y2)[(k - 8) % 4]
            a = b = sl(B, slot, yy, c)
            d = dC
        return rc(a, b, gsend.at[g, k], grecv.at[g, k], d)

    def gland(B, g, k):
        h = ROWS // 2
        if k in (0, 18):
            b = sl(B, 1, y, c, 0 if k == 0 else h, h)
        elif k in (1, 16):
            b = sl(B, 0, ym, c, 0 if k == 1 else h, h)
        elif k in (2, 17):
            b = sl(B, 0, yp, c, h if k == 2 else 0, h)
        elif k == 3:
            b = sl(B, 0, y2, c, 0, h)
        elif k == 4:
            b = sl(B, 0, y2, c, h, h)
        elif k in (5, 6, 19, 20):
            b = sl(B, 1, ym if k in (5, 19) else yp, c, 0 if k < 7 else h, h)
        elif k == 7:
            b = sl(B, 1, y2, c)
        else:
            b = sl(B, (k - 8) // 4, (y, ym, yp, y2)[(k - 8) % 4], 1 - c)
        rc(b, b, gsend.at[g, k], grecv.at[g, k], dC).wait_recv()

    def gstart(B, g, *ks):
        for k in ks:
            gcopy(B, g, k).start()

    def fwd(B, g, land, *sends):
        for k in land:
            gland(B, g, k)
        gstart(B, g, *sends)

    def tcopy(e, a, k):
        buf, me, d = ((TZ, z, z_others), (TX, x, x_others))[a]
        ref = buf.at[e, me]
        return rc(ref, ref, ssend.at[e, a, k], srecv.at[e, a, k], d[k - 1])

    def tsum(e, a):
        buf, me = ((TZ, z), (TX, x))[a]
        for k in range(1, 4):
            ref = buf.at[e, (me + 4 - k) % 4]
            rc(ref, ref, ssend.at[e, a, k], srecv.at[e, a, k], dC).wait_recv()
        return (buf[e, 0].astype(F32) + buf[e, 1].astype(F32)) + (
            buf[e, 2].astype(F32) + buf[e, 3].astype(F32)
        )

    def tsend(e, a):
        for k in range(1, 4):
            tcopy(e, a, k).start()

    def tmid(e):
        TX[e, x] = tsum(e, 0).astype(BF16)
        tsend(e, 1)

    def onehots():
        grow = GR[...]
        rows = lax.broadcasted_iota(jnp.int32, (GROUPS, NB), 0)
        onehot = (rows == jnp.broadcast_to(grow, (GROUPS, NB))).astype(F32)
        diag = lax.broadcasted_iota(jnp.int32, (NB, NB), 0) == lax.broadcasted_iota(
            jnp.int32, (NB, NB), 1
        )
        gcol = jnp.sum(
            jnp.where(diag, jnp.broadcast_to(grow, (NB, NB)), 0).astype(F32),
            axis=1, keepdims=True,
        )
        onehot_t = (
            lax.broadcasted_iota(jnp.int32, (NB, GROUPS), 1).astype(F32)
            == jnp.broadcast_to(gcol, (NB, GROUPS))
        ).astype(F32)
        return onehot, onehot_t

    def start():
        cp_dy.wait()
        pl.semaphore_wait(bar, 9)
        gstart(DYB, 0, 1, 2, 0, 16, 17, 8)

    def stat0():
        cp_x.wait()
        for d in small:
            d.wait()
        for b in range(NB):
            xb = XT[b * BLK : (b + 1) * BLK, :].astype(F32)
            BSUM[b : b + 1, :] = jnp.sum(xb * xb, axis=0, keepdims=True)
        TZ[0, z] = jnp.dot(
            onehots()[0], BSUM[...], precision=HIGHEST, preferred_element_type=F32
        ).astype(BF16)
        tsend(0, 0)
        gstart(DYB, 0, 18)

    def stat2():
        quad = tsum(0, 1) / GHOST
        rn_ref[...] = (1.0 - momentum) * RN[...] + momentum * (
            jnp.sum(quad, axis=0, keepdims=True) / GROUPS
        )
        gain = GN[...]
        SCB[...] = jnp.dot(
            onehots()[1], lax.rsqrt(quad + epsilon), precision=HIGHEST, preferred_element_type=F32
        )
        for b in range(NB):
            rows = slice(b * BLK, (b + 1) * BLK)
            nb = XT[rows, :].astype(F32) * SCB[b : b + 1, :]
            NRM[rows, :] = nb
            HB[0, rows, own_cols] = (gain * nb).astype(BF16)
        gstart(HB, 1, 1, 2, 0, 18, 16, 17, 8)

    def transposed(B, i, slot):
        @pl.loop(0, 8)
        def _(j):
            cols = pl.ds(pl.multiple_of(j * FEAT, FEAT), FEAT)
            LT[i, cols, pl.ds(slot * ROWS, ROWS)] = B[slot, :, cols].T

    def k_part(wi, slot, yy):
        ks = pl.ds(pl.multiple_of(yy * 2 * FEAT, 2 * FEAT), 2 * FEAT)
        return jnp.dot(HB[slot, :, ks], W[wi, ks, :], preferred_element_type=F32)

    def units_a(slot):
        if slot == 0:
            cp_w[0].wait()
            cp_w[1].wait()
        for wi, dst in ((0, GT), (1, LF)):
            dst[slot] = k_part(wi, slot, y) + k_part(wi, slot, ym) + k_part(wi, slot, yp)

    def units_b(slot):
        GT[slot] += k_part(0, slot, y2)
        LF[slot] += k_part(1, slot, y2)

        @pl.loop(0, ROWS // 32)
        def _(i):
            r = pl.ds(pl.multiple_of(i * 32, 32), 32)
            ro = pl.ds(pl.multiple_of(slot * ROWS + i * 32, 32), 32)
            gate, lift, gh = GT[slot, r, :], LF[slot, r, :], GH[slot, r, :]
            sigma = jax.nn.sigmoid(gate)
            G[0, ro, :] = (gate * sigma * lift).astype(BF16)
            G[1, ro, :] = (gh * lift * sigma * (1.0 + gate * (1.0 - sigma))).astype(BF16)
            G[2, ro, :] = (gh * gate * sigma).astype(BF16)

    def gh(slot):
        if slot == 0:
            cp_w[2].wait()
        GH[slot] = jnp.dot(DYB[slot], W[2], preferred_element_type=F32)

    def ready(B, g, *ks):
        for k in ks:
            gland(B, g, k)

    AS, AP, AX1P, AX1M, AXIP, AXIM, AX2P, AX2M = range(8)
    BX1P, BX1M, BXIP, BXIM, BX2P, BX2M, BSK, BPK = range(8)
    pair = z // 2
    lo2, hi2 = pl.ds(0, 2), pl.ds(2, 2)

    def a_copy(k, a):
        far = pl.ds(pl.multiple_of((1 - pair) * 1024, 1024), 1024)
        src, dst, d = (
            (PA.at[a, far], RSA.at[a], dS),
            (SPA.at[a], QA.at[a, :, role], dP),
            (QA.at[a, x2, 0], R1.at[a, 0], dXp),
            (QA.at[a, x2, 1], R1.at[a, 1], dXm),
            (QA.at[a, xp, 1], R2.at[a, 0, 1], dXp),
            (QA.at[a, xm, 0], R2.at[a, 1, 0], dXm),
            (QA.at[a, xp, 0], R2.at[a, 0, 0], dXp),
            (QA.at[a, xm, 1], R2.at[a, 1, 1], dXm),
        )[k]
        return rc(src, dst, asend.at[k, a], arecv.at[k, a], d)

    def a_land(k, a):
        b = (
            RSA.at[a], QA.at[a, :, 1 - role], R1.at[a, 0], R1.at[a, 1],
            R2.at[a, 0, 1], R2.at[a, 1, 0], R2.at[a, 0, 0], R2.at[a, 1, 1],
        )[k]
        rc(b, b, asend.at[k, a], arecv.at[k, a], dC).wait_recv()

    def b_copy(k, b):
        src, dst, d = (
            (PB.at[b, x2, lo2], T1.at[b, 0], dXp),
            (PB.at[b, x2, hi2], T1.at[b, 1], dXm),
            (PB.at[b, xp, hi2], T2.at[b, 0, hi2], dXp),
            (PB.at[b, xm, lo2], T2.at[b, 1, lo2], dXm),
            (PB.at[b, xp, lo2], T2.at[b, 0, lo2], dXp),
            (PB.at[b, xm, hi2], T2.at[b, 1, hi2], dXm),
            (BS.at[b], U1.at[b], dS),
            (BP.at[b], U2.at[b], dP),
        )[k]
        return rc(src, dst, bsend.at[k, b], brecv.at[k, b], d)

    def b_land(k, b):
        r = (
            T1.at[b, 0], T1.at[b, 1], T2.at[b, 0, hi2], T2.at[b, 1, lo2],
            T2.at[b, 0, lo2], T2.at[b, 1, hi2], U1.at[b], U2.at[b],
        )[k]
        rc(r, r, bsend.at[k, b], brecv.at[k, b], dC).wait_recv()

    def weights(p):
        mi, j = p // 2, p % 2

        @pl.loop(0, 2)
        def _(n):
            rh = (1 - pair + n) % 2
            rows = pl.ds(pl.multiple_of(rh * 1024, 1024), 1024)
            res = jnp.dot(
                LT[(mi + 1) // 2, rows, :],
                G[mi, :, j * 256 : (j + 1) * 256],
                preferred_element_type=F32,
            ).astype(BF16)
            for off in range(2):
                part = res[:, off * 128 : (off + 1) * 128]
                if (p, off) in A_PARTS:
                    PA[A_PARTS.index((p, off)), rows, :] = part
                else:
                    b = B_PARTS.index((p, off))
                    for i in range(8):
                        PB[b, i % 4, rh * 2 + i // 4] = part[i * 128 : (i + 1) * 128]

            @pl.when(n == 0)
            def _():
                for off in range(2):
                    if (p, off) in A_PARTS:
                        a_copy(AS, A_PARTS.index((p, off))).start()

        for ks in ((BX1P, BX1M), (BXIP, BXIM)):
            for off in range(2):
                if (p, off) in B_PARTS:
                    for k in ks:
                        b_copy(k, B_PARTS.index((p, off))).start()

    def plus(a, b):
        return a.astype(F32) + b.astype(F32)

    def out_cols(part, half):
        p, off = part
        return pl.ds(pl.multiple_of(half * HALF + (p % 2) * 256 + off * 128, 128), 128)

    def step_ap(a):
        a_land(AS, a)
        for xd in range(4):
            ra = pl.ds(pl.multiple_of(zp * HALF + xd * 128, 128), 128)
            rr = pl.ds(pl.multiple_of((zp % 2) * HALF + xd * 128, 128), 128)
            SPA[a, xd] = plus(PA[a, ra, :], RSA[a, rr, :]).astype(BF16)
        a_copy(AP, a).start()
        for xd in range(4):
            ra = pl.ds(pl.multiple_of(z * HALF + xd * 128, 128), 128)
            rr = pl.ds(pl.multiple_of((z % 2) * HALF + xd * 128, 128), 128)
            QA[a, xd, role] = plus(PA[a, ra, :], RSA[a, rr, :]).astype(BF16)

    def step_ax1(a):
        a_land(AP, a)
        for k in (AX1P, AX1M, AXIP, AXIM):
            a_copy(k, a).start()

    def step_ax2(a):
        a_land(AX1P, a)
        QA[a, xp, 0] = plus(QA[a, xp, 0], R1[a, 0]).astype(BF16)
        a_copy(AX2P, a).start()
        a_land(AX1M, a)
        QA[a, xm, 1] = plus(QA[a, xm, 1], R1[a, 1]).astype(BF16)
        a_copy(AX2M, a).start()

    def step_af(a):
        for k in (AXIP, AXIM, AX2P, AX2M):
            a_land(k, a)
        for h in range(2):
            gr_ref[A_PARTS[a][0] // 2, :, out_cols(A_PARTS[a], h)] = plus(
                QA[a, x, h], R2[a, 0, h]
            ) + R2[a, 1, h].astype(F32)

    def step_bx2(b):
        b_land(BX1P, b)
        for i in range(2):
            PB[b, xp, i] = plus(PB[b, xp, i], T1[b, 0, i]).astype(BF16)
        b_copy(BX2P, b).start()
        b_land(BX1M, b)
        for i in range(2):
            PB[b, xm, 2 + i] = plus(PB[b, xm, 2 + i], T1[b, 1, i]).astype(BF16)
        b_copy(BX2M, b).start()

    def step_bs(b):
        for k in (BXIP, BXIM, BX2P, BX2M):
            b_land(k, b)
        for i in range(2):
            o = 2 * (1 - pair) + i
            BS[b, i] = (plus(PB[b, x, o], T2[b, 0, o]) + T2[b, 1, o].astype(F32)).astype(BF16)
        b_copy(BSK, b).start()
        for i in range(2):
            o = 2 * pair + i
            BK[b, i] = plus(PB[b, x, o], T2[b, 0, o]) + T2[b, 1, o].astype(F32)

    def step_bp(b):
        b_land(BSK, b)
        BP[b] = plus(BK[b, zp % 2], U1[b, zp % 2]).astype(BF16)
        b_copy(BPK, b).start()
        gr_ref[B_PARTS[b][0] // 2, :, out_cols(B_PARTS[b], role)] = plus(
            BK[b, z % 2], U1[b, z % 2]
        )

    def step_bf(b):
        b_land(BPK, b)
        gr_ref[B_PARTS[b][0] // 2, :, out_cols(B_PARTS[b], 1 - role)] = U2[b].astype(F32)

    V1P, V1M, VIP, VIM, V2P, V2M, WSK = range(7)
    lo, hi = pl.ds(0, ROWS), pl.ds(ROWS, ROWS)
    y_of = (y2, yp, ym, y)

    def y_copy(k, e):
        a, b, d = (
            (EK.at[e, y2, lo], V1.at[e, 0], dYp),
            (EK.at[e, y2, hi], V1.at[e, 1], dYm),
            (EK.at[e, yp, hi], V2.at[e, 0, hi], dYp),
            (EK.at[e, ym, lo], V2.at[e, 1, lo], dYm),
            (EK.at[e, yp, lo], V2.at[e, 0, lo], dYp),
            (EK.at[e, ym, hi], V2.at[e, 1, hi], dYm),
            (WS.at[e], W1.at[e], dP),
        )[k]
        return rc(a, b, ysend.at[e, k], yrecv.at[e, k], d)

    def y_land(k, e):
        b = (
            V1.at[e, 0], V1.at[e, 1], V2.at[e, 0, hi], V2.at[e, 1, lo],
            V2.at[e, 0, lo], V2.at[e, 1, hi], W1.at[e],
        )[k]
        rc(b, b, ysend.at[e, k], yrecv.at[e, k], dC).wait_recv()

    def sib_copy(e, i):
        return rc(
            ES.at[e, y_of[i]], ER.at[e, y_of[i]], csend.at[e, i], crecv.at[e, i], dC
        )

    def nt(a, b):
        return lax.dot_general(a, b, (((1,), (1,)), ((), ())), preferred_element_type=F32)

    def y_product(e, yy, cc):
        rows = pl.ds(pl.multiple_of((yy * 2 + cc) * FEAT, FEAT), FEAT)
        if e == 0:
            v = nt(G[1], W[0, rows, :]) + nt(G[2], W[1, rows, :])
        else:
            v = nt(G[0], W[2, rows, :])
        return v.astype(BF16)

    def y_sib(e, i):
        ES[e, y_of[i]] = y_product(e, y_of[i], 1 - c)
        sib_copy(e, i).start()

    def y_own(e, i):
        EK[e, y_of[i]] = y_product(e, y_of[i], c)

    def y_merge(e, i, *sends):
        sib_copy(e, i).wait_recv()
        yy = y_of[i]

        @pl.loop(0, 6)
        def _(n):
            r = pl.ds(pl.multiple_of(n * 128, 128), 128)
            EK[e, yy, r, :] = plus(EK[e, yy, r, :], ER[e, yy, r, :]).astype(BF16)

        for k in sends:
            y_copy(k, e).start()

    def y_relay(e, d):
        y_land((V1P, V1M)[d], e)
        yy = (yp, ym)[d]

        @pl.loop(0, 3)
        def _(n):
            r = pl.ds(pl.multiple_of(d * ROWS + n * 128, 128), 128)
            rv = pl.ds(pl.multiple_of(n * 128, 128), 128)
            EK[e, yy, r, :] = plus(EK[e, yy, r, :], V1[e, d, rv, :]).astype(BF16)

        y_copy((V2P, V2M)[d], e).start()

    def y_p(e):
        y_land(VIP, e)
        y_land(V2M, e)

        @pl.loop(0, 3)
        def _(n):
            r = pl.ds(pl.multiple_of(ROWS + n * 128, 128), 128)
            rv = pl.ds(pl.multiple_of(n * 128, 128), 128)
            WS[e, rv, :] = (
                plus(EK[e, y, r, :], V2[e, 0, r, :]) + V2[e, 1, r, :].astype(F32)
            ).astype(BF16)

        y_copy(WSK, e).start()

    def y_f(e):
        y_land(VIM, e)
        y_land(V2P, e)

        @pl.loop(0, 3)
        def _(n):
            r = pl.ds(pl.multiple_of(n * 128, 128), 128)
            FS[e, r, :] = plus(EK[e, y, r, :], V2[e, 0, r, :]) + V2[e, 1, r, :].astype(F32)

    def y_block_out():
        y_land(WSK, 1)
        for b in range(NB):
            rows = slice(b * BLK, (b + 1) * BLK)
            branch = FS[1, rows, :] + W1[1, rows, :].astype(F32)
            bo_ref[rows, :] = (XT[rows, :].astype(F32) + branch).astype(BF16)

    def y_partial():
        y_land(WSK, 0)
        for b in range(NB):
            rows = slice(b * BLK, (b + 1) * BLK)
            g = FS[0, rows, :] + W1[0, rows, :].astype(F32)
            FS[0, rows, :] = g
            BSUM[b : b + 1, :] = jnp.sum(g * NRM[rows, :], axis=0, keepdims=True)
        TZ[1, z] = jnp.dot(
            onehots()[0], BSUM[...], precision=HIGHEST, preferred_element_type=F32
        ).astype(BF16)
        tsend(1, 0)

    def y_grad_tokens():
        total = tsum(1, 1)
        gg_ref[...] = jnp.sum(total, axis=0, keepdims=True)
        gain = GN[...]
        BSUM[...] = jnp.dot(
            onehots()[1], gain * total / GHOST, precision=HIGHEST, preferred_element_type=F32
        )
        for b in range(NB):
            rows = slice(b * BLK, (b + 1) * BLK)
            g, nb = FS[0, rows, :], NRM[rows, :]
            dyb = DYB[0, rows, own_cols].astype(F32)
            gt_ref[rows, :] = (
                dyb + SCB[b : b + 1, :] * (gain * g - nb * BSUM[b : b + 1, :])
            ).astype(BF16)

    start()
    stat0()
    fwd(DYB, 0, (2,), 4)
    fwd(DYB, 0, (1,), 3)
    fwd(DYB, 0, (0,), 5, 6)
    tmid(0)
    fwd(DYB, 0, (16,), 9)
    fwd(DYB, 0, (17,), 10)
    fwd(DYB, 0, (18,), 19, 20, 12)
    fwd(DYB, 0, (3, 4), 7, 11)
    stat2()
    ready(DYB, 0, 8, 9, 10)
    ready(DYB, 0, 11)
    transposed(DYB, 0, 0)
    gh(0)
    fwd(DYB, 0, (6, 20), 14)
    fwd(DYB, 0, (5, 19), 13)
    fwd(DYB, 0, (7,), 15)
    fwd(HB, 1, (2,), 4)
    fwd(HB, 1, (1,), 3)
    ready(DYB, 0, 12, 13, 14)
    ready(DYB, 0, 15)
    gh(1)
    fwd(HB, 1, (0,), 5, 6)
    fwd(HB, 1, (16,), 9)
    transposed(DYB, 0, 1)
    fwd(HB, 1, (17,), 10)
    fwd(HB, 1, (18,), 19, 20, 12)
    fwd(HB, 1, (3, 4), 7, 11)
    ready(HB, 1, 8, 9, 10)
    units_a(0)
    ready(HB, 1, 11)
    transposed(HB, 1, 0)
    units_b(0)
    fwd(HB, 1, (5, 19), 13)
    fwd(HB, 1, (6, 20), 14)
    fwd(HB, 1, (7,), 15)
    ready(HB, 1, 12, 13, 14)
    units_a(1)
    ready(HB, 1, 15)
    units_b(1)
    weights(0)
    y_own(1, 2)
    y_sib(0, 0)
    weights(1)
    y_own(0, 0)
    step_bx2(0)
    y_merge(0, 0, V1P, V1M)
    transposed(HB, 1, 1)
    y_sib(1, 1)
    weights(4)
    y_sib(0, 2)
    weights(3)
    step_ap(0)
    y_sib(0, 1)
    y_own(0, 2)
    y_merge(0, 2, VIM)
    y_relay(0, 1)
    step_bx2(4)
    y_own(0, 1)
    y_merge(0, 1, VIP)
    y_relay(0, 0)
    weights(2)
    step_bx2(3)
    step_ap(1)
    y_sib(1, 0)
    step_bs(0)
    y_own(1, 0)
    y_sib(1, 3)
    y_sib(0, 3)
    step_bs(4)
    step_bx2(1)
    y_own(1, 3)
    y_sib(1, 2)
    step_bx2(2)
    y_merge(1, 0, V1P, V1M)
    weights(5)
    step_ap(4)
    step_ax1(1)
    step_ax1(0)
    y_own(1, 1)
    y_merge(1, 1, VIP)
    y_merge(1, 2, VIM)
    y_own(0, 3)
    y_merge(0, 3)
    step_bs(3)
    y_merge(1, 3)
    y_p(0)
    step_bs(1)
    y_f(0)
    step_bs(2)
    step_ax1(4)
    step_bx2(5)
    step_ap(3)
    y_relay(1, 1)
    step_bx2(6)
    y_relay(1, 0)
    y_partial()
    step_ax2(1)
    step_ap(2)
    step_ax2(0)
    step_ax1(3)
    step_bp(0)
    step_ax2(4)
    step_bp(4)
    y_p(1)
    step_bs(5)
    step_bp(3)
    step_ax1(2)
    y_f(1)
    step_bs(6)
    step_bf(0)
    step_bp(1)
    step_af(1)
    step_bf(4)
    step_af(0)
    step_bp(2)
    step_ax2(3)
    tmid(1)
    step_af(4)
    step_bp(5)
    step_ax2(2)
    step_bp(6)
    y_block_out()
    step_af(3)
    step_bf(3)
    step_bf(1)
    step_bf(2)
    step_af(2)
    y_grad_tokens()
    step_bf(5)
    step_bf(6)
    for g, B in ((0, DYB), (1, HB)):
        for k in range(21):
            gcopy(B, g, k).wait_send()
    for e in range(2):
        for a in range(2):
            for k in range(1, 4):
                tcopy(e, a, k).wait_send()
        for i in range(4):
            sib_copy(e, i).wait_send()
        for k in range(7):
            y_copy(k, e).wait_send()
    for k in range(8):
        for a in range(len(A_PARTS)):
            a_copy(k, a).wait_send()
        for b in range(len(B_PARTS)):
            b_copy(k, b).wait_send()


def emit(bo_ref, gt_ref, rn_ref, gg_ref, gr_ref, bo, gt, rn, gg, g_gate, g_up, g_down, sem):
    copies = [
        pltpu.make_async_copy(a, b, sem.at[i])
        for i, (a, b) in enumerate((
            (gr_ref.at[1], g_gate), (gr_ref.at[2], g_up), (gr_ref.at[0], g_down),
            (bo_ref, bo), (gt_ref, gt), (rn_ref, rn), (gg_ref, gg),
        ))
    ]
    for d in copies:
        d.start()
    for d in copies:
        d.wait()


def body(tokens, norm_gain, running_sq, gate_weight, up_weight, down_weight_t, groups, cotangent):
    V = pltpu.VMEM
    any_spec = pl.BlockSpec(memory_space=pl.ANY)
    vmem_spec = pl.BlockSpec(memory_space=pltpu.VMEM)
    na, nb = len(A_PARTS), len(B_PARTS)
    sq = (128, 128)
    dma = pltpu.SemaphoreType.DMA
    scratch = [
        V((1, NB), jnp.int32), V((1, FEAT), F32), V((1, FEAT), F32),
        V((ROWS, FEAT), BF16), V((ROWS, FEAT), F32), V((NB, FEAT), F32), V((NB, FEAT), F32),
        V((2, ROWS, WIDTH), BF16), V((2, ROWS, WIDTH), BF16), V((2, WIDTH, 2 * ROWS), BF16),
        V((3, WIDTH, HALF), BF16), V((3, 2 * ROWS, HALF), BF16),
        V((2, ROWS, HALF), F32), V((2, ROWS, HALF), F32), V((2, ROWS, HALF), F32),
        V((2, 4, GROUPS, FEAT), BF16), V((2, 4, GROUPS, FEAT), BF16),
        V((na, WIDTH, 128), BF16), V((na, 1024, 128), BF16), V((na, 4, *sq), BF16),
        V((na, 4, 2, *sq), BF16), V((na, 2, *sq), BF16), V((na, 2, 2, *sq), BF16),
        V((nb, 4, 4, *sq), BF16), V((nb, 2, 2, *sq), BF16), V((nb, 2, 4, *sq), BF16),
        V((nb, 2, *sq), F32), V((nb, 2, *sq), BF16), V((nb, 2, *sq), BF16),
        V((nb, *sq), BF16), V((nb, *sq), BF16),
        V((2, 4, 2 * ROWS, FEAT), BF16), V((2, 4, 2 * ROWS, FEAT), BF16),
        V((2, 4, 2 * ROWS, FEAT), BF16), V((2, 2, ROWS, FEAT), BF16),
        V((2, 2, 2 * ROWS, FEAT), BF16), V((2, ROWS, FEAT), BF16), V((2, ROWS, FEAT), BF16),
        V((2, ROWS, FEAT), F32),
        dma((8,)), dma((2, 21)), dma((2, 21)), dma((2, 2, 4)), dma((2, 2, 4)),
        dma((8, na)), dma((8, na)), dma((8, nb)), dma((8, nb)), dma((2, 7)), dma((2, 7)),
        dma((2, 4)), dma((2, 4)),
    ]
    held = (
        ((ROWS, FEAT), BF16), ((ROWS, FEAT), BF16), ((1, FEAT), F32), ((1, FEAT), F32),
        ((3, 128, 1024), F32),
    )
    results = pl.pallas_call(
        kernel,
        out_shape=tuple(pltpu.VMEM(shape, dtype) for shape, dtype in held),
        in_specs=[any_spec] * 8,
        out_specs=(vmem_spec,) * 5,
        scratch_shapes=scratch,
        compiler_params=pltpu.CompilerParams(
            collective_id=0, has_side_effects=True, vmem_limit_bytes=VMEM_LIMIT
        ),
    )(
        tokens, norm_gain.reshape(1, -1), running_sq.reshape(1, -1), gate_weight, up_weight,
        down_weight_t, groups.reshape(1, -1), cotangent,
    )
    weight = jax.ShapeDtypeStruct((128, 1024), F32)
    block_out, grad_tokens, run_new, gain_grad, g_gate, g_up, g_down = pl.pallas_call(
        emit,
        out_shape=tuple(jax.ShapeDtypeStruct(*a) for a in held[:4]) + (weight,) * 3,
        in_specs=[vmem_spec] * 5,
        out_specs=(any_spec,) * 7,
        scratch_shapes=[dma((7,))],
        compiler_params=pltpu.CompilerParams(vmem_limit_bytes=4 << 20),
    )(*results)
    return (
        block_out, grad_tokens, run_new.reshape(-1), gain_grad.reshape(-1), g_gate, g_up, g_down,
    )


def solution(mesh):
    placed = (
        P("tok", "mp"),
        P(),
        P("mp"),
        P(None, "mp"),
        P(None, "mp"),
        P(None, "mp"),
        P("tok"),
        P("tok", "mp"),
    )
    return jax.shard_map(
        body,
        mesh=mesh,
        in_specs=placed,
        out_specs=(
            P("tok", "mp"),
            P("tok", "mp"),
            P("mp"),
            P("mp"),
            P("tok", "mp"),
            P("tok", "mp"),
            P("tok", "mp"),
        ),
        check_vma=False,
    )
```

```python
import jax
import jax.numpy as jnp
from jax import lax
from jax.experimental import pallas as pl
from jax.experimental.pallas import tpu as pltpu
from jax.sharding import PartitionSpec as P

GHOST = 128
BLK = 16
ROWS = 384
FEAT = 256
WIDTH = 2048
HALF = 512
GROUPS = 48
G_SEM = (0, 1, 2, 3, 3, 4, 5, 6, 7, 8, 9, 10, 11, 12, 13, 14, 15, 16, 17, 4, 5)
VMEM_LIMIT = 62 << 20
NB = 24
A_PARTS = tuple((p, 0) for p in range(5))
B_PARTS = tuple((p, 1) for p in range(5)) + ((5, 0), (5, 1))

epsilon = 1e-05
momentum = 0.1
F32 = jnp.float32
BF16 = jnp.bfloat16
HIGHEST = lax.Precision.HIGHEST


def kernel(
    tok_hbm, gain_hbm, run_hbm, gw_hbm, uw_hbm, dw_hbm, grp_hbm, cot_hbm,
    bo_ref, gt_ref, rn_ref, gg_ref, gr_ref,
    GR, GN, RN, XT, NRM, BSUM, SCB, DYB, HB, LT, W, G, GT, LF, GH,
    TZ, TX, PA, RSA, SPA, QA, R1, R2, PB, T1, T2, BK, BS, U1, BP, U2,
    EK, ES, ER, V1, V2, WS, W1, FS,
    lsem, gsend, grecv, ssend, srecv, asend, arecv, bsend, brecv, ysend, yrecv, csend, crecv,
):
    t = lax.axis_index("tok")
    m = lax.axis_index("mp")
    z, x = t // 4, t % 4
    y, c = m // 2, m % 2
    zp = z + 1 - 2 * (z % 2)
    zs = 3 - z
    role = ((z + 1) // 2) % 2
    yp, ym, y2 = (y + 1) % 4, (y + 3) % 4, (y + 2) % 4
    xp, xm, x2 = (x + 1) % 4, (x + 3) % 4, (x + 2) % 4
    dC = (t, y * 2 + 1 - c)
    dP = (zp * 4 + x, m)
    dS = (zs * 4 + x, m)
    dYp, dYm = (t, yp * 2 + c), (t, ym * 2 + c)
    dXp, dXm = (z * 4 + xp, m), (z * 4 + xm, m)

    def rc(src, dst, ss, rs, dev):
        return pltpu.make_async_remote_copy(
            src_ref=src, dst_ref=dst, send_sem=ss, recv_sem=rs,
            device_id=dev, device_id_type=pl.DeviceIdType.MESH,
        )

    own_cols = pl.ds(pl.multiple_of(m * FEAT, FEAT), FEAT)

    bar = pltpu.get_barrier_semaphore()
    z_others = [(((z + k) % 4) * 4 + x, m) for k in range(1, 4)]
    x_others = [(z * 4 + (x + k) % 4, m) for k in range(1, 4)]
    for d in (*z_others, *x_others, dC, dYp, dYm):
        pl.semaphore_signal(bar, inc=1, device_id=d, device_id_type=pl.DeviceIdType.MESH)

    cp_dy = pltpu.make_async_copy(cot_hbm, DYB.at[0, :, own_cols], lsem.at[0])
    cp_dy.start()
    cp_x = pltpu.make_async_copy(tok_hbm, XT, lsem.at[1])
    cp_x.start()
    small = [
        pltpu.make_async_copy(a, b, lsem.at[5 + i])
        for i, (a, b) in enumerate(
            ((grp_hbm, GR), (gain_hbm.at[:, own_cols], GN), (run_hbm, RN))
        )
    ]
    for d in small:
        d.start()
    wcols = pl.ds(pl.multiple_of(role * HALF, HALF), HALF)
    cp_w = [
        pltpu.make_async_copy(h.at[:, wcols], W.at[i], lsem.at[2 + i])
        for i, h in enumerate((gw_hbm, uw_hbm, dw_hbm))
    ]
    for k in (2, 0, 1):
        cp_w[k].start()

    def sl(B, slot, yy, cc, r0=0, n=ROWS):
        return B.at[slot, pl.ds(r0, n), pl.ds(pl.multiple_of((yy * 2 + cc) * FEAT, FEAT), FEAT)]

    def gcopy(B, g, k):
        h = ROWS // 2
        if k in (0, 18):
            r = 0 if k == 0 else h
            a, b, d = sl(B, 0, y, c, r, h), sl(B, 1, y, c, r, h), dP
        elif k in (1, 16):
            a = b = sl(B, 0, y, c, 0 if k == 1 else h, h)
            d = dYp
        elif k in (2, 17):
            a = b = sl(B, 0, y, c, h if k == 2 else 0, h)
            d = dYm
        elif k == 3:
            a = b = sl(B, 0, ym, c, 0, h)
            d = dYp
        elif k == 4:
            a = b = sl(B, 0, yp, c, h, h)
            d = dYm
        elif k in (5, 6, 19, 20):
            a = b = sl(B, 1, y, c, 0 if k < 7 else h, h)
            d = dYp if k in (5, 19) else dYm
        elif k == 7:
            a, b, d = sl(B, 0, y2, c), sl(B, 1, y2, c), dP
        else:
            slot = (k - 8) // 4
            yy = (y, ym, yp, y2)[(k - 8) % 4]
            a = b = sl(B, slot, yy, c)
            d = dC
        return rc(a, b, gsend.at[g], grecv.at[g, G_SEM[k]], d)

    def gland(B, g, k):
        h = ROWS // 2
        if k in (0, 18):
            b = sl(B, 1, y, c, 0 if k == 0 else h, h)
        elif k in (1, 16):
            b = sl(B, 0, ym, c, 0 if k == 1 else h, h)
        elif k in (2, 17):
            b = sl(B, 0, yp, c, h if k == 2 else 0, h)
        elif k == 3:
            b = sl(B, 0, y2, c)
        elif k == 5:
            b = sl(B, 1, ym, c)
        elif k == 6:
            b = sl(B, 1, yp, c)
        elif k == 7:
            b = sl(B, 1, y2, c)
        else:
            b = sl(B, (k - 8) // 4, (y, ym, yp, y2)[(k - 8) % 4], 1 - c)
        rc(b, b, gsend.at[g], grecv.at[g, G_SEM[k]], dC).wait_recv()

    def gstart(B, g, *ks):
        for k in ks:
            gcopy(B, g, k).start()

    def fwd(B, g, land, *sends):
        for k in land:
            gland(B, g, k)
        gstart(B, g, *sends)

    def tcopy(e, a, k):
        buf, me, d = ((TZ, z, z_others), (TX, x, x_others))[a]
        ref = buf.at[e, me]
        return rc(ref, ref, ssend.at[e], srecv.at[e, a, k - 1], d[k - 1])

    def tsum(e, a):
        buf, me = ((TZ, z), (TX, x))[a]
        for k in range(1, 4):
            ref = buf.at[e, (me + 4 - k) % 4]
            rc(ref, ref, ssend.at[e], srecv.at[e, a, k - 1], dC).wait_recv()
        return (buf[e, 0].astype(F32) + buf[e, 1].astype(F32)) + (
            buf[e, 2].astype(F32) + buf[e, 3].astype(F32)
        )

    def tsend(e, a):
        for k in range(1, 4):
            tcopy(e, a, k).start()

    def tmid(e):
        TX[e, x] = tsum(e, 0).astype(BF16)
        tsend(e, 1)

    def onehots():
        grow = GR[...]
        rows = lax.broadcasted_iota(jnp.int32, (GROUPS, NB), 0)
        onehot = (rows == jnp.broadcast_to(grow, (GROUPS, NB))).astype(F32)
        diag = lax.broadcasted_iota(jnp.int32, (NB, NB), 0) == lax.broadcasted_iota(
            jnp.int32, (NB, NB), 1
        )
        gcol = jnp.sum(
            jnp.where(diag, jnp.broadcast_to(grow, (NB, NB)), 0).astype(F32),
            axis=1, keepdims=True,
        )
        onehot_t = (
            lax.broadcasted_iota(jnp.int32, (NB, GROUPS), 1).astype(F32)
            == jnp.broadcast_to(gcol, (NB, GROUPS))
        ).astype(F32)
        return onehot, onehot_t

    def start():
        cp_dy.wait()
        pl.semaphore_wait(bar, 9)
        gstart(DYB, 0, 1, 2, 16, 17, 8)

    def stat0():
        cp_x.wait()
        for d in small:
            d.wait()
        for b in range(NB):
            xb = XT[b * BLK : (b + 1) * BLK, :].astype(F32)
            BSUM[b : b + 1, :] = jnp.sum(xb * xb, axis=0, keepdims=True)
        TZ[0, z] = jnp.dot(
            onehots()[0], BSUM[...], precision=HIGHEST, preferred_element_type=F32
        ).astype(BF16)
        tsend(0, 0)
        gstart(DYB, 0, 0, 18)

    def stat2():
        quad = tsum(0, 1) / GHOST
        rn_ref[...] = (1.0 - momentum) * RN[...] + momentum * (
            jnp.sum(quad, axis=0, keepdims=True) / GROUPS
        )
        gain = GN[...]
        SCB[...] = jnp.dot(
            onehots()[1], lax.rsqrt(quad + epsilon), precision=HIGHEST, preferred_element_type=F32
        )
        for b in range(NB):
            rows = slice(b * BLK, (b + 1) * BLK)
            nb = XT[rows, :].astype(F32) * SCB[b : b + 1, :]
            NRM[rows, :] = nb
            HB[0, rows, own_cols] = (gain * nb).astype(BF16)
        gstart(HB, 1, 1, 2, 0, 18, 16, 17, 8)

    def transposed(B, i, slot):
        @pl.loop(0, 8)
        def _(j):
            cols = pl.ds(pl.multiple_of(j * FEAT, FEAT), FEAT)
            LT[i, cols, pl.ds(slot * ROWS, ROWS)] = B[slot, :, cols].T

    def k_part(wi, slot, yy):
        ks = pl.ds(pl.multiple_of(yy * 2 * FEAT, 2 * FEAT), 2 * FEAT)
        return jnp.dot(HB[slot, :, ks], W[wi, ks, :], preferred_element_type=F32)

    def k_block(slot, i, first):
        yy = (y, ym, yp, y2)[i]
        if first and slot == 0:
            cp_w[0].wait()
            cp_w[1].wait()
        for wi, dst in ((0, GT), (1, LF)):
            v = k_part(wi, slot, yy)
            dst[slot] = v if first else dst[slot] + v

    def units(slot):
        @pl.loop(0, ROWS // 32)
        def _(i):
            r = pl.ds(pl.multiple_of(i * 32, 32), 32)
            ro = pl.ds(pl.multiple_of(slot * ROWS + i * 32, 32), 32)
            gate, lift, gh = GT[slot, r, :], LF[slot, r, :], GH[slot, r, :]
            sigma = jax.nn.sigmoid(gate)
            G[0, ro, :] = (gate * sigma * lift).astype(BF16)
            G[1, ro, :] = (gh * lift * sigma * (1.0 + gate * (1.0 - sigma))).astype(BF16)
            G[2, ro, :] = (gh * gate * sigma).astype(BF16)

    def gh(slot):
        if slot == 0:
            cp_w[2].wait()
        GH[slot] = jnp.dot(DYB[slot], W[2], preferred_element_type=F32)

    def ready(B, g, *ks):
        for k in ks:
            gland(B, g, k)

    AS, AP, AX1P, AX1M, AXIP, AXIM, AX2P, AX2M = range(8)
    BX1P, BX1M, BXIP, BXIM, BX2P, BX2M, BSK, BPK = range(8)
    A_SEM = (0, 1, 2, 2, 3, 3, 3, 3)
    B_SEM = (0, 0, 1, 1, 1, 1, 2, 3)
    pair = z // 2
    lo2, hi2 = pl.ds(0, 2), pl.ds(2, 2)

    def a_copy(k, a):
        far = pl.ds(pl.multiple_of((1 - pair) * 1024, 1024), 1024)
        src, dst, d = (
            (PA.at[a, far], RSA.at[a], dS),
            (SPA.at[a], QA.at[a, :, role], dP),
            (QA.at[a, x2, 0], R1.at[a, 0], dXp),
            (QA.at[a, x2, 1], R1.at[a, 1], dXm),
            (QA.at[a, xp, 1], R2.at[a, 0, 1], dXp),
            (QA.at[a, xm, 0], R2.at[a, 1, 0], dXm),
            (QA.at[a, xp, 0], R2.at[a, 0, 0], dXp),
            (QA.at[a, xm, 1], R2.at[a, 1, 1], dXm),
        )[k]
        return rc(src, dst, asend.at[a], arecv.at[A_SEM[k], a], d)

    def a_land(n, a):
        b = (RSA.at[a], QA.at[a, :, 1 - role], R1.at[a], R2.at[a])[n]
        rc(b, b, asend.at[a], arecv.at[n, a], dC).wait_recv()

    def b_copy(k, b):
        src, dst, d = (
            (PB.at[b, x2, lo2], T1.at[b, 0], dXp),
            (PB.at[b, x2, hi2], T1.at[b, 1], dXm),
            (PB.at[b, xp, hi2], T2.at[b, 0, hi2], dXp),
            (PB.at[b, xm, lo2], T2.at[b, 1, lo2], dXm),
            (PB.at[b, xp, lo2], T2.at[b, 0, lo2], dXp),
            (PB.at[b, xm, hi2], T2.at[b, 1, hi2], dXm),
            (BS.at[b], U1.at[b], dS),
            (BP.at[b], U2.at[b], dP),
        )[k]
        return rc(src, dst, bsend.at[b], brecv.at[B_SEM[k], b], d)

    def b_land(n, b):
        r = (T1.at[b], T2.at[b], U1.at[b], U2.at[b])[n]
        rc(r, r, bsend.at[b], brecv.at[n, b], dC).wait_recv()

    def weights(p):
        mi, j = p // 2, p % 2

        @pl.loop(0, 2)
        def _(n):
            rh = (1 - pair + n) % 2
            rows = pl.ds(pl.multiple_of(rh * 1024, 1024), 1024)
            res = jnp.dot(
                LT[(mi + 1) // 2, rows, :],
                G[mi, :, j * 256 : (j + 1) * 256],
                preferred_element_type=F32,
            ).astype(BF16)
            for off in range(2):
                part = res[:, off * 128 : (off + 1) * 128]
                if (p, off) in A_PARTS:
                    PA[A_PARTS.index((p, off)), rows, :] = part
                else:
                    b = B_PARTS.index((p, off))
                    for i in range(8):
                        PB[b, i % 4, rh * 2 + i // 4] = part[i * 128 : (i + 1) * 128]

            @pl.when(n == 0)
            def _():
                for off in range(2):
                    if (p, off) in A_PARTS:
                        a_copy(AS, A_PARTS.index((p, off))).start()

        for ks in ((BX1P, BX1M), (BXIP, BXIM)):
            for off in range(2):
                if (p, off) in B_PARTS:
                    for k in ks:
                        b_copy(k, B_PARTS.index((p, off))).start()

    def plus(a, b):
        return a.astype(F32) + b.astype(F32)

    def out_cols(part, half):
        p, off = part
        return pl.ds(pl.multiple_of(half * HALF + (p % 2) * 256 + off * 128, 128), 128)

    def step_ap(a):
        a_land(0, a)
        for xd in range(4):
            ra = pl.ds(pl.multiple_of(zp * HALF + xd * 128, 128), 128)
            rr = pl.ds(pl.multiple_of((zp % 2) * HALF + xd * 128, 128), 128)
            SPA[a, xd] = plus(PA[a, ra, :], RSA[a, rr, :]).astype(BF16)
        a_copy(AP, a).start()
        for xd in range(4):
            ra = pl.ds(pl.multiple_of(z * HALF + xd * 128, 128), 128)
            rr = pl.ds(pl.multiple_of((z % 2) * HALF + xd * 128, 128), 128)
            QA[a, xd, role] = plus(PA[a, ra, :], RSA[a, rr, :]).astype(BF16)

    def step_ax1(a):
        a_land(1, a)
        for k in (AX1P, AX1M, AXIP, AXIM):
            a_copy(k, a).start()

    def step_ax2(a):
        a_land(2, a)
        QA[a, xp, 0] = plus(QA[a, xp, 0], R1[a, 0]).astype(BF16)
        a_copy(AX2P, a).start()
        QA[a, xm, 1] = plus(QA[a, xm, 1], R1[a, 1]).astype(BF16)
        a_copy(AX2M, a).start()

    def step_af(a):
        a_land(3, a)
        for h in range(2):
            gr_ref[A_PARTS[a][0] // 2, :, out_cols(A_PARTS[a], h)] = plus(
                QA[a, x, h], R2[a, 0, h]
            ) + R2[a, 1, h].astype(F32)

    def step_bx2(b):
        b_land(0, b)
        for i in range(2):
            PB[b, xp, i] = plus(PB[b, xp, i], T1[b, 0, i]).astype(BF16)
        b_copy(BX2P, b).start()
        for i in range(2):
            PB[b, xm, 2 + i] = plus(PB[b, xm, 2 + i], T1[b, 1, i]).astype(BF16)
        b_copy(BX2M, b).start()

    def step_bs(b):
        b_land(1, b)
        for i in range(2):
            o = 2 * (1 - pair) + i
            BS[b, i] = (plus(PB[b, x, o], T2[b, 0, o]) + T2[b, 1, o].astype(F32)).astype(BF16)
        b_copy(BSK, b).start()
        for i in range(2):
            o = 2 * pair + i
            BK[b, i] = plus(PB[b, x, o], T2[b, 0, o]) + T2[b, 1, o].astype(F32)

    def step_bp(b):
        b_land(2, b)
        BP[b] = plus(BK[b, zp % 2], U1[b, zp % 2]).astype(BF16)
        b_copy(BPK, b).start()
        gr_ref[B_PARTS[b][0] // 2, :, out_cols(B_PARTS[b], role)] = plus(
            BK[b, z % 2], U1[b, z % 2]
        )

    def step_bf(b):
        b_land(3, b)
        gr_ref[B_PARTS[b][0] // 2, :, out_cols(B_PARTS[b], 1 - role)] = U2[b].astype(F32)

    V1P, V1M, VIP, VIM, V2P, V2M, WSK = range(7)
    lo, hi = pl.ds(0, ROWS), pl.ds(ROWS, ROWS)
    y_of = (y2, yp, ym, y)
    Y_SEM = (0, 1, 2, 3, 3, 2, 4)

    def y_copy(k, e):
        a, b, d = (
            (EK.at[e, y2, lo], V1.at[e, 0], dYp),
            (EK.at[e, y2, hi], V1.at[e, 1], dYm),
            (EK.at[e, yp, hi], V2.at[e, 0, hi], dYp),
            (EK.at[e, ym, lo], V2.at[e, 1, lo], dYm),
            (EK.at[e, yp, lo], V2.at[e, 0, lo], dYp),
            (EK.at[e, ym, hi], V2.at[e, 1, hi], dYm),
            (WS.at[e], W1.at[e], dP),
        )[k]
        return rc(a, b, ysend.at[e], yrecv.at[e, Y_SEM[k]], d)

    def y_land(n, e):
        b = (V1.at[e, 0], V1.at[e, 1], V2.at[e, :, hi], V2.at[e, :, lo], W1.at[e])[n]
        rc(b, b, ysend.at[e], yrecv.at[e, n], dC).wait_recv()

    def sib_copy(e, i):
        return rc(
            ES.at[e, y_of[i]], ER.at[e, y_of[i]], csend.at[e], crecv.at[e, i], dC
        )

    def nt(a, b):
        return lax.dot_general(a, b, (((1,), (1,)), ((), ())), preferred_element_type=F32)

    def y_product(e, yy, cc):
        rows = pl.ds(pl.multiple_of((yy * 2 + cc) * FEAT, FEAT), FEAT)
        if e == 0:
            v = nt(G[1], W[0, rows, :]) + nt(G[2], W[1, rows, :])
        else:
            v = nt(G[0], W[2, rows, :])
        return v.astype(BF16)

    def y_sib(e, i):
        ES[e, y_of[i]] = y_product(e, y_of[i], 1 - c)
        sib_copy(e, i).start()

    def y_own(e, i):
        EK[e, y_of[i]] = y_product(e, y_of[i], c)

    def y_merge(e, i, *sends):
        sib_copy(e, i).wait_recv()
        yy = y_of[i]

        @pl.loop(0, 6)
        def _(n):
            r = pl.ds(pl.multiple_of(n * 128, 128), 128)
            EK[e, yy, r, :] = plus(EK[e, yy, r, :], ER[e, yy, r, :]).astype(BF16)

        for k in sends:
            y_copy(k, e).start()

    def y_relay(e, d):
        y_land(d, e)
        yy = (yp, ym)[d]

        @pl.loop(0, 3)
        def _(n):
            r = pl.ds(pl.multiple_of(d * ROWS + n * 128, 128), 128)
            rv = pl.ds(pl.multiple_of(n * 128, 128), 128)
            EK[e, yy, r, :] = plus(EK[e, yy, r, :], V1[e, d, rv, :]).astype(BF16)

        y_copy((V2P, V2M)[d], e).start()

    def y_p(e):
        y_land(2, e)

        @pl.loop(0, 3)
        def _(n):
            r = pl.ds(pl.multiple_of(ROWS + n * 128, 128), 128)
            rv = pl.ds(pl.multiple_of(n * 128, 128), 128)
            WS[e, rv, :] = (
                plus(EK[e, y, r, :], V2[e, 0, r, :]) + V2[e, 1, r, :].astype(F32)
            ).astype(BF16)

        y_copy(WSK, e).start()

    def y_f(e):
        y_land(3, e)

        @pl.loop(0, 3)
        def _(n):
            r = pl.ds(pl.multiple_of(n * 128, 128), 128)
            FS[e, r, :] = plus(EK[e, y, r, :], V2[e, 0, r, :]) + V2[e, 1, r, :].astype(F32)

    def y_block_out():
        y_land(4, 1)
        for b in range(NB):
            rows = slice(b * BLK, (b + 1) * BLK)
            branch = FS[1, rows, :] + W1[1, rows, :].astype(F32)
            bo_ref[rows, :] = (XT[rows, :].astype(F32) + branch).astype(BF16)

    def y_partial():
        y_land(4, 0)
        for b in range(NB):
            rows = slice(b * BLK, (b + 1) * BLK)
            g = FS[0, rows, :] + W1[0, rows, :].astype(F32)
            FS[0, rows, :] = g
            BSUM[b : b + 1, :] = jnp.sum(g * NRM[rows, :], axis=0, keepdims=True)
        TZ[1, z] = jnp.dot(
            onehots()[0], BSUM[...], precision=HIGHEST, preferred_element_type=F32
        ).astype(BF16)
        tsend(1, 0)

    def y_grad_tokens():
        total = tsum(1, 1)
        gg_ref[...] = jnp.sum(total, axis=0, keepdims=True)
        gain = GN[...]
        BSUM[...] = jnp.dot(
            onehots()[1], gain * total / GHOST, precision=HIGHEST, preferred_element_type=F32
        )
        for b in range(NB):
            rows = slice(b * BLK, (b + 1) * BLK)
            g, nb = FS[0, rows, :], NRM[rows, :]
            dyb = DYB[0, rows, own_cols].astype(F32)
            gt_ref[rows, :] = (
                dyb + SCB[b : b + 1, :] * (gain * g - nb * BSUM[b : b + 1, :])
            ).astype(BF16)

    def left(sem, kib):
        ref = LT.at[0, pl.ds(0, kib * 1024 // (4 * ROWS))]
        rc(ref, ref, sem, sem, dC).wait_send()

    def left_gather(B, g):
        left(gsend.at[g], 30 * 96)

    def left_table(e):
        left(ssend.at[e], 6 * 24)

    def left_sums(e):
        left(csend.at[e], 4 * 384)
        left(ysend.at[e], 7 * 192)

    def left_a(a):
        left(asend.at[a], 18 * 32)

    def left_b(b):
        left(bsend.at[b], 15 * 32)

    start()
    stat0()
    tmid(0)
    fwd(DYB, 0, (2,), 4)
    fwd(DYB, 0, (1,), 3)
    fwd(DYB, 0, (0,), 5, 6)
    fwd(DYB, 0, (16,), 9)
    fwd(DYB, 0, (17,), 10)
    stat2()
    gland(DYB, 0, 8)
    fwd(DYB, 0, (3,), 7, 11)
    gland(DYB, 0, 9)
    gland(DYB, 0, 10)
    gland(HB, 1, 8)
    k_block(0, 0, True)
    gland(DYB, 0, 11)
    transposed(DYB, 0, 0)
    gh(0)
    fwd(HB, 1, (1,), 3)
    fwd(HB, 1, (2,), 4)
    fwd(DYB, 0, (18,), 19, 20, 12)
    fwd(HB, 1, (0,), 5, 6)
    gland(DYB, 0, 12)
    fwd(HB, 1, (18,), 19, 20, 12)
    fwd(HB, 1, (17,), 10)
    fwd(HB, 1, (16,), 9)
    gland(HB, 1, 12)
    k_block(1, 0, True)
    gland(HB, 1, 10)
    k_block(0, 2, False)
    fwd(HB, 1, (3,), 7, 11)
    gland(HB, 1, 9)
    k_block(0, 1, False)
    fwd(DYB, 0, (7,), 15)
    fwd(DYB, 0, (5,), 13)
    fwd(DYB, 0, (6,), 14)
    gland(HB, 1, 11)
    transposed(HB, 1, 0)
    k_block(0, 3, False)
    units(0)
    gland(DYB, 0, 15)
    gland(DYB, 0, 13)
    gland(DYB, 0, 14)
    gh(1)
    transposed(DYB, 0, 1)
    fwd(HB, 1, (6,), 14)
    fwd(HB, 1, (5,), 13)
    fwd(HB, 1, (7,), 15)
    gland(HB, 1, 14)
    k_block(1, 2, False)
    gland(HB, 1, 13)
    k_block(1, 1, False)
    gland(HB, 1, 15)
    k_block(1, 3, False)
    units(1)
    weights(0)
    transposed(HB, 1, 1)
    weights(2)
    weights(4)
    y_sib(0, 0)
    y_own(0, 0)
    y_sib(0, 2)
    y_sib(0, 1)
    y_merge(0, 0, V1P, V1M)
    weights(5)
    step_ap(0)
    left_gather(HB, 1)
    y_own(0, 2)
    y_merge(0, 2, VIM)
    weights(1)
    y_own(0, 1)
    y_merge(0, 1, VIP)
    step_bx2(5)
    y_own(1, 2)
    y_sib(1, 3)
    y_relay(0, 1)
    step_ap(2)
    y_own(1, 3)
    step_bx2(2)
    step_bx2(6)
    y_relay(0, 0)
    left_table(0)
    y_sib(1, 0)
    y_sib(1, 1)
    y_merge(1, 3)
    y_own(1, 0)
    step_ax1(0)
    step_bx2(0)
    y_own(1, 1)
    y_sib(1, 2)
    step_bx2(1)
    y_merge(1, 0, V1P, V1M)
    y_sib(0, 3)
    step_ap(4)
    y_merge(1, 1, VIP)
    step_ax1(2)
    weights(3)
    step_bs(5)
    y_merge(1, 2, VIM)
    step_bx2(4)
    y_own(0, 3)
    y_merge(0, 3)
    step_bs(2)
    y_p(0)
    left_gather(DYB, 0)
    y_f(0)
    step_bs(6)
    step_ax2(0)
    step_ax1(4)
    step_ap(1)
    step_bs(0)
    y_relay(1, 1)
    y_relay(1, 0)
    step_bs(1)
    step_ax2(2)
    y_partial()
    step_bx2(3)
    step_ap(3)
    step_ax1(1)
    step_bp(5)
    step_bs(4)
    step_bp(2)
    step_af(0)
    left_a(0)
    step_ax2(4)
    step_bp(6)
    y_p(1)
    step_ax1(3)
    y_f(1)
    step_af(2)
    left_a(2)
    step_bp(0)
    step_bf(5)
    left_b(5)
    step_bf(2)
    left_b(2)
    step_bs(3)
    step_bf(6)
    step_bp(1)
    left_b(6)
    tmid(1)
    step_ax2(1)
    step_bp(4)
    step_af(4)
    left_a(4)
    step_ax2(3)
    step_bp(3)
    y_block_out()
    left_sums(1)
    step_bf(0)
    left_b(0)
    step_af(1)
    left_a(1)
    y_grad_tokens()
    left_sums(0)
    step_bf(1)
    left_table(1)
    step_af(3)
    left_a(3)
    left_b(1)
    step_bf(4)
    left_b(4)
    step_bf(3)
    left_b(3)


def emit(bo_ref, gt_ref, rn_ref, gg_ref, gr_ref, bo, gt, rn, gg, g_gate, g_up, g_down, sem):
    copies = [
        pltpu.make_async_copy(a, b, sem.at[i])
        for i, (a, b) in enumerate((
            (gr_ref.at[1], g_gate), (gr_ref.at[2], g_up), (gr_ref.at[0], g_down),
            (bo_ref, bo), (gt_ref, gt), (rn_ref, rn), (gg_ref, gg),
        ))
    ]
    for d in copies:
        d.start()
    for d in copies:
        d.wait()


def body(tokens, norm_gain, running_sq, gate_weight, up_weight, down_weight_t, groups, cotangent):
    V = pltpu.VMEM
    any_spec = pl.BlockSpec(memory_space=pl.ANY)
    vmem_spec = pl.BlockSpec(memory_space=pltpu.VMEM)
    na, nb = len(A_PARTS), len(B_PARTS)
    sq = (128, 128)
    dma = pltpu.SemaphoreType.DMA
    scratch = [
        V((1, NB), jnp.int32), V((1, FEAT), F32), V((1, FEAT), F32),
        V((ROWS, FEAT), BF16), V((ROWS, FEAT), F32), V((NB, FEAT), F32), V((NB, FEAT), F32),
        V((2, ROWS, WIDTH), BF16), V((2, ROWS, WIDTH), BF16), V((2, WIDTH, 2 * ROWS), BF16),
        V((3, WIDTH, HALF), BF16), V((3, 2 * ROWS, HALF), BF16),
        V((2, ROWS, HALF), F32), V((2, ROWS, HALF), F32), V((2, ROWS, HALF), F32),
        V((2, 4, GROUPS, FEAT), BF16), V((2, 4, GROUPS, FEAT), BF16),
        V((na, WIDTH, 128), BF16), V((na, 1024, 128), BF16), V((na, 4, *sq), BF16),
        V((na, 4, 2, *sq), BF16), V((na, 2, *sq), BF16), V((na, 2, 2, *sq), BF16),
        V((nb, 4, 4, *sq), BF16), V((nb, 2, 2, *sq), BF16), V((nb, 2, 4, *sq), BF16),
        V((nb, 2, *sq), F32), V((nb, 2, *sq), BF16), V((nb, 2, *sq), BF16),
        V((nb, *sq), BF16), V((nb, *sq), BF16),
        V((2, 4, 2 * ROWS, FEAT), BF16), V((2, 4, 2 * ROWS, FEAT), BF16),
        V((2, 4, 2 * ROWS, FEAT), BF16), V((2, 2, ROWS, FEAT), BF16),
        V((2, 2, 2 * ROWS, FEAT), BF16), V((2, ROWS, FEAT), BF16), V((2, ROWS, FEAT), BF16),
        V((2, ROWS, FEAT), F32),
        dma((8,)), dma((2,)), dma((2, 18)), dma((2,)), dma((2, 2, 3)),
        dma((na,)), dma((4, na)), dma((nb,)), dma((4, nb)), dma((2,)), dma((2, 5)),
        dma((2,)), dma((2, 4)),
    ]
    held = (
        ((ROWS, FEAT), BF16), ((ROWS, FEAT), BF16), ((1, FEAT), F32), ((1, FEAT), F32),
        ((3, 128, 1024), F32),
    )
    results = pl.pallas_call(
        kernel,
        out_shape=tuple(pltpu.VMEM(shape, dtype) for shape, dtype in held),
        in_specs=[any_spec] * 8,
        out_specs=(vmem_spec,) * 5,
        scratch_shapes=scratch,
        compiler_params=pltpu.CompilerParams(
            collective_id=0, has_side_effects=True, vmem_limit_bytes=VMEM_LIMIT
        ),
    )(
        tokens, norm_gain.reshape(1, -1), running_sq.reshape(1, -1), gate_weight, up_weight,
        down_weight_t, groups.reshape(1, -1), cotangent,
    )
    weight = jax.ShapeDtypeStruct((128, 1024), F32)
    block_out, grad_tokens, run_new, gain_grad, g_gate, g_up, g_down = pl.pallas_call(
        emit,
        out_shape=tuple(jax.ShapeDtypeStruct(*a) for a in held[:4]) + (weight,) * 3,
        in_specs=[vmem_spec] * 5,
        out_specs=(any_spec,) * 7,
        scratch_shapes=[dma((7,))],
        compiler_params=pltpu.CompilerParams(vmem_limit_bytes=4 << 20),
    )(*results)
    return (
        block_out, grad_tokens, run_new.reshape(-1), gain_grad.reshape(-1), g_gate, g_up, g_down,
    )


def solution(mesh):
    placed = (
        P("tok", "mp"),
        P(),
        P("mp"),
        P(None, "mp"),
        P(None, "mp"),
        P(None, "mp"),
        P("tok"),
        P("tok", "mp"),
    )
    return jax.shard_map(
        body,
        mesh=mesh,
        in_specs=placed,
        out_specs=(
            P("tok", "mp"),
            P("tok", "mp"),
            P("mp"),
            P("mp"),
            P("tok", "mp"),
            P("tok", "mp"),
            P("tok", "mp"),
        ),
        check_vma=False,
    )
```

```python
import jax
import jax.numpy as jnp
from jax import lax
from jax.experimental import pallas as pl
from jax.experimental.pallas import tpu as pltpu
from jax.sharding import PartitionSpec as P

GHOST = 128
BLK = 16
ROWS = 384
FEAT = 256
WIDTH = 2048
HALF = 512
GROUPS = 48
G_SEM = (0, 1, 2, 3, 3, 4, 5, 6, 7, 8, 9, 10, 11, 12, 13, 14, 15, 16, 17, 4, 5)
VMEM_LIMIT = 62 << 20
NB = 24
A_PARTS = tuple((p, 0) for p in range(5))
B_PARTS = tuple((p, 1) for p in range(5)) + ((5, 0), (5, 1))

epsilon = 1e-05
momentum = 0.1
F32 = jnp.float32
BF16 = jnp.bfloat16
HIGHEST = lax.Precision.HIGHEST


def kernel(
    tok_hbm, gain_hbm, run_hbm, gw_hbm, uw_hbm, dw_hbm, grp_hbm, cot_hbm,
    bo_ref, gt_ref, rn_ref, gg_ref, gr_ref,
    GR, GN, RN, XT, NRM, BSUM, SCB, DYB, HB, LT, W, G, GT, LF, GH,
    TZ, TX, PA, RSA, SPA, QA, R1, R2, PB, T1, T2, BK, BS, U1, BP, U2,
    EK, ES, ER, V1, V2, WS, W1, FS,
    lsem, gsend, grecv, ssend, srecv, asend, arecv, bsend, brecv, ysend, yrecv, csend, crecv,
):
    t = lax.axis_index("tok")
    m = lax.axis_index("mp")
    z, x = t // 4, t % 4
    y, c = m // 2, m % 2
    zp = z + 1 - 2 * (z % 2)
    zs = 3 - z
    role = ((z + 1) // 2) % 2
    yp, ym, y2 = (y + 1) % 4, (y + 3) % 4, (y + 2) % 4
    xp, xm, x2 = (x + 1) % 4, (x + 3) % 4, (x + 2) % 4
    dC = (t, y * 2 + 1 - c)
    dP = (zp * 4 + x, m)
    dS = (zs * 4 + x, m)
    dYp, dYm = (t, yp * 2 + c), (t, ym * 2 + c)
    dXp, dXm = (z * 4 + xp, m), (z * 4 + xm, m)

    def rc(src, dst, ss, rs, dev):
        return pltpu.make_async_remote_copy(
            src_ref=src, dst_ref=dst, send_sem=ss, recv_sem=rs,
            device_id=dev, device_id_type=pl.DeviceIdType.MESH,
        )

    own_cols = pl.ds(pl.multiple_of(m * FEAT, FEAT), FEAT)

    bar = pltpu.get_barrier_semaphore()
    z_others = [(((z + k) % 4) * 4 + x, m) for k in range(1, 4)]
    x_others = [(z * 4 + (x + k) % 4, m) for k in range(1, 4)]
    for d in (*z_others, *x_others, dC, dYp, dYm):
        pl.semaphore_signal(bar, inc=1, device_id=d, device_id_type=pl.DeviceIdType.MESH)

    cp_dy = pltpu.make_async_copy(cot_hbm, DYB.at[0, :, own_cols], lsem.at[0])
    cp_dy.start()
    cp_x = pltpu.make_async_copy(tok_hbm, XT, lsem.at[1])
    cp_x.start()
    small = [
        pltpu.make_async_copy(a, b, lsem.at[5 + i])
        for i, (a, b) in enumerate(
            ((grp_hbm, GR), (gain_hbm.at[:, own_cols], GN), (run_hbm, RN))
        )
    ]
    for d in small:
        d.start()
    wcols = pl.ds(pl.multiple_of(role * HALF, HALF), HALF)
    cp_w = [
        pltpu.make_async_copy(h.at[:, wcols], W.at[i], lsem.at[2 + i])
        for i, h in enumerate((gw_hbm, uw_hbm, dw_hbm))
    ]
    for k in (2, 0, 1):
        cp_w[k].start()

    def sl(B, slot, yy, cc, r0=0, n=ROWS):
        return B.at[slot, pl.ds(r0, n), pl.ds(pl.multiple_of((yy * 2 + cc) * FEAT, FEAT), FEAT)]

    def gcopy(B, g, k):
        h = ROWS // 2
        if k in (0, 18):
            r = 0 if k == 0 else h
            a, b, d = sl(B, 0, y, c, r, h), sl(B, 1, y, c, r, h), dP
        elif k in (1, 16):
            a = b = sl(B, 0, y, c, 0 if k == 1 else h, h)
            d = dYp
        elif k in (2, 17):
            a = b = sl(B, 0, y, c, h if k == 2 else 0, h)
            d = dYm
        elif k == 3:
            a = b = sl(B, 0, ym, c, 0, h)
            d = dYp
        elif k == 4:
            a = b = sl(B, 0, yp, c, h, h)
            d = dYm
        elif k in (5, 6, 19, 20):
            a = b = sl(B, 1, y, c, 0 if k < 7 else h, h)
            d = dYp if k in (5, 19) else dYm
        elif k == 7:
            a, b, d = sl(B, 0, y2, c), sl(B, 1, y2, c), dP
        else:
            slot = (k - 8) // 4
            yy = (y, ym, yp, y2)[(k - 8) % 4]
            a = b = sl(B, slot, yy, c)
            d = dC
        return rc(a, b, gsend.at[g], grecv.at[g, G_SEM[k]], d)

    def gland(B, g, k):
        h = ROWS // 2
        if k in (0, 18):
            b = sl(B, 1, y, c, 0 if k == 0 else h, h)
        elif k in (1, 16):
            b = sl(B, 0, ym, c, 0 if k == 1 else h, h)
        elif k in (2, 17):
            b = sl(B, 0, yp, c, h if k == 2 else 0, h)
        elif k == 3:
            b = sl(B, 0, y2, c)
        elif k == 5:
            b = sl(B, 1, ym, c)
        elif k == 6:
            b = sl(B, 1, yp, c)
        elif k == 7:
            b = sl(B, 1, y2, c)
        else:
            b = sl(B, (k - 8) // 4, (y, ym, yp, y2)[(k - 8) % 4], 1 - c)
        rc(b, b, gsend.at[g], grecv.at[g, G_SEM[k]], dC).wait_recv()

    def gstart(B, g, *ks):
        for k in ks:
            gcopy(B, g, k).start()

    def fwd(B, g, land, *sends):
        for k in land:
            gland(B, g, k)
        gstart(B, g, *sends)

    def tcopy(e, a, k):
        buf, me, d = ((TZ, z, z_others), (TX, x, x_others))[a]
        ref = buf.at[e, me]
        return rc(ref, ref, ssend.at[e], srecv.at[e, a, k - 1], d[k - 1])

    def tsum(e, a):
        buf, me = ((TZ, z), (TX, x))[a]
        for k in range(1, 4):
            ref = buf.at[e, (me + 4 - k) % 4]
            rc(ref, ref, ssend.at[e], srecv.at[e, a, k - 1], dC).wait_recv()
        return (buf[e, 0].astype(F32) + buf[e, 1].astype(F32)) + (
            buf[e, 2].astype(F32) + buf[e, 3].astype(F32)
        )

    def tsend(e, a):
        for k in range(1, 4):
            tcopy(e, a, k).start()

    def tmid(e):
        TX[e, x] = tsum(e, 0).astype(BF16)
        tsend(e, 1)

    def onehots():
        grow = GR[...]
        rows = lax.broadcasted_iota(jnp.int32, (GROUPS, NB), 0)
        onehot = (rows == jnp.broadcast_to(grow, (GROUPS, NB))).astype(F32)
        diag = lax.broadcasted_iota(jnp.int32, (NB, NB), 0) == lax.broadcasted_iota(
            jnp.int32, (NB, NB), 1
        )
        gcol = jnp.sum(
            jnp.where(diag, jnp.broadcast_to(grow, (NB, NB)), 0).astype(F32),
            axis=1, keepdims=True,
        )
        onehot_t = (
            lax.broadcasted_iota(jnp.int32, (NB, GROUPS), 1).astype(F32)
            == jnp.broadcast_to(gcol, (NB, GROUPS))
        ).astype(F32)
        return onehot, onehot_t

    def start():
        cp_dy.wait()
        pl.semaphore_wait(bar, 9)
        gstart(DYB, 0, 1, 2, 16, 17, 8)

    def stat0():
        cp_x.wait()
        for d in small:
            d.wait()
        for b in range(NB):
            xb = XT[b * BLK : (b + 1) * BLK, :].astype(F32)
            BSUM[b : b + 1, :] = jnp.sum(xb * xb, axis=0, keepdims=True)
        TZ[0, z] = jnp.dot(
            onehots()[0], BSUM[...], precision=HIGHEST, preferred_element_type=F32
        ).astype(BF16)
        tsend(0, 0)
        gstart(DYB, 0, 0, 18)

    def stat2():
        quad = tsum(0, 1) / GHOST
        rn_ref[...] = (1.0 - momentum) * RN[...] + momentum * (
            jnp.sum(quad, axis=0, keepdims=True) / GROUPS
        )
        gain = GN[...]
        SCB[...] = jnp.dot(
            onehots()[1], lax.rsqrt(quad + epsilon), precision=HIGHEST, preferred_element_type=F32
        )
        for b in range(NB):
            rows = slice(b * BLK, (b + 1) * BLK)
            nb = XT[rows, :].astype(F32) * SCB[b : b + 1, :]
            NRM[rows, :] = nb
            HB[0, rows, own_cols] = (gain * nb).astype(BF16)
        gstart(HB, 1, 1, 2, 0, 18, 16, 17, 8)

    def transposed(B, i, slot):
        @pl.loop(0, 8)
        def _(j):
            cols = pl.ds(pl.multiple_of(j * FEAT, FEAT), FEAT)
            LT[i, cols, pl.ds(slot * ROWS, ROWS)] = B[slot, :, cols].T

    def k_part(wi, slot, yy):
        ks = pl.ds(pl.multiple_of(yy * 2 * FEAT, 2 * FEAT), 2 * FEAT)
        return jnp.dot(HB[slot, :, ks], W[wi, ks, :], preferred_element_type=F32)

    def k_block(slot, i, first):
        yy = (y, ym, yp, y2)[i]
        if first and slot == 0:
            cp_w[0].wait()
            cp_w[1].wait()
        for wi, dst in ((0, GT), (1, LF)):
            v = k_part(wi, slot, yy)
            dst[slot] = v if first else dst[slot] + v

    def units(slot):
        @pl.loop(0, ROWS // 32)
        def _(i):
            r = pl.ds(pl.multiple_of(i * 32, 32), 32)
            ro = pl.ds(pl.multiple_of(slot * ROWS + i * 32, 32), 32)
            gate, lift, gh = GT[slot, r, :], LF[slot, r, :], GH[slot, r, :]
            sigma = jax.nn.sigmoid(gate)
            G[0, ro, :] = (gate * sigma * lift).astype(BF16)
            G[1, ro, :] = (gh * lift * sigma * (1.0 + gate * (1.0 - sigma))).astype(BF16)
            G[2, ro, :] = (gh * gate * sigma).astype(BF16)

    def k_half(slot, i, sib, first):
        cc = 1 - c if sib else c
        ks = pl.ds(pl.multiple_of(((y, ym, yp, y2)[i] * 2 + cc) * FEAT, FEAT), FEAT)
        for wi, dst in ((0, GT), (1, LF)):
            v = jnp.dot(HB[slot, :, ks], W[wi, ks, :], preferred_element_type=F32)
            dst[slot] = v if first else dst[slot] + v

    def gh_block(i, first):
        yy = (y, ym, yp, y2)[i]
        ks = pl.ds(pl.multiple_of(yy * 2 * FEAT, 2 * FEAT), 2 * FEAT)
        v = jnp.dot(DYB[1, :, ks], W[2, ks, :], preferred_element_type=F32)
        GH[1] = v if first else GH[1] + v

    def tx_block(B, n, slot, i):
        yy = (y, ym, yp, y2)[i]
        for h in range(2):
            cols = pl.ds(pl.multiple_of((yy * 2 + h) * FEAT, FEAT), FEAT)
            LT[n, cols, pl.ds(slot * ROWS, ROWS)] = B[slot, :, cols].T

    def gh(slot):
        if slot == 0:
            cp_w[2].wait()
        GH[slot] = jnp.dot(DYB[slot], W[2], preferred_element_type=F32)

    def ready(B, g, *ks):
        for k in ks:
            gland(B, g, k)

    AS, AP, AX1P, AX1M, AXIP, AXIM, AX2P, AX2M = range(8)
    BX1P, BX1M, BXIP, BXIM, BX2P, BX2M, BSK, BPK = range(8)
    A_SEM = (0, 1, 2, 2, 3, 3, 3, 3)
    B_SEM = (0, 0, 1, 1, 1, 1, 2, 3)
    pair = z // 2
    lo2, hi2 = pl.ds(0, 2), pl.ds(2, 2)

    def a_copy(k, a):
        far = pl.ds(pl.multiple_of((1 - pair) * 1024, 1024), 1024)
        src, dst, d = (
            (PA.at[a, far], RSA.at[a], dS),
            (SPA.at[a], QA.at[a, :, role], dP),
            (QA.at[a, x2, 0], R1.at[a, 0], dXp),
            (QA.at[a, x2, 1], R1.at[a, 1], dXm),
            (QA.at[a, xp, 1], R2.at[a, 0, 1], dXp),
            (QA.at[a, xm, 0], R2.at[a, 1, 0], dXm),
            (QA.at[a, xp, 0], R2.at[a, 0, 0], dXp),
            (QA.at[a, xm, 1], R2.at[a, 1, 1], dXm),
        )[k]
        return rc(src, dst, asend.at[a], arecv.at[A_SEM[k], a], d)

    def a_land(n, a):
        b = (RSA.at[a], QA.at[a, :, 1 - role], R1.at[a], R2.at[a])[n]
        rc(b, b, asend.at[a], arecv.at[n, a], dC).wait_recv()

    def b_copy(k, b):
        src, dst, d = (
            (PB.at[b, x2, lo2], T1.at[b, 0], dXp),
            (PB.at[b, x2, hi2], T1.at[b, 1], dXm),
            (PB.at[b, xp, hi2], T2.at[b, 0, hi2], dXp),
            (PB.at[b, xm, lo2], T2.at[b, 1, lo2], dXm),
            (PB.at[b, xp, lo2], T2.at[b, 0, lo2], dXp),
            (PB.at[b, xm, hi2], T2.at[b, 1, hi2], dXm),
            (BS.at[b], U1.at[b], dS),
            (BP.at[b], U2.at[b], dP),
        )[k]
        return rc(src, dst, bsend.at[b], brecv.at[B_SEM[k], b], d)

    def b_land(n, b):
        r = (T1.at[b], T2.at[b], U1.at[b], U2.at[b])[n]
        rc(r, r, bsend.at[b], brecv.at[n, b], dC).wait_recv()

    def weights(p):
        mi, j = p // 2, p % 2

        @pl.loop(0, 2)
        def _(n):
            rh = (1 - pair + n) % 2
            rows = pl.ds(pl.multiple_of(rh * 1024, 1024), 1024)
            res = jnp.dot(
                LT[(mi + 1) // 2, rows, :],
                G[mi, :, j * 256 : (j + 1) * 256],
                preferred_element_type=F32,
            ).astype(BF16)
            for off in range(2):
                part = res[:, off * 128 : (off + 1) * 128]
                if (p, off) in A_PARTS:
                    PA[A_PARTS.index((p, off)), rows, :] = part
                else:
                    b = B_PARTS.index((p, off))
                    for i in range(8):
                        PB[b, i % 4, rh * 2 + i // 4] = part[i * 128 : (i + 1) * 128]

            @pl.when(n == 0)
            def _():
                for off in range(2):
                    if (p, off) in A_PARTS:
                        a_copy(AS, A_PARTS.index((p, off))).start()

        for ks in ((BX1P, BX1M), (BXIP, BXIM)):
            for off in range(2):
                if (p, off) in B_PARTS:
                    for k in ks:
                        b_copy(k, B_PARTS.index((p, off))).start()

    def weights_first(p):
        mi, j = p // 2, p % 2

        @pl.loop(0, 4)
        def _(n):
            xd = (x + 2 + n) % 4
            blocks = [pl.multiple_of(zd * HALF + xd * 128, 128) for zd in range(4)]
            lhs = jnp.concatenate(
                [LT[(mi + 1) // 2, pl.ds(r, 128), :] for r in blocks], axis=0
            )
            res = jnp.dot(
                lhs, G[mi, :, j * 256 : (j + 1) * 256], preferred_element_type=F32
            ).astype(BF16)
            for off in range(2):
                for zd in range(4):
                    part = res[zd * 128 : (zd + 1) * 128, off * 128 : (off + 1) * 128]
                    if (p, off) in A_PARTS:
                        PA[A_PARTS.index((p, off)), pl.ds(blocks[zd], 128), :] = part
                    else:
                        PB[B_PARTS.index((p, off)), xd, zd] = part
            for at, ks in ((0, (BX1P, BX1M)), (1, (BXIM,)), (3, (BXIP,))):

                @pl.when(n == at)
                def _():
                    for k in ks:
                        for off in range(2):
                            if (p, off) in B_PARTS:
                                b_copy(k, B_PARTS.index((p, off))).start()

        for off in range(2):
            if (p, off) in A_PARTS:
                a_copy(AS, A_PARTS.index((p, off))).start()

    def plus(a, b):
        return a.astype(F32) + b.astype(F32)

    def out_cols(part, half):
        p, off = part
        return pl.ds(pl.multiple_of(half * HALF + (p % 2) * 256 + off * 128, 128), 128)

    def step_ap(a):
        a_land(0, a)
        for xd in range(4):
            ra = pl.ds(pl.multiple_of(zp * HALF + xd * 128, 128), 128)
            rr = pl.ds(pl.multiple_of((zp % 2) * HALF + xd * 128, 128), 128)
            SPA[a, xd] = plus(PA[a, ra, :], RSA[a, rr, :]).astype(BF16)
        a_copy(AP, a).start()
        for xd in range(4):
            ra = pl.ds(pl.multiple_of(z * HALF + xd * 128, 128), 128)
            rr = pl.ds(pl.multiple_of((z % 2) * HALF + xd * 128, 128), 128)
            QA[a, xd, role] = plus(PA[a, ra, :], RSA[a, rr, :]).astype(BF16)

    def step_ax1(a):
        a_land(1, a)
        for k in (AX1P, AX1M, AXIP, AXIM):
            a_copy(k, a).start()

    def step_ax2(a):
        a_land(2, a)
        QA[a, xp, 0] = plus(QA[a, xp, 0], R1[a, 0]).astype(BF16)
        a_copy(AX2P, a).start()
        QA[a, xm, 1] = plus(QA[a, xm, 1], R1[a, 1]).astype(BF16)
        a_copy(AX2M, a).start()

    def step_af(a):
        a_land(3, a)
        for h in range(2):
            gr_ref[A_PARTS[a][0] // 2, :, out_cols(A_PARTS[a], h)] = plus(
                QA[a, x, h], R2[a, 0, h]
            ) + R2[a, 1, h].astype(F32)

    def step_bx2(b):
        b_land(0, b)
        for i in range(2):
            PB[b, xp, i] = plus(PB[b, xp, i], T1[b, 0, i]).astype(BF16)
        b_copy(BX2P, b).start()
        for i in range(2):
            PB[b, xm, 2 + i] = plus(PB[b, xm, 2 + i], T1[b, 1, i]).astype(BF16)
        b_copy(BX2M, b).start()

    def step_bs(b):
        b_land(1, b)
        for i in range(2):
            o = 2 * (1 - pair) + i
            BS[b, i] = (plus(PB[b, x, o], T2[b, 0, o]) + T2[b, 1, o].astype(F32)).astype(BF16)
        b_copy(BSK, b).start()
        for i in range(2):
            o = 2 * pair + i
            BK[b, i] = plus(PB[b, x, o], T2[b, 0, o]) + T2[b, 1, o].astype(F32)

    def step_bp(b):
        b_land(2, b)
        BP[b] = plus(BK[b, zp % 2], U1[b, zp % 2]).astype(BF16)
        b_copy(BPK, b).start()
        gr_ref[B_PARTS[b][0] // 2, :, out_cols(B_PARTS[b], role)] = plus(
            BK[b, z % 2], U1[b, z % 2]
        )

    def step_bf(b):
        b_land(3, b)
        gr_ref[B_PARTS[b][0] // 2, :, out_cols(B_PARTS[b], 1 - role)] = U2[b].astype(F32)

    V1P, V1M, VIP, VIM, V2P, V2M, WSK = range(7)
    lo, hi = pl.ds(0, ROWS), pl.ds(ROWS, ROWS)
    y_of = (y2, yp, ym, y)
    Y_SEM = (0, 1, 2, 3, 3, 2, 4)

    def y_copy(k, e):
        a, b, d = (
            (EK.at[e, y2, lo], V1.at[e, 0], dYp),
            (EK.at[e, y2, hi], V1.at[e, 1], dYm),
            (EK.at[e, yp, hi], V2.at[e, 0, hi], dYp),
            (EK.at[e, ym, lo], V2.at[e, 1, lo], dYm),
            (EK.at[e, yp, lo], V2.at[e, 0, lo], dYp),
            (EK.at[e, ym, hi], V2.at[e, 1, hi], dYm),
            (WS.at[e], W1.at[e], dP),
        )[k]
        return rc(a, b, ysend.at[e], yrecv.at[e, Y_SEM[k]], d)

    def y_land(n, e):
        b = (V1.at[e, 0], V1.at[e, 1], V2.at[e, :, hi], V2.at[e, :, lo], W1.at[e])[n]
        rc(b, b, ysend.at[e], yrecv.at[e, n], dC).wait_recv()

    def sib_copy(e, i):
        return rc(
            ES.at[e, y_of[i]], ER.at[e, y_of[i]], csend.at[e], crecv.at[e, i], dC
        )

    def nt(a, b):
        return lax.dot_general(a, b, (((1,), (1,)), ((), ())), preferred_element_type=F32)

    def y_product(e, yy, cc):
        rows = pl.ds(pl.multiple_of((yy * 2 + cc) * FEAT, FEAT), FEAT)
        if e == 0:
            v = nt(G[1], W[0, rows, :]) + nt(G[2], W[1, rows, :])
        else:
            v = nt(G[0], W[2, rows, :])
        return v.astype(BF16)

    def y_sib(e, i):
        ES[e, y_of[i]] = y_product(e, y_of[i], 1 - c)
        sib_copy(e, i).start()

    def y_own(e, i):
        EK[e, y_of[i]] = y_product(e, y_of[i], c)

    def y_merge(e, i, *sends):
        sib_copy(e, i).wait_recv()
        yy = y_of[i]

        @pl.loop(0, 6)
        def _(n):
            r = pl.ds(pl.multiple_of(n * 128, 128), 128)
            EK[e, yy, r, :] = plus(EK[e, yy, r, :], ER[e, yy, r, :]).astype(BF16)

        for k in sends:
            y_copy(k, e).start()

    def y_relay(e, d):
        y_land(d, e)
        yy = (yp, ym)[d]

        @pl.loop(0, 3)
        def _(n):
            r = pl.ds(pl.multiple_of(d * ROWS + n * 128, 128), 128)
            rv = pl.ds(pl.multiple_of(n * 128, 128), 128)
            EK[e, yy, r, :] = plus(EK[e, yy, r, :], V1[e, d, rv, :]).astype(BF16)

        y_copy((V2P, V2M)[d], e).start()

    def y_p(e):
        y_land(2, e)

        @pl.loop(0, 3)
        def _(n):
            r = pl.ds(pl.multiple_of(ROWS + n * 128, 128), 128)
            rv = pl.ds(pl.multiple_of(n * 128, 128), 128)
            WS[e, rv, :] = (
                plus(EK[e, y, r, :], V2[e, 0, r, :]) + V2[e, 1, r, :].astype(F32)
            ).astype(BF16)

        y_copy(WSK, e).start()

    def y_f(e):
        y_land(3, e)

        @pl.loop(0, 3)
        def _(n):
            r = pl.ds(pl.multiple_of(n * 128, 128), 128)
            FS[e, r, :] = plus(EK[e, y, r, :], V2[e, 0, r, :]) + V2[e, 1, r, :].astype(F32)

    def y_block_out():
        y_land(4, 1)
        for b in range(NB):
            rows = slice(b * BLK, (b + 1) * BLK)
            branch = FS[1, rows, :] + W1[1, rows, :].astype(F32)
            bo_ref[rows, :] = (XT[rows, :].astype(F32) + branch).astype(BF16)

    def y_partial():
        y_land(4, 0)
        for b in range(NB):
            rows = slice(b * BLK, (b + 1) * BLK)
            g = FS[0, rows, :] + W1[0, rows, :].astype(F32)
            FS[0, rows, :] = g
            BSUM[b : b + 1, :] = jnp.sum(g * NRM[rows, :], axis=0, keepdims=True)
        TZ[1, z] = jnp.dot(
            onehots()[0], BSUM[...], precision=HIGHEST, preferred_element_type=F32
        ).astype(BF16)
        tsend(1, 0)

    def y_grad_tokens():
        total = tsum(1, 1)
        gg_ref[...] = jnp.sum(total, axis=0, keepdims=True)
        gain = GN[...]
        BSUM[...] = jnp.dot(
            onehots()[1], gain * total / GHOST, precision=HIGHEST, preferred_element_type=F32
        )
        for b in range(NB):
            rows = slice(b * BLK, (b + 1) * BLK)
            g, nb = FS[0, rows, :], NRM[rows, :]
            dyb = DYB[0, rows, own_cols].astype(F32)
            gt_ref[rows, :] = (
                dyb + SCB[b : b + 1, :] * (gain * g - nb * BSUM[b : b + 1, :])
            ).astype(BF16)

    def left(sem, kib):
        ref = LT.at[0, pl.ds(0, kib * 1024 // (4 * ROWS))]
        rc(ref, ref, sem, sem, dC).wait_send()

    def left_gather(B, g):
        left(gsend.at[g], 30 * 96)

    def left_table(e):
        left(ssend.at[e], 6 * 24)

    def left_sums(e):
        left(csend.at[e], 4 * 384)
        left(ysend.at[e], 7 * 192)

    def left_a(a):
        left(asend.at[a], 18 * 32)

    def left_b(b):
        left(bsend.at[b], 15 * 32)

    start()
    stat0()
    tmid(0)
    fwd(DYB, 0, (2,), 4)
    fwd(DYB, 0, (1,), 3)
    fwd(DYB, 0, (0,), 5, 6)
    fwd(DYB, 0, (16,), 9)
    fwd(DYB, 0, (17,), 10)
    stat2()
    gland(DYB, 0, 9)
    gland(DYB, 0, 8)
    gland(DYB, 0, 10)
    gland(HB, 1, 8)
    fwd(DYB, 0, (3,), 7, 11)
    k_block(0, 0, True)
    gland(DYB, 0, 11)
    gh(0)
    fwd(HB, 1, (1,), 3)
    fwd(HB, 1, (2,), 4)
    fwd(DYB, 0, (18,), 19, 20, 12)
    fwd(HB, 1, (0,), 5, 6)
    transposed(DYB, 0, 0)
    gland(DYB, 0, 12)
    fwd(HB, 1, (16,), 9)
    fwd(HB, 1, (17,), 10)
    fwd(HB, 1, (18,), 19, 20, 12)
    tx_block(DYB, 0, 1, 0)
    gh_block(0, True)
    gland(HB, 1, 9)
    gland(HB, 1, 12)
    k_block(1, 0, True)
    fwd(HB, 1, (3,), 7, 11)
    gland(HB, 1, 10)
    k_block(0, 1, False)
    fwd(DYB, 0, (7,), 15)
    k_block(0, 2, False)
    gland(HB, 1, 11)
    fwd(DYB, 0, (5,), 13)
    fwd(DYB, 0, (6,), 14)
    k_block(0, 3, False)
    units(0)
    gland(DYB, 0, 15)
    transposed(HB, 1, 0)
    gland(DYB, 0, 14)
    gh_block(2, False)
    gland(DYB, 0, 13)
    tx_block(DYB, 0, 1, 1)
    gh_block(3, False)
    tx_block(DYB, 0, 1, 2)
    gh_block(1, False)
    tx_block(DYB, 0, 1, 3)
    fwd(HB, 1, (5,), 13)
    fwd(HB, 1, (6,), 14)
    k_half(1, 2, False, False)
    fwd(HB, 1, (7,), 15)
    k_half(1, 1, False, False)
    k_half(1, 3, False, False)
    gland(HB, 1, 13)
    k_half(1, 1, True, False)
    gland(HB, 1, 14)
    k_half(1, 2, True, False)
    gland(HB, 1, 15)
    k_half(1, 3, True, False)
    units(1)
    weights_first(1)
    weights(0)
    y_sib(0, 0)
    transposed(HB, 1, 1)
    left_gather(HB, 1)
    weights(5)
    left_gather(DYB, 0)
    left_table(0)
    y_own(0, 0)
    y_merge(0, 0, V1P, V1M)
    y_sib(0, 2)
    y_sib(1, 0)
    y_own(0, 2)
    weights(4)
    y_merge(0, 2, VIM)
    step_bx2(0)
    y_sib(0, 1)
    weights(2)
    step_bx2(5)
    y_own(0, 1)
    y_merge(0, 1, VIP)
    step_ap(1)
    step_bx2(1)
    y_own(1, 0)
    y_relay(0, 1)
    y_own(1, 3)
    y_sib(1, 3)
    y_sib(1, 1)
    y_own(1, 1)
    step_ap(0)
    y_merge(1, 0, V1P, V1M)
    y_sib(1, 2)
    y_relay(0, 0)
    y_sib(0, 3)
    weights(3)
    step_ap(4)
    step_bs(0)
    y_own(1, 2)
    y_merge(1, 3)
    step_bx2(2)
    y_own(0, 3)
    y_merge(0, 3)
    step_ax1(1)
    y_merge(1, 2, VIM)
    y_p(0)
    y_merge(1, 1, VIP)
    step_bs(5)
    y_relay(1, 0)
    step_bx2(4)
    step_bx2(3)
    step_ap(2)
    step_bx2(6)
    step_ax1(4)
    step_ax1(0)
    y_relay(1, 1)
    step_bs(2)
    y_f(0)
    step_ax2(1)
    y_partial()
    step_ap(3)
    step_bs(3)
    step_bs(4)
    step_bp(0)
    step_bp(5)
    step_ax1(2)
    step_ax2(4)
    step_bs(6)
    step_bs(1)
    step_bp(2)
    y_p(1)
    step_ax1(3)
    step_ax2(0)
    y_f(1)
    tmid(1)
    step_bp(3)
    step_bf(5)
    step_af(1)
    step_bf(2)
    step_af(4)
    left_b(5)
    step_bp(6)
    step_bp(4)
    step_ax2(2)
    step_bf(0)
    left_b(0)
    step_ax2(3)
    step_bp(1)
    left_b(2)
    left_a(1)
    left_a(4)
    step_af(0)
    step_bf(3)
    y_grad_tokens()
    left_a(0)
    step_af(2)
    y_block_out()
    left_b(3)
    left_sums(0)
    left_table(1)
    left_a(2)
    step_bf(6)
    step_bf(4)
    left_sums(1)
    left_b(4)
    left_b(6)
    step_af(3)
    left_a(3)
    step_bf(1)
    left_b(1)


def emit(bo_ref, gt_ref, rn_ref, gg_ref, gr_ref, bo, gt, rn, gg, g_gate, g_up, g_down, sem):
    copies = [
        pltpu.make_async_copy(a, b, sem.at[i])
        for i, (a, b) in enumerate((
            (gr_ref.at[1], g_gate), (gr_ref.at[2], g_up), (gr_ref.at[0], g_down),
            (bo_ref, bo), (gt_ref, gt), (rn_ref, rn), (gg_ref, gg),
        ))
    ]
    for d in copies:
        d.start()
    for d in copies:
        d.wait()


def body(tokens, norm_gain, running_sq, gate_weight, up_weight, down_weight_t, groups, cotangent):
    V = pltpu.VMEM
    any_spec = pl.BlockSpec(memory_space=pl.ANY)
    vmem_spec = pl.BlockSpec(memory_space=pltpu.VMEM)
    na, nb = len(A_PARTS), len(B_PARTS)
    sq = (128, 128)
    dma = pltpu.SemaphoreType.DMA
    scratch = [
        V((1, NB), jnp.int32), V((1, FEAT), F32), V((1, FEAT), F32),
        V((ROWS, FEAT), BF16), V((ROWS, FEAT), F32), V((NB, FEAT), F32), V((NB, FEAT), F32),
        V((2, ROWS, WIDTH), BF16), V((2, ROWS, WIDTH), BF16), V((2, WIDTH, 2 * ROWS), BF16),
        V((3, WIDTH, HALF), BF16), V((3, 2 * ROWS, HALF), BF16),
        V((2, ROWS, HALF), F32), V((2, ROWS, HALF), F32), V((2, ROWS, HALF), F32),
        V((2, 4, GROUPS, FEAT), BF16), V((2, 4, GROUPS, FEAT), BF16),
        V((na, WIDTH, 128), BF16), V((na, 1024, 128), BF16), V((na, 4, *sq), BF16),
        V((na, 4, 2, *sq), BF16), V((na, 2, *sq), BF16), V((na, 2, 2, *sq), BF16),
        V((nb, 4, 4, *sq), BF16), V((nb, 2, 2, *sq), BF16), V((nb, 2, 4, *sq), BF16),
        V((nb, 2, *sq), F32), V((nb, 2, *sq), BF16), V((nb, 2, *sq), BF16),
        V((nb, *sq), BF16), V((nb, *sq), BF16),
        V((2, 4, 2 * ROWS, FEAT), BF16), V((2, 4, 2 * ROWS, FEAT), BF16),
        V((2, 4, 2 * ROWS, FEAT), BF16), V((2, 2, ROWS, FEAT), BF16),
        V((2, 2, 2 * ROWS, FEAT), BF16), V((2, ROWS, FEAT), BF16), V((2, ROWS, FEAT), BF16),
        V((2, ROWS, FEAT), F32),
        dma((8,)), dma((2,)), dma((2, 18)), dma((2,)), dma((2, 2, 3)),
        dma((na,)), dma((4, na)), dma((nb,)), dma((4, nb)), dma((2,)), dma((2, 5)),
        dma((2,)), dma((2, 4)),
    ]
    held = (
        ((ROWS, FEAT), BF16), ((ROWS, FEAT), BF16), ((1, FEAT), F32), ((1, FEAT), F32),
        ((3, 128, 1024), F32),
    )
    results = pl.pallas_call(
        kernel,
        out_shape=tuple(pltpu.VMEM(shape, dtype) for shape, dtype in held),
        in_specs=[any_spec] * 8,
        out_specs=(vmem_spec,) * 5,
        scratch_shapes=scratch,
        compiler_params=pltpu.CompilerParams(
            collective_id=0, has_side_effects=True, vmem_limit_bytes=VMEM_LIMIT
        ),
    )(
        tokens, norm_gain.reshape(1, -1), running_sq.reshape(1, -1), gate_weight, up_weight,
        down_weight_t, groups.reshape(1, -1), cotangent,
    )
    weight = jax.ShapeDtypeStruct((128, 1024), F32)
    block_out, grad_tokens, run_new, gain_grad, g_gate, g_up, g_down = pl.pallas_call(
        emit,
        out_shape=tuple(jax.ShapeDtypeStruct(*a) for a in held[:4]) + (weight,) * 3,
        in_specs=[vmem_spec] * 5,
        out_specs=(any_spec,) * 7,
        scratch_shapes=[dma((7,))],
        compiler_params=pltpu.CompilerParams(vmem_limit_bytes=4 << 20),
    )(*results)
    return (
        block_out, grad_tokens, run_new.reshape(-1), gain_grad.reshape(-1), g_gate, g_up, g_down,
    )


def solution(mesh):
    placed = (
        P("tok", "mp"),
        P(),
        P("mp"),
        P(None, "mp"),
        P(None, "mp"),
        P(None, "mp"),
        P("tok"),
        P("tok", "mp"),
    )
    return jax.shard_map(
        body,
        mesh=mesh,
        in_specs=placed,
        out_specs=(
            P("tok", "mp"),
            P("tok", "mp"),
            P("mp"),
            P("mp"),
            P("tok", "mp"),
            P("tok", "mp"),
            P("tok", "mp"),
        ),
        check_vma=False,
    )
```

```python
import jax
import jax.numpy as jnp
from jax import lax
from jax.experimental import pallas as pl
from jax.experimental.pallas import tpu as pltpu
from jax.sharding import PartitionSpec as P

GHOST = 128
BLK = 16
ROWS = 384
FEAT = 256
WIDTH = 2048
HALF = 512
GROUPS = 48
G_SEM = (0, 1, 2, 3, 3, 4, 5, 6, 7, 8, 9, 10, 11, 12, 13, 14, 15, 16, 17, 4, 5)
VMEM_LIMIT = 62 << 20
NB = 24
A_PARTS = tuple((p, 0) for p in range(5))
B_PARTS = tuple((p, 1) for p in range(5)) + ((5, 0), (5, 1))

epsilon = 1e-05
momentum = 0.1
F32 = jnp.float32
BF16 = jnp.bfloat16
HIGHEST = lax.Precision.HIGHEST


def kernel(
    tok_hbm, gain_hbm, run_hbm, gw_hbm, uw_hbm, dw_hbm, grp_hbm, cot_hbm,
    bo_ref, gt_ref, rn_ref, gg_ref, gr_ref,
    GR, GN, RN, XT, NRM, BSUM, SCB, DYB, HB, LT, W, G, GT, LF, GH,
    TZ, TX, PA, RSA, SPA, QA, R1, R2, PB, T1, T2, BK, BS, U1, BP, U2,
    EK, ES, ER, V1, V2, WS, W1, FS,
    lsem, gsend, grecv, ssend, srecv, asend, arecv, bsend, brecv, ysend, yrecv, csend, crecv,
):
    t = lax.axis_index("tok")
    m = lax.axis_index("mp")
    z, x = t // 4, t % 4
    y, c = m // 2, m % 2
    zp = z + 1 - 2 * (z % 2)
    zs = 3 - z
    role = ((z + 1) // 2) % 2
    yp, ym, y2 = (y + 1) % 4, (y + 3) % 4, (y + 2) % 4
    xp, xm, x2 = (x + 1) % 4, (x + 3) % 4, (x + 2) % 4
    dC = (t, y * 2 + 1 - c)
    dP = (zp * 4 + x, m)
    dS = (zs * 4 + x, m)
    dYp, dYm = (t, yp * 2 + c), (t, ym * 2 + c)
    dXp, dXm = (z * 4 + xp, m), (z * 4 + xm, m)

    def rc(src, dst, ss, rs, dev):
        return pltpu.make_async_remote_copy(
            src_ref=src, dst_ref=dst, send_sem=ss, recv_sem=rs,
            device_id=dev, device_id_type=pl.DeviceIdType.MESH,
        )

    own_cols = pl.ds(pl.multiple_of(m * FEAT, FEAT), FEAT)

    bar = pltpu.get_barrier_semaphore()
    z_others = [(((z + k) % 4) * 4 + x, m) for k in range(1, 4)]
    x_others = [(z * 4 + (x + k) % 4, m) for k in range(1, 4)]
    for d in (*z_others, *x_others, dC, dYp, dYm):
        pl.semaphore_signal(bar, inc=1, device_id=d, device_id_type=pl.DeviceIdType.MESH)

    cp_dy = pltpu.make_async_copy(cot_hbm, DYB.at[0, :, own_cols], lsem.at[0])
    cp_dy.start()
    cp_x = pltpu.make_async_copy(tok_hbm, XT, lsem.at[1])
    cp_x.start()
    small = [
        pltpu.make_async_copy(a, b, lsem.at[5 + i])
        for i, (a, b) in enumerate(
            ((grp_hbm, GR), (gain_hbm.at[:, own_cols], GN), (run_hbm, RN))
        )
    ]
    for d in small:
        d.start()
    wcols = pl.ds(pl.multiple_of(role * HALF, HALF), HALF)
    cp_w = [
        pltpu.make_async_copy(h.at[:, wcols], W.at[i], lsem.at[2 + i])
        for i, h in enumerate((gw_hbm, uw_hbm, dw_hbm))
    ]
    for k in (2, 0, 1):
        cp_w[k].start()

    def sl(B, slot, yy, cc, r0=0, n=ROWS):
        return B.at[slot, pl.ds(r0, n), pl.ds(pl.multiple_of((yy * 2 + cc) * FEAT, FEAT), FEAT)]

    def gcopy(B, g, k):
        h = ROWS // 2
        if k in (0, 18):
            r = 0 if k == 0 else h
            a, b, d = sl(B, 0, y, c, r, h), sl(B, 1, y, c, r, h), dP
        elif k in (1, 16):
            a = b = sl(B, 0, y, c, 0 if k == 1 else h, h)
            d = dYp
        elif k in (2, 17):
            a = b = sl(B, 0, y, c, h if k == 2 else 0, h)
            d = dYm
        elif k == 3:
            a = b = sl(B, 0, ym, c, 0, h)
            d = dYp
        elif k == 4:
            a = b = sl(B, 0, yp, c, h, h)
            d = dYm
        elif k in (5, 6, 19, 20):
            a = b = sl(B, 1, y, c, 0 if k < 7 else h, h)
            d = dYp if k in (5, 19) else dYm
        elif k == 7:
            a, b, d = sl(B, 0, y2, c), sl(B, 1, y2, c), dP
        else:
            slot = (k - 8) // 4
            yy = (y, ym, yp, y2)[(k - 8) % 4]
            a = b = sl(B, slot, yy, c)
            d = dC
        return rc(a, b, gsend.at[g], grecv.at[g, G_SEM[k]], d)

    def gland(B, g, k):
        h = ROWS // 2
        if k in (0, 18):
            b = sl(B, 1, y, c, 0 if k == 0 else h, h)
        elif k in (1, 16):
            b = sl(B, 0, ym, c, 0 if k == 1 else h, h)
        elif k in (2, 17):
            b = sl(B, 0, yp, c, h if k == 2 else 0, h)
        elif k == 3:
            b = sl(B, 0, y2, c)
        elif k == 5:
            b = sl(B, 1, ym, c)
        elif k == 6:
            b = sl(B, 1, yp, c)
        elif k == 7:
            b = sl(B, 1, y2, c)
        else:
            b = sl(B, (k - 8) // 4, (y, ym, yp, y2)[(k - 8) % 4], 1 - c)
        rc(b, b, gsend.at[g], grecv.at[g, G_SEM[k]], dC).wait_recv()

    def gstart(B, g, *ks):
        for k in ks:
            gcopy(B, g, k).start()

    def fwd(B, g, land, *sends):
        for k in land:
            gland(B, g, k)
        gstart(B, g, *sends)

    def tcopy(e, a, k):
        buf, me, d = ((TZ, z, z_others), (TX, x, x_others))[a]
        ref = buf.at[e, me]
        return rc(ref, ref, ssend.at[e], srecv.at[e, a, k - 1], d[k - 1])

    def tsum(e, a):
        buf, me = ((TZ, z), (TX, x))[a]
        for k in range(1, 4):
            ref = buf.at[e, (me + 4 - k) % 4]
            rc(ref, ref, ssend.at[e], srecv.at[e, a, k - 1], dC).wait_recv()
        return (buf[e, 0].astype(F32) + buf[e, 1].astype(F32)) + (
            buf[e, 2].astype(F32) + buf[e, 3].astype(F32)
        )

    def tsend(e, a):
        for k in range(1, 4):
            tcopy(e, a, k).start()

    def tmid(e):
        TX[e, x] = tsum(e, 0).astype(BF16)
        tsend(e, 1)

    def onehots():
        grow = GR[...]
        rows = lax.broadcasted_iota(jnp.int32, (GROUPS, NB), 0)
        onehot = (rows == jnp.broadcast_to(grow, (GROUPS, NB))).astype(F32)
        diag = lax.broadcasted_iota(jnp.int32, (NB, NB), 0) == lax.broadcasted_iota(
            jnp.int32, (NB, NB), 1
        )
        gcol = jnp.sum(
            jnp.where(diag, jnp.broadcast_to(grow, (NB, NB)), 0).astype(F32),
            axis=1, keepdims=True,
        )
        onehot_t = (
            lax.broadcasted_iota(jnp.int32, (NB, GROUPS), 1).astype(F32)
            == jnp.broadcast_to(gcol, (NB, GROUPS))
        ).astype(F32)
        return onehot, onehot_t

    def start():
        cp_dy.wait()
        pl.semaphore_wait(bar, 9)
        gstart(DYB, 0, 1, 2, 16, 17, 8)

    def stat0():
        cp_x.wait()
        for d in small:
            d.wait()
        for b in range(NB):
            xb = XT[b * BLK : (b + 1) * BLK, :].astype(F32)
            BSUM[b : b + 1, :] = jnp.sum(xb * xb, axis=0, keepdims=True)
        TZ[0, z] = jnp.dot(
            onehots()[0], BSUM[...], precision=HIGHEST, preferred_element_type=F32
        ).astype(BF16)
        tsend(0, 0)
        gstart(DYB, 0, 0, 18)

    def stat2():
        quad = tsum(0, 1) / GHOST
        rn_ref[...] = (1.0 - momentum) * RN[...] + momentum * (
            jnp.sum(quad, axis=0, keepdims=True) / GROUPS
        )
        gain = GN[...]
        SCB[...] = jnp.dot(
            onehots()[1], lax.rsqrt(quad + epsilon), precision=HIGHEST, preferred_element_type=F32
        )
        for b in range(NB):
            rows = slice(b * BLK, (b + 1) * BLK)
            nb = XT[rows, :].astype(F32) * SCB[b : b + 1, :]
            NRM[rows, :] = nb
            HB[0, rows, own_cols] = (gain * nb).astype(BF16)
        gstart(HB, 1, 1, 2, 0, 18, 16, 17, 8)

    def transposed(B, i, slot):
        @pl.loop(0, 8)
        def _(j):
            cols = pl.ds(pl.multiple_of(j * FEAT, FEAT), FEAT)
            LT[i, cols, pl.ds(slot * ROWS, ROWS)] = B[slot, :, cols].T

    def k_part(wi, slot, yy):
        ks = pl.ds(pl.multiple_of(yy * 2 * FEAT, 2 * FEAT), 2 * FEAT)
        return jnp.dot(HB[slot, :, ks], W[wi, ks, :], preferred_element_type=F32)

    def k_block(slot, i, first):
        yy = (y, ym, yp, y2)[i]
        if first and slot == 0:
            cp_w[0].wait()
            cp_w[1].wait()
        for wi, dst in ((0, GT), (1, LF)):
            v = k_part(wi, slot, yy)
            dst[slot] = v if first else dst[slot] + v

    def units(slot):
        @pl.loop(0, ROWS // 32)
        def _(i):
            r = pl.ds(pl.multiple_of(i * 32, 32), 32)
            ro = pl.ds(pl.multiple_of(slot * ROWS + i * 32, 32), 32)
            gate, lift, gh = GT[slot, r, :], LF[slot, r, :], GH[slot, r, :]
            sigma = jax.nn.sigmoid(gate)
            G[0, ro, :] = (gate * sigma * lift).astype(BF16)
            G[1, ro, :] = (gh * lift * sigma * (1.0 + gate * (1.0 - sigma))).astype(BF16)
            G[2, ro, :] = (gh * gate * sigma).astype(BF16)

    def k_half(slot, i, sib, first):
        cc = 1 - c if sib else c
        ks = pl.ds(pl.multiple_of(((y, ym, yp, y2)[i] * 2 + cc) * FEAT, FEAT), FEAT)
        for wi, dst in ((0, GT), (1, LF)):
            v = jnp.dot(HB[slot, :, ks], W[wi, ks, :], preferred_element_type=F32)
            dst[slot] = v if first else dst[slot] + v

    def gh_block(i, first):
        yy = (y, ym, yp, y2)[i]
        ks = pl.ds(pl.multiple_of(yy * 2 * FEAT, 2 * FEAT), 2 * FEAT)
        v = jnp.dot(DYB[1, :, ks], W[2, ks, :], preferred_element_type=F32)
        GH[1] = v if first else GH[1] + v

    def tx_block(B, n, slot, i):
        yy = (y, ym, yp, y2)[i]
        for h in range(2):
            cols = pl.ds(pl.multiple_of((yy * 2 + h) * FEAT, FEAT), FEAT)
            LT[n, cols, pl.ds(slot * ROWS, ROWS)] = B[slot, :, cols].T

    def gh(slot):
        if slot == 0:
            cp_w[2].wait()
        GH[slot] = jnp.dot(DYB[slot], W[2], preferred_element_type=F32)

    def ready(B, g, *ks):
        for k in ks:
            gland(B, g, k)

    AS, AP, AX1P, AX1M, AXIP, AXIM, AX2P, AX2M = range(8)
    BX1P, BX1M, BXIP, BXIM, BX2P, BX2M, BSK, BPK = range(8)
    A_SEM = (0, 1, 2, 2, 3, 3, 3, 3)
    B_SEM = (0, 0, 1, 1, 1, 1, 2, 3)
    pair = z // 2
    lo2, hi2 = pl.ds(0, 2), pl.ds(2, 2)

    def a_copy(k, a):
        far = pl.ds(pl.multiple_of((1 - pair) * 1024, 1024), 1024)
        src, dst, d = (
            (PA.at[a, far], RSA.at[a], dS),
            (SPA.at[a], QA.at[a, :, role], dP),
            (QA.at[a, x2, 0], R1.at[a, 0], dXp),
            (QA.at[a, x2, 1], R1.at[a, 1], dXm),
            (QA.at[a, xp, 1], R2.at[a, 0, 1], dXp),
            (QA.at[a, xm, 0], R2.at[a, 1, 0], dXm),
            (QA.at[a, xp, 0], R2.at[a, 0, 0], dXp),
            (QA.at[a, xm, 1], R2.at[a, 1, 1], dXm),
        )[k]
        return rc(src, dst, asend.at[a], arecv.at[A_SEM[k], a], d)

    def a_land(n, a):
        b = (RSA.at[a], QA.at[a, :, 1 - role], R1.at[a], R2.at[a])[n]
        rc(b, b, asend.at[a], arecv.at[n, a], dC).wait_recv()

    def b_copy(k, b):
        src, dst, d = (
            (PB.at[b, x2, lo2], T1.at[b, 0], dXp),
            (PB.at[b, x2, hi2], T1.at[b, 1], dXm),
            (PB.at[b, xp, hi2], T2.at[b, 0, hi2], dXp),
            (PB.at[b, xm, lo2], T2.at[b, 1, lo2], dXm),
            (PB.at[b, xp, lo2], T2.at[b, 0, lo2], dXp),
            (PB.at[b, xm, hi2], T2.at[b, 1, hi2], dXm),
            (BS.at[b], U1.at[b], dS),
            (BP.at[b], U2.at[b], dP),
        )[k]
        return rc(src, dst, bsend.at[b], brecv.at[B_SEM[k], b], d)

    def b_land(n, b):
        r = (T1.at[b], T2.at[b], U1.at[b], U2.at[b])[n]
        rc(r, r, bsend.at[b], brecv.at[n, b], dC).wait_recv()

    def weights(p):
        mi, j = p // 2, p % 2

        @pl.loop(0, 2)
        def _(n):
            rh = (1 - pair + n) % 2
            rows = pl.ds(pl.multiple_of(rh * 1024, 1024), 1024)
            res = jnp.dot(
                LT[(mi + 1) // 2, rows, :],
                G[mi, :, j * 256 : (j + 1) * 256],
                preferred_element_type=F32,
            ).astype(BF16)
            for off in range(2):
                part = res[:, off * 128 : (off + 1) * 128]
                if (p, off) in A_PARTS:
                    PA[A_PARTS.index((p, off)), rows, :] = part
                else:
                    b = B_PARTS.index((p, off))
                    for i in range(8):
                        PB[b, i % 4, rh * 2 + i // 4] = part[i * 128 : (i + 1) * 128]

            @pl.when(n == 0)
            def _():
                for off in range(2):
                    if (p, off) in A_PARTS:
                        a_copy(AS, A_PARTS.index((p, off))).start()

        for ks in ((BX1P, BX1M), (BXIP, BXIM)):
            for off in range(2):
                if (p, off) in B_PARTS:
                    for k in ks:
                        b_copy(k, B_PARTS.index((p, off))).start()

    def weights_first(p):
        mi, j = p // 2, p % 2

        @pl.loop(0, 4)
        def _(n):
            xd = (x + 2 + n) % 4
            blocks = [pl.multiple_of(zd * HALF + xd * 128, 128) for zd in range(4)]
            lhs = jnp.concatenate(
                [LT[(mi + 1) // 2, pl.ds(r, 128), :] for r in blocks], axis=0
            )
            res = jnp.dot(
                lhs, G[mi, :, j * 256 : (j + 1) * 256], preferred_element_type=F32
            ).astype(BF16)
            for off in range(2):
                for zd in range(4):
                    part = res[zd * 128 : (zd + 1) * 128, off * 128 : (off + 1) * 128]
                    if (p, off) in A_PARTS:
                        PA[A_PARTS.index((p, off)), pl.ds(blocks[zd], 128), :] = part
                    else:
                        PB[B_PARTS.index((p, off)), xd, zd] = part
            for at, ks in ((0, (BX1P, BX1M)), (1, (BXIM,)), (3, (BXIP,))):

                @pl.when(n == at)
                def _():
                    for k in ks:
                        for off in range(2):
                            if (p, off) in B_PARTS:
                                b_copy(k, B_PARTS.index((p, off))).start()

        for off in range(2):
            if (p, off) in A_PARTS:
                a_copy(AS, A_PARTS.index((p, off))).start()

    def plus(a, b):
        return a.astype(F32) + b.astype(F32)

    def out_cols(part, half):
        p, off = part
        return pl.ds(pl.multiple_of(half * HALF + (p % 2) * 256 + off * 128, 128), 128)

    def step_ap(a):
        a_land(0, a)
        for xd in range(4):
            ra = pl.ds(pl.multiple_of(zp * HALF + xd * 128, 128), 128)
            rr = pl.ds(pl.multiple_of((zp % 2) * HALF + xd * 128, 128), 128)
            SPA[a, xd] = plus(PA[a, ra, :], RSA[a, rr, :]).astype(BF16)
        a_copy(AP, a).start()
        for xd in range(4):
            ra = pl.ds(pl.multiple_of(z * HALF + xd * 128, 128), 128)
            rr = pl.ds(pl.multiple_of((z % 2) * HALF + xd * 128, 128), 128)
            QA[a, xd, role] = plus(PA[a, ra, :], RSA[a, rr, :]).astype(BF16)

    def step_ax1(a):
        a_land(1, a)
        for k in (AX1P, AX1M, AXIP, AXIM):
            a_copy(k, a).start()

    def step_ax2(a):
        a_land(2, a)
        QA[a, xp, 0] = plus(QA[a, xp, 0], R1[a, 0]).astype(BF16)
        a_copy(AX2P, a).start()
        QA[a, xm, 1] = plus(QA[a, xm, 1], R1[a, 1]).astype(BF16)
        a_copy(AX2M, a).start()

    def step_af(a):
        a_land(3, a)
        for h in range(2):
            gr_ref[A_PARTS[a][0] // 2, :, out_cols(A_PARTS[a], h)] = plus(
                QA[a, x, h], R2[a, 0, h]
            ) + R2[a, 1, h].astype(F32)

    def step_bx2(b):
        b_land(0, b)
        for i in range(2):
            PB[b, xp, i] = plus(PB[b, xp, i], T1[b, 0, i]).astype(BF16)
        b_copy(BX2P, b).start()
        for i in range(2):
            PB[b, xm, 2 + i] = plus(PB[b, xm, 2 + i], T1[b, 1, i]).astype(BF16)
        b_copy(BX2M, b).start()

    def step_bs(b):
        b_land(1, b)
        for i in range(2):
            o = 2 * (1 - pair) + i
            BS[b, i] = (plus(PB[b, x, o], T2[b, 0, o]) + T2[b, 1, o].astype(F32)).astype(BF16)
        b_copy(BSK, b).start()
        for i in range(2):
            o = 2 * pair + i
            BK[b, i] = plus(PB[b, x, o], T2[b, 0, o]) + T2[b, 1, o].astype(F32)

    def step_bp(b):
        b_land(2, b)
        BP[b] = plus(BK[b, zp % 2], U1[b, zp % 2]).astype(BF16)
        b_copy(BPK, b).start()
        gr_ref[B_PARTS[b][0] // 2, :, out_cols(B_PARTS[b], role)] = plus(
            BK[b, z % 2], U1[b, z % 2]
        )

    def step_bf(b):
        b_land(3, b)
        gr_ref[B_PARTS[b][0] // 2, :, out_cols(B_PARTS[b], 1 - role)] = U2[b].astype(F32)

    V1P, V1M, VIP, VIM, V2P, V2M, WSK = range(7)
    lo, hi = pl.ds(0, ROWS), pl.ds(ROWS, ROWS)
    y_of = (y2, yp, ym, y)
    Y_SEM = (0, 1, 2, 3, 3, 2, 4)

    def y_copy(k, e):
        a, b, d = (
            (EK.at[e, y2, lo], V1.at[e, 0], dYp),
            (EK.at[e, y2, hi], V1.at[e, 1], dYm),
            (EK.at[e, yp, hi], V2.at[e, 0, hi], dYp),
            (EK.at[e, ym, lo], V2.at[e, 1, lo], dYm),
            (EK.at[e, yp, lo], V2.at[e, 0, lo], dYp),
            (EK.at[e, ym, hi], V2.at[e, 1, hi], dYm),
            (WS.at[e], W1.at[e], dP),
        )[k]
        return rc(a, b, ysend.at[e], yrecv.at[e, Y_SEM[k]], d)

    def y_land(n, e):
        b = (V1.at[e, 0], V1.at[e, 1], V2.at[e, :, hi], V2.at[e, :, lo], W1.at[e])[n]
        rc(b, b, ysend.at[e], yrecv.at[e, n], dC).wait_recv()

    def sib_copy(e, i):
        return rc(
            ES.at[e, y_of[i]], ER.at[e, y_of[i]], csend.at[e], crecv.at[e, i], dC
        )

    def nt(a, b):
        return lax.dot_general(a, b, (((1,), (1,)), ((), ())), preferred_element_type=F32)

    def y_product(e, yy, cc):
        rows = pl.ds(pl.multiple_of((yy * 2 + cc) * FEAT, FEAT), FEAT)
        if e == 0:
            v = nt(G[1], W[0, rows, :]) + nt(G[2], W[1, rows, :])
        else:
            v = nt(G[0], W[2, rows, :])
        return v.astype(BF16)

    def y_sib(e, i):
        ES[e, y_of[i]] = y_product(e, y_of[i], 1 - c)
        sib_copy(e, i).start()

    def y_own(e, i):
        EK[e, y_of[i]] = y_product(e, y_of[i], c)

    def y_merge(e, i, *sends):
        sib_copy(e, i).wait_recv()
        yy = y_of[i]

        @pl.loop(0, 6)
        def _(n):
            r = pl.ds(pl.multiple_of(n * 128, 128), 128)
            EK[e, yy, r, :] = plus(EK[e, yy, r, :], ER[e, yy, r, :]).astype(BF16)

        for k in sends:
            y_copy(k, e).start()

    def y_relay(e, d):
        y_land(d, e)
        yy = (yp, ym)[d]

        @pl.loop(0, 3)
        def _(n):
            r = pl.ds(pl.multiple_of(d * ROWS + n * 128, 128), 128)
            rv = pl.ds(pl.multiple_of(n * 128, 128), 128)
            EK[e, yy, r, :] = plus(EK[e, yy, r, :], V1[e, d, rv, :]).astype(BF16)

        y_copy((V2P, V2M)[d], e).start()

    def y_p(e):
        y_land(2, e)

        @pl.loop(0, 3)
        def _(n):
            r = pl.ds(pl.multiple_of(ROWS + n * 128, 128), 128)
            rv = pl.ds(pl.multiple_of(n * 128, 128), 128)
            WS[e, rv, :] = (
                plus(EK[e, y, r, :], V2[e, 0, r, :]) + V2[e, 1, r, :].astype(F32)
            ).astype(BF16)

        y_copy(WSK, e).start()

    def y_f(e):
        y_land(3, e)

        @pl.loop(0, 3)
        def _(n):
            r = pl.ds(pl.multiple_of(n * 128, 128), 128)
            FS[e, r, :] = plus(EK[e, y, r, :], V2[e, 0, r, :]) + V2[e, 1, r, :].astype(F32)

    def y_block_out():
        y_land(4, 1)
        for b in range(NB):
            rows = slice(b * BLK, (b + 1) * BLK)
            branch = FS[1, rows, :] + W1[1, rows, :].astype(F32)
            bo_ref[rows, :] = (XT[rows, :].astype(F32) + branch).astype(BF16)

    def y_partial():
        y_land(4, 0)
        for b in range(NB):
            rows = slice(b * BLK, (b + 1) * BLK)
            g = FS[0, rows, :] + W1[0, rows, :].astype(F32)
            FS[0, rows, :] = g
            BSUM[b : b + 1, :] = jnp.sum(g * NRM[rows, :], axis=0, keepdims=True)
        TZ[1, z] = jnp.dot(
            onehots()[0], BSUM[...], precision=HIGHEST, preferred_element_type=F32
        ).astype(BF16)
        tsend(1, 0)

    def y_grad_tokens():
        total = tsum(1, 1)
        gg_ref[...] = jnp.sum(total, axis=0, keepdims=True)
        gain = GN[...]
        BSUM[...] = jnp.dot(
            onehots()[1], gain * total / GHOST, precision=HIGHEST, preferred_element_type=F32
        )
        for b in range(NB):
            rows = slice(b * BLK, (b + 1) * BLK)
            g, nb = FS[0, rows, :], NRM[rows, :]
            dyb = DYB[0, rows, own_cols].astype(F32)
            gt_ref[rows, :] = (
                dyb + SCB[b : b + 1, :] * (gain * g - nb * BSUM[b : b + 1, :])
            ).astype(BF16)

    def left(sem, kib):
        ref = LT.at[0, pl.ds(0, kib * 1024 // (4 * ROWS))]
        rc(ref, ref, sem, sem, dC).wait_send()

    def left_gather(B, g):
        left(gsend.at[g], 30 * 96)

    def left_table(e):
        left(ssend.at[e], 6 * 24)

    def left_sums(e):
        left(csend.at[e], 4 * 384)
        left(ysend.at[e], 7 * 192)

    def left_a(a):
        left(asend.at[a], 18 * 32)

    def left_b(b):
        left(bsend.at[b], 15 * 32)

    start()
    stat0()
    tmid(0)
    fwd(DYB, 0, (2,), 4)
    fwd(DYB, 0, (1,), 3)
    fwd(DYB, 0, (16,), 9)
    fwd(DYB, 0, (0,), 5, 6)
    stat2()
    gland(DYB, 0, 8)
    gland(DYB, 0, 9)
    fwd(DYB, 0, (17,), 10)
    fwd(DYB, 0, (3,), 7, 11)
    gland(HB, 1, 8)
    gland(DYB, 0, 11)
    gland(DYB, 0, 10)
    transposed(DYB, 0, 0)
    gh(0)
    fwd(HB, 1, (1,), 3)
    fwd(HB, 1, (2,), 4)
    fwd(DYB, 0, (18,), 19, 20, 12)
    fwd(HB, 1, (0,), 5, 6)
    gland(DYB, 0, 12)
    fwd(HB, 1, (17,), 10)
    tx_block(DYB, 0, 1, 0)
    gh_block(0, True)
    k_block(0, 0, True)
    fwd(HB, 1, (16,), 9)
    fwd(HB, 1, (18,), 19, 20, 12)
    fwd(HB, 1, (3,), 7, 11)
    gland(HB, 1, 10)
    gland(HB, 1, 9)
    gland(HB, 1, 12)
    k_block(1, 0, True)
    k_block(0, 2, False)
    fwd(DYB, 0, (7,), 15)
    fwd(DYB, 0, (5,), 13)
    gland(HB, 1, 11)
    fwd(DYB, 0, (6,), 14)
    transposed(HB, 1, 0)
    k_block(0, 1, False)
    gland(DYB, 0, 15)
    k_block(0, 3, False)
    gland(DYB, 0, 14)
    gland(DYB, 0, 13)
    tx_block(DYB, 0, 1, 1)
    gh_block(1, False)
    tx_block(DYB, 0, 1, 3)
    units(0)
    gh_block(2, False)
    fwd(HB, 1, (5,), 13)
    fwd(HB, 1, (6,), 14)
    k_half(1, 1, False, False)
    gh_block(3, False)
    fwd(HB, 1, (7,), 15)
    tx_block(DYB, 0, 1, 2)
    k_half(1, 3, False, False)
    k_half(1, 2, False, False)
    gland(HB, 1, 13)
    k_half(1, 1, True, False)
    gland(HB, 1, 14)
    k_half(1, 2, True, False)
    gland(HB, 1, 15)
    k_half(1, 3, True, False)
    units(1)
    weights_first(0)
    weights(1)
    left_gather(HB, 1)
    left_table(0)
    left_gather(DYB, 0)
    transposed(HB, 1, 1)
    y_sib(0, 0)
    weights(5)
    y_own(0, 0)
    y_merge(0, 0, V1P, V1M)
    y_sib(0, 2)
    weights(4)
    y_own(0, 2)
    y_sib(1, 0)
    y_merge(0, 2, VIM)
    y_own(0, 1)
    y_sib(0, 1)
    step_bx2(1)
    step_ap(0)
    weights(2)
    y_sib(0, 3)
    y_merge(0, 1, VIP)
    y_relay(0, 1)
    step_bx2(0)
    step_bx2(5)
    y_sib(1, 3)
    y_sib(1, 1)
    step_ap(1)
    y_own(1, 1)
    step_bx2(4)
    y_own(1, 0)
    y_relay(0, 0)
    y_own(0, 3)
    y_merge(1, 0, V1P, V1M)
    y_own(1, 3)
    y_merge(1, 3)
    y_own(1, 2)
    step_ap(4)
    y_merge(0, 3)
    y_sib(1, 2)
    step_bx2(2)
    weights(3)
    y_p(0)
    step_ax1(0)
    step_ax1(1)
    step_bx2(6)
    y_merge(1, 2, VIM)
    y_merge(1, 1, VIP)
    step_bs(0)
    step_ap(2)
    y_f(0)
    step_bs(5)
    y_relay(1, 1)
    step_bs(2)
    step_bs(4)
    step_bs(1)
    step_ax1(4)
    y_partial()
    step_ap(3)
    step_bx2(3)
    y_relay(1, 0)
    step_ax2(0)
    step_bp(0)
    step_ax2(1)
    step_bp(5)
    step_ax1(2)
    step_bs(6)
    step_ax2(4)
    step_bp(2)
    y_p(1)
    step_ax1(3)
    step_bp(4)
    step_bs(3)
    step_bp(1)
    step_af(0)
    step_bf(0)
    step_af(1)
    tmid(1)
    step_bf(5)
    left_a(0)
    left_b(0)
    left_a(1)
    left_b(5)
    step_ax2(2)
    step_bp(6)
    y_f(1)
    step_af(4)
    step_ax2(3)
    step_bp(3)
    step_bf(2)
    y_grad_tokens()
    left_sums(0)
    left_a(4)
    y_block_out()
    left_sums(1)
    step_af(2)
    left_table(1)
    step_bf(4)
    left_b(4)
    left_b(2)
    step_bf(1)
    left_a(2)
    step_bf(6)
    left_b(1)
    left_b(6)
    step_af(3)
    left_a(3)
    step_bf(3)
    left_b(3)


def emit(bo_ref, gt_ref, rn_ref, gg_ref, gr_ref, bo, gt, rn, gg, g_gate, g_up, g_down, sem):
    copies = [
        pltpu.make_async_copy(a, b, sem.at[i])
        for i, (a, b) in enumerate((
            (gr_ref.at[1], g_gate), (gr_ref.at[2], g_up), (gr_ref.at[0], g_down),
            (bo_ref, bo), (gt_ref, gt), (rn_ref, rn), (gg_ref, gg),
        ))
    ]
    for d in copies:
        d.start()
    for d in copies:
        d.wait()


def body(tokens, norm_gain, running_sq, gate_weight, up_weight, down_weight_t, groups, cotangent):
    V = pltpu.VMEM
    any_spec = pl.BlockSpec(memory_space=pl.ANY)
    vmem_spec = pl.BlockSpec(memory_space=pltpu.VMEM)
    na, nb = len(A_PARTS), len(B_PARTS)
    sq = (128, 128)
    dma = pltpu.SemaphoreType.DMA
    scratch = [
        V((1, NB), jnp.int32), V((1, FEAT), F32), V((1, FEAT), F32),
        V((ROWS, FEAT), BF16), V((ROWS, FEAT), F32), V((NB, FEAT), F32), V((NB, FEAT), F32),
        V((2, ROWS, WIDTH), BF16), V((2, ROWS, WIDTH), BF16), V((2, WIDTH, 2 * ROWS), BF16),
        V((3, WIDTH, HALF), BF16), V((3, 2 * ROWS, HALF), BF16),
        V((2, ROWS, HALF), F32), V((2, ROWS, HALF), F32), V((2, ROWS, HALF), F32),
        V((2, 4, GROUPS, FEAT), BF16), V((2, 4, GROUPS, FEAT), BF16),
        V((na, WIDTH, 128), BF16), V((na, 1024, 128), BF16), V((na, 4, *sq), BF16),
        V((na, 4, 2, *sq), BF16), V((na, 2, *sq), BF16), V((na, 2, 2, *sq), BF16),
        V((nb, 4, 4, *sq), BF16), V((nb, 2, 2, *sq), BF16), V((nb, 2, 4, *sq), BF16),
        V((nb, 2, *sq), F32), V((nb, 2, *sq), BF16), V((nb, 2, *sq), BF16),
        V((nb, *sq), BF16), V((nb, *sq), BF16),
        V((2, 4, 2 * ROWS, FEAT), BF16), V((2, 4, 2 * ROWS, FEAT), BF16),
        V((2, 4, 2 * ROWS, FEAT), BF16), V((2, 2, ROWS, FEAT), BF16),
        V((2, 2, 2 * ROWS, FEAT), BF16), V((2, ROWS, FEAT), BF16), V((2, ROWS, FEAT), BF16),
        V((2, ROWS, FEAT), F32),
        dma((8,)), dma((2,)), dma((2, 18)), dma((2,)), dma((2, 2, 3)),
        dma((na,)), dma((4, na)), dma((nb,)), dma((4, nb)), dma((2,)), dma((2, 5)),
        dma((2,)), dma((2, 4)),
    ]
    held = (
        ((ROWS, FEAT), BF16), ((ROWS, FEAT), BF16), ((1, FEAT), F32), ((1, FEAT), F32),
        ((3, 128, 1024), F32),
    )
    results = pl.pallas_call(
        kernel,
        out_shape=tuple(pltpu.VMEM(shape, dtype) for shape, dtype in held),
        in_specs=[any_spec] * 8,
        out_specs=(vmem_spec,) * 5,
        scratch_shapes=scratch,
        compiler_params=pltpu.CompilerParams(
            collective_id=0, has_side_effects=True, vmem_limit_bytes=VMEM_LIMIT
        ),
    )(
        tokens, norm_gain.reshape(1, -1), running_sq.reshape(1, -1), gate_weight, up_weight,
        down_weight_t, groups.reshape(1, -1), cotangent,
    )
    weight = jax.ShapeDtypeStruct((128, 1024), F32)
    block_out, grad_tokens, run_new, gain_grad, g_gate, g_up, g_down = pl.pallas_call(
        emit,
        out_shape=tuple(jax.ShapeDtypeStruct(*a) for a in held[:4]) + (weight,) * 3,
        in_specs=[vmem_spec] * 5,
        out_specs=(any_spec,) * 7,
        scratch_shapes=[dma((7,))],
        compiler_params=pltpu.CompilerParams(vmem_limit_bytes=4 << 20),
    )(*results)
    return (
        block_out, grad_tokens, run_new.reshape(-1), gain_grad.reshape(-1), g_gate, g_up, g_down,
    )


def solution(mesh):
    placed = (
        P("tok", "mp"),
        P(),
        P("mp"),
        P(None, "mp"),
        P(None, "mp"),
        P(None, "mp"),
        P("tok"),
        P("tok", "mp"),
    )
    return jax.shard_map(
        body,
        mesh=mesh,
        in_specs=placed,
        out_specs=(
            P("tok", "mp"),
            P("tok", "mp"),
            P("mp"),
            P("mp"),
            P("tok", "mp"),
            P("tok", "mp"),
            P("tok", "mp"),
        ),
        check_vma=False,
    )
```
